8 devices in a mesh: dp: 1 (over z), tp: 2 (over y), sp: 4 (over x, core).
Axes of the slice: x: 2, y: 2, z: 1, core: 2. Of those that a mesh axis runs over, the one named last changes fastest.
Arguments:
- hidden: bfloat16 [16, 3072], P('dp')
- positions: int32 [16], P('dp')
- norm_attn: float32 [3072], replicated
- norm_mlp: float32 [3072], replicated
- w_qkv: bfloat16 [3072, 9216], P(None, 'tp')
- w_out: bfloat16 [3072, 3072], P('tp')
- w_gate_up: bfloat16 [3072, 16384], P(None, 'tp')
- w_down: bfloat16 [8192, 3072], P('tp')
- k_cache: bfloat16 [16, 3072, 32, 96], P('dp', 'sp', 'tp')
- v_cache: bfloat16 [16, 3072, 32, 96], P('dp', 'sp', 'tp')
Outputs:
- output 1: bfloat16 [16, 3072], P('dp')
- output 2: bfloat16 [16, 3072, 32, 96], P('dp', 'sp', 'tp')
- output 3: bfloat16 [16, 3072, 32, 96], P('dp', 'sp', 'tp')
All inputs are finite; a program needn't handle non-finite values.
Results may differ from the reference program's by a relative error of at most 0.00882399.
Values sent between devices are 32-bit elements.
A program may use at most 1 GiB of HBM per device.

```python
import jax
import jax.numpy as jnp
from jax import lax

NUM_SEQS = 16
CACHE_LEN = 3072
TEN_PAR = 2
MODEL_DIM = 3072
NUM_HEADS = 32
KV_HEADS = 32
HEAD_DIM = 96
FFN_DIM = 8192
WINDOW = 2047

GROUP_SIZE = NUM_HEADS // KV_HEADS
QKV_COLS = (NUM_HEADS + 2 * KV_HEADS) * HEAD_DIM
FFN_LOCAL = FFN_DIM // TEN_PAR
ROPE_BASE = 10000.0
NORM_EPS = 1e-5


def rms_norm(values, gain_vec):
    mean_sq = jnp.mean(values * values, axis=-1, keepdims=True)
    return values * lax.rsqrt(mean_sq + NORM_EPS) * gain_vec


def rope_angles(positions):
    inv_freq = ROPE_BASE ** (-jnp.arange(0, HEAD_DIM, 2).astype(jnp.float32) / HEAD_DIM)
    angles = positions.astype(jnp.float32)[:, None] * inv_freq[None, :]
    angles = jnp.concatenate([angles, angles], axis=-1)
    return jnp.cos(angles), jnp.sin(angles)


def rotate_half(values, cos_tab, sin_tab):
    half_dim = values.shape[-1] // 2
    turned = jnp.concatenate([-values[..., half_dim:], values[..., :half_dim]], axis=-1)
    return values * cos_tab + turned * sin_tab


def seq_attention(operands):
    q_rows, k_seq, v_seq, position = operands
    scores = jnp.einsum('kgd,jkd->kgj', q_rows.astype(jnp.float32), k_seq.astype(jnp.float32)) * (HEAD_DIM ** -0.5)
    slot_ids = jnp.arange(CACHE_LEN)
    in_window = (slot_ids <= position) & (slot_ids >= position - WINDOW)
    scores = jnp.where(in_window, scores, -jnp.inf)
    row_max = jnp.max(scores, axis=-1, keepdims=True)
    weights = jnp.exp(scores - row_max)
    weight_sum = jnp.sum(weights, axis=-1)
    acc_sum = jnp.einsum('kgj,jkd->kgd', weights.astype(jnp.bfloat16).astype(jnp.float32), v_seq.astype(jnp.float32))
    return (acc_sum / weight_sum[..., None]).astype(jnp.bfloat16)


def setup_inputs(seed: int = 0, part: int = 0) -> dict:
    base_key = jax.random.key(seed)
    shared_keys = jax.random.split(base_key, 6)
    own_keys = jax.random.split(jax.random.fold_in(base_key, part), 6)
    cache_shape = (NUM_SEQS, CACHE_LEN, KV_HEADS, HEAD_DIM)
    hidden = jax.random.normal(own_keys[0], (NUM_SEQS, MODEL_DIM), jnp.float32).astype(jnp.bfloat16)
    low_pos = WINDOW // 2
    drawn_pos = jax.random.randint(own_keys[1], (NUM_SEQS,), low_pos, CACHE_LEN, jnp.int32)
    row_ids = jnp.arange(NUM_SEQS)
    positions = jnp.where(row_ids == 0, CACHE_LEN - 1, drawn_pos)
    positions = jnp.where(jnp.logical_and(row_ids == NUM_SEQS - 1, NUM_SEQS > 1), low_pos, positions).astype(jnp.int32)
    norm_attn = 1.0 + 0.3 * jax.random.normal(shared_keys[0], (MODEL_DIM,), jnp.float32)
    norm_mlp = 1.0 + 0.3 * jax.random.normal(shared_keys[1], (MODEL_DIM,), jnp.float32)
    w_qkv = (jax.random.normal(shared_keys[2], (MODEL_DIM, QKV_COLS), jnp.float32) * MODEL_DIM ** -0.5).astype(jnp.bfloat16)
    w_out = (jax.random.normal(shared_keys[3], (NUM_HEADS * HEAD_DIM, MODEL_DIM), jnp.float32) * (NUM_HEADS * HEAD_DIM) ** -0.5).astype(jnp.bfloat16)
    w_gate_up = (jax.random.normal(shared_keys[4], (MODEL_DIM, 2 * FFN_DIM), jnp.float32) * MODEL_DIM ** -0.5).astype(jnp.bfloat16)
    w_down = (jax.random.normal(shared_keys[5], (FFN_DIM, MODEL_DIM), jnp.float32) * FFN_DIM ** -0.5).astype(jnp.bfloat16)
    pos_wave = jnp.cos(jnp.pi * jnp.arange(CACHE_LEN).astype(jnp.float32) / WINDOW)[None, :, None, None]
    key_dir = jax.random.normal(own_keys[3], (NUM_SEQS, 1, KV_HEADS, HEAD_DIM), jnp.float32)
    k_cache = (jax.random.normal(own_keys[2], cache_shape, jnp.float32) + key_dir * pos_wave).astype(jnp.bfloat16)
    v_trend = 2.0 * jax.random.normal(own_keys[5], (NUM_SEQS, 1, KV_HEADS, HEAD_DIM), jnp.float32)
    v_cache = (jax.random.normal(own_keys[4], cache_shape, jnp.float32) + v_trend * pos_wave).astype(jnp.bfloat16)
    return {'hidden': hidden, 'positions': positions, 'norm_attn': norm_attn, 'norm_mlp': norm_mlp, 'w_qkv': w_qkv, 'w_out': w_out, 'w_gate_up': w_gate_up, 'w_down': w_down, 'k_cache': k_cache, 'v_cache': v_cache}


def reference(hidden, positions, norm_attn, norm_mlp, w_qkv, w_out, w_gate_up, w_down, k_cache, v_cache):
    num_rows = hidden.shape[0]
    resid_in = hidden.astype(jnp.float32)
    normed = rms_norm(resid_in, norm_attn).astype(jnp.bfloat16)
    qkv_proj = jnp.dot(normed, w_qkv, preferred_element_type=jnp.float32).reshape(num_rows, KV_HEADS, GROUP_SIZE + 2, HEAD_DIM)
    cos_tab, sin_tab = rope_angles(positions)
    q_new = rotate_half(qkv_proj[:, :, :GROUP_SIZE], cos_tab[:, None, None], sin_tab[:, None, None]).astype(jnp.bfloat16)
    k_new = rotate_half(qkv_proj[:, :, GROUP_SIZE], cos_tab[:, None], sin_tab[:, None]).astype(jnp.bfloat16)
    v_new = qkv_proj[:, :, GROUP_SIZE + 1].astype(jnp.bfloat16)
    slot_ids = jnp.arange(CACHE_LEN)
    at_slot = (slot_ids[None, :] == positions[:, None])[:, :, None, None]
    k_upd = jnp.where(at_slot, k_new[:, None], k_cache)
    v_upd = jnp.where(at_slot, v_new[:, None], v_cache)
    attended = lax.map(seq_attention, (q_new, k_upd, v_upd, positions)).reshape(num_rows, NUM_HEADS * HEAD_DIM)
    out_parts = jnp.einsum('bsk,skd->bsd', attended.reshape(num_rows, TEN_PAR, -1).astype(jnp.float32), w_out.reshape(TEN_PAR, -1, MODEL_DIM).astype(jnp.float32))
    mid_resid = resid_in + jnp.sum(out_parts.astype(jnp.bfloat16).astype(jnp.float32), axis=1)
    normed_mlp = rms_norm(mid_resid, norm_mlp).astype(jnp.bfloat16)
    gate_up = jnp.dot(normed_mlp, w_gate_up, preferred_element_type=jnp.float32).reshape(num_rows, TEN_PAR, 2, FFN_LOCAL)
    act_vals = (jax.nn.silu(gate_up[:, :, 0]) * gate_up[:, :, 1]).astype(jnp.bfloat16)
    down_parts = jnp.einsum('bsf,sfd->bsd', act_vals.astype(jnp.float32), w_down.reshape(TEN_PAR, FFN_LOCAL, MODEL_DIM).astype(jnp.float32))
    result = mid_resid + jnp.sum(down_parts.astype(jnp.bfloat16).astype(jnp.float32), axis=1)
    return (result.astype(jnp.bfloat16), k_upd, v_upd)
```

```python
import functools

import jax
import jax.numpy as jnp
from jax import lax
from jax.experimental import pallas as pl
from jax.experimental.pallas import tpu as pltpu
from jax.sharding import PartitionSpec as P

WINDOW = 2047
ROPE_BASE = 10000.0
NORM_EPS = 1e-5
NEG = -1e30
MESH = pl.DeviceIdType.MESH


def rms_norm(values, gain_vec):
    mean_sq = jnp.mean(values * values, axis=-1, keepdims=True)
    return values * lax.rsqrt(mean_sq + NORM_EPS) * gain_vec


def rope_tables(positions, head_dim):
    inv_freq = ROPE_BASE ** (-jnp.arange(0, head_dim, 2).astype(jnp.float32) / head_dim)
    angles = positions.astype(jnp.float32)[:, None] * inv_freq[None, :]
    angles = jnp.concatenate([angles, angles], axis=-1)
    return jnp.cos(angles), jnp.sin(angles)


def rotate_half(values, cos_tab, sin_tab):
    half_dim = values.shape[-1] // 2
    turned = jnp.concatenate([-values[..., half_dim:], values[..., :half_dim]], axis=-1)
    return values * cos_tab + turned * sin_tab


def new_entries(hidden, positions, norm_attn, w_qkv, kv_count, head_dim):
    num_rows = hidden.shape[0]
    resid_in = hidden.astype(jnp.float32)
    normed = rms_norm(resid_in, norm_attn).astype(jnp.bfloat16)
    qkv_proj = jnp.dot(normed, w_qkv, preferred_element_type=jnp.float32).reshape(num_rows, kv_count, 3, head_dim)
    cos_tab, sin_tab = rope_tables(positions, head_dim)
    q_new = rotate_half(qkv_proj[:, :, 0], cos_tab[:, None], sin_tab[:, None])
    k_new = rotate_half(qkv_proj[:, :, 1], cos_tab[:, None], sin_tab[:, None])
    v_new = qkv_proj[:, :, 2]
    rows = lambda x: x.reshape(num_rows, -1)
    return rows(q_new), rows(k_new), rows(v_new)


def attend_kernel(pos_ref, q_ref, kn_ref, vn_ref, k_ref, v_ref, ko_ref, vo_ref, o_ref, ml_ref, kt_ref, vt_ref):
    b = pl.program_id(0)
    rows, heads, dim, block = q_ref.shape[0], k_ref.shape[1], k_ref.shape[2], k_ref.shape[3]
    width = heads * dim

    @pl.when(b == 0)
    def _():
        pad = jnp.zeros((128 - rows, width), jnp.float32)
        kt_ref[...] = jnp.concatenate([kn_ref[...], pad], axis=0).T
        vt_ref[...] = jnp.concatenate([vn_ref[...], pad], axis=0).T

    base = lax.axis_index('sp') * block
    pos = pos_ref[b]
    slot = pos - base
    ko_ref[...] = k_ref[...]
    vo_ref[...] = v_ref[...]

    @pl.when((slot >= 0) & (slot < block))
    def _():
        lane = lax.rem(slot, 128)
        start = pl.multiple_of(slot - lane, 128)
        shift = lax.rem(lane - b + 128, 128)
        hit = lax.broadcasted_iota(jnp.int32, (width, 128), 1) == lane
        for new_ref, out_ref in ((kt_ref, ko_ref), (vt_ref, vo_ref)):
            entry = pltpu.roll(new_ref[...], shift, 1)
            old = out_ref[0, :, :, pl.ds(start, 128)].reshape(width, 128).astype(jnp.float32)
            out_ref[0, :, :, pl.ds(start, 128)] = jnp.where(hit, entry, old).astype(jnp.bfloat16).reshape(heads, dim, 128)

    own = lax.broadcasted_iota(jnp.int32, (heads, width), 1) // dim == lax.broadcasted_iota(jnp.int32, (heads, width), 0)
    q_row = jnp.broadcast_to(q_ref[pl.ds(b, 1), :], (heads, width))
    q_diag = jnp.where(own, q_row, 0.0).astype(jnp.bfloat16)
    scores = jnp.dot(q_diag, ko_ref[0].reshape(width, block), preferred_element_type=jnp.float32) * (dim ** -0.5)
    slot_ids = lax.broadcasted_iota(jnp.int32, (heads, block), 1) + base
    in_window = (slot_ids <= pos) & (slot_ids >= pos - WINDOW)
    scores = jnp.where(in_window, scores, NEG)
    row_max = jnp.max(scores, axis=1, keepdims=True)
    weights = jnp.where(in_window, jnp.exp(scores - row_max), 0.0)
    row_sum = jnp.sum(weights, axis=1, keepdims=True)
    acc = lax.dot_general(weights.astype(jnp.bfloat16), vo_ref[0].reshape(width, block), (((1,), (1,)), ((), ())), preferred_element_type=jnp.float32)
    o_ref[pl.ds(b, 1), :] = jnp.sum(jnp.where(own, acc, 0.0), axis=0, keepdims=True)
    lane_ids = lax.broadcasted_iota(jnp.int32, (heads, 128), 1)
    head_ids = lax.broadcasted_iota(jnp.int32, (heads, 128), 0)
    stats = jnp.where(lane_ids == head_ids, row_max, 0.0) + jnp.where(lane_ids == head_ids + heads, row_sum, 0.0)
    ml_ref[pl.ds(b, 1), :] = jnp.sum(stats, axis=0, keepdims=True)


def attend(positions, q_rows, k_rows, v_rows, k_t, v_t):
    rows, heads, dim, block = k_t.shape
    width = heads * dim
    full = lambda shape: pl.BlockSpec(shape, lambda b, pos: (0, 0))
    cache = pl.BlockSpec((1, heads, dim, block), lambda b, pos: (b, 0, 0, 0))
    return pl.pallas_call(
        attend_kernel,
        out_shape=(jax.ShapeDtypeStruct(k_t.shape, k_t.dtype), jax.ShapeDtypeStruct(v_t.shape, v_t.dtype), jax.ShapeDtypeStruct((rows, width), jnp.float32), jax.ShapeDtypeStruct((rows, 128), jnp.float32)),
        grid_spec=pltpu.PrefetchScalarGridSpec(
            num_scalar_prefetch=1,
            grid=(rows,),
            in_specs=[full((rows, width))] * 3 + [cache] * 2,
            out_specs=(cache, cache, full((rows, width)), full((rows, 128))),
            scratch_shapes=[pltpu.VMEM((width, 128), jnp.float32)] * 2,
        ),
        compiler_params=pltpu.CompilerParams(dimension_semantics=("arbitrary",), vmem_limit_bytes=48 << 20),
        name="attend",
    )(positions, q_rows, k_rows, v_rows, k_t, v_t)


def layer_tail(resid_in, attended, norm_mlp, w_out, w_gate_up, w_down):
    out_part = jnp.dot(attended, w_out, preferred_element_type=jnp.float32).astype(jnp.bfloat16).astype(jnp.float32)
    mid_resid = resid_in + lax.psum(out_part, 'tp')
    normed_mlp = rms_norm(mid_resid, norm_mlp).astype(jnp.bfloat16)
    gate_up = jnp.dot(normed_mlp, w_gate_up, preferred_element_type=jnp.float32)
    ffn_local = w_down.shape[0]
    act_vals = (jax.nn.silu(gate_up[:, :ffn_local]) * gate_up[:, ffn_local:]).astype(jnp.bfloat16)
    down_part = jnp.dot(act_vals, w_down, preferred_element_type=jnp.float32).astype(jnp.bfloat16).astype(jnp.float32)
    result = mid_resid + lax.psum(down_part, 'tp')
    return result.astype(jnp.bfloat16)


def solution(mesh):
    cache_spec = P('dp', 'sp', 'tp', None)

    def local_step(hidden, positions, norm_attn, norm_mlp, w_qkv, w_out, w_gate_up, w_down, k_cache, v_cache):
        num_rows, block_len, kv_local, head_dim = k_cache.shape
        q_rows, k_rows, v_rows = new_entries(hidden, positions, norm_attn, w_qkv, kv_local, head_dim)
        k_upd, v_upd, o_part, stats = attend(positions, q_rows, k_rows, v_rows, k_cache.transpose(0, 2, 3, 1), v_cache.transpose(0, 2, 3, 1))
        row_max, row_sum = stats[:, :kv_local], stats[:, kv_local:2 * kv_local]
        alpha = jnp.exp(row_max - lax.pmax(row_max, 'sp'))
        total = lax.psum(alpha * row_sum, 'sp')
        acc = lax.psum(o_part.reshape(num_rows, kv_local, head_dim) * alpha[..., None], 'sp')
        attended = (acc / total[..., None]).astype(jnp.bfloat16).reshape(num_rows, -1)
        result = layer_tail(hidden.astype(jnp.float32), attended, norm_mlp, w_out, w_gate_up, w_down)
        return result, k_upd.transpose(0, 3, 1, 2), v_upd.transpose(0, 3, 1, 2)

    return jax.shard_map(local_step, mesh=mesh, in_specs=(P('dp', None), P('dp'), P(None), P(None), P(None, 'tp'), P('tp', None), P(None, 'tp'), P('tp', None), cache_spec, cache_spec), out_specs=(P('dp', None), cache_spec, cache_spec), check_vma=False)
```

```python
import functools

import jax
import jax.numpy as jnp
from jax import lax
from jax.experimental import pallas as pl
from jax.experimental.pallas import tpu as pltpu
from jax.sharding import PartitionSpec as P

WINDOW = 2047
ROPE_BASE = 10000.0
NORM_EPS = 1e-5
NEG = -1e30
MESH = pl.DeviceIdType.MESH


def rms_norm(values, gain_vec):
    mean_sq = jnp.mean(values * values, axis=-1, keepdims=True)
    return values * lax.rsqrt(mean_sq + NORM_EPS) * gain_vec


def rope_tables(positions, head_dim):
    inv_freq = ROPE_BASE ** (-jnp.arange(0, head_dim, 2).astype(jnp.float32) / head_dim)
    angles = positions.astype(jnp.float32)[:, None] * inv_freq[None, :]
    angles = jnp.concatenate([angles, angles], axis=-1)
    return jnp.cos(angles), jnp.sin(angles)


def rotate_half(values, cos_tab, sin_tab):
    half_dim = values.shape[-1] // 2
    turned = jnp.concatenate([-values[..., half_dim:], values[..., :half_dim]], axis=-1)
    return values * cos_tab + turned * sin_tab


def new_entries(hidden, positions, norm_attn, w_qkv, kv_count, head_dim):
    num_rows = hidden.shape[0]
    resid_in = hidden.astype(jnp.float32)
    normed = rms_norm(resid_in, norm_attn).astype(jnp.bfloat16)
    qkv_proj = jnp.dot(normed, w_qkv, preferred_element_type=jnp.float32).reshape(num_rows, kv_count, 3, head_dim)
    cos_tab, sin_tab = rope_tables(positions, head_dim)
    q_new = rotate_half(qkv_proj[:, :, 0], cos_tab[:, None], sin_tab[:, None])
    k_new = rotate_half(qkv_proj[:, :, 1], cos_tab[:, None], sin_tab[:, None])
    v_new = qkv_proj[:, :, 2]
    rows = lambda x: x.reshape(num_rows, -1)
    return rows(q_new), rows(k_new), rows(v_new)


def attend_kernel(pos_ref, q_ref, kn_ref, vn_ref, k_ref, v_ref, ko_ref, vo_ref, om_ref, kt_ref, vt_ref):
    b = pl.program_id(0)
    rows, heads, dim, block = q_ref.shape[0], k_ref.shape[1], k_ref.shape[2], k_ref.shape[3]
    width = heads * dim

    @pl.when(b == 0)
    def _():
        pad = jnp.zeros((128 - rows, width), jnp.float32)
        kt_ref[...] = jnp.concatenate([kn_ref[...], pad], axis=0).T
        vt_ref[...] = jnp.concatenate([vn_ref[...], pad], axis=0).T

    base = lax.axis_index('sp') * block
    pos = pos_ref[b]
    slot = pos - base
    ko_ref[...] = k_ref[...]
    vo_ref[...] = v_ref[...]

    @pl.when((slot >= 0) & (slot < block))
    def _():
        lane = lax.rem(slot, 128)
        start = pl.multiple_of(slot - lane, 128)
        shift = lax.rem(lane - b + 128, 128)
        hit = lax.broadcasted_iota(jnp.int32, (width, 128), 1) == lane
        for new_ref, out_ref in ((kt_ref, ko_ref), (vt_ref, vo_ref)):
            entry = pltpu.roll(new_ref[...], shift, 1)
            old = out_ref[0, :, :, pl.ds(start, 128)].reshape(width, 128).astype(jnp.float32)
            out_ref[0, :, :, pl.ds(start, 128)] = jnp.where(hit, entry, old).astype(jnp.bfloat16).reshape(heads, dim, 128)

    own = lax.broadcasted_iota(jnp.int32, (heads, width), 1) // dim == lax.broadcasted_iota(jnp.int32, (heads, width), 0)
    q_row = jnp.broadcast_to(q_ref[pl.ds(b, 1), :], (heads, width))
    q_diag = jnp.where(own, q_row, 0.0).astype(jnp.bfloat16)
    scores = jnp.dot(q_diag, ko_ref[0].reshape(width, block), preferred_element_type=jnp.float32) * (dim ** -0.5)
    slot_ids = lax.broadcasted_iota(jnp.int32, (heads, block), 1) + base
    in_window = (slot_ids <= pos) & (slot_ids >= pos - WINDOW)
    scores = jnp.where(in_window, scores, NEG)
    row_max = jnp.max(scores, axis=1, keepdims=True)
    weights = jnp.where(in_window, jnp.exp(scores - row_max), 0.0)
    row_sum = jnp.sum(weights, axis=1, keepdims=True)
    acc = lax.dot_general(weights.astype(jnp.bfloat16), vo_ref[0].reshape(width, block), (((1,), (1,)), ((), ())), preferred_element_type=jnp.float32)
    o_row = jnp.sum(jnp.where(own, acc, 0.0), axis=0, keepdims=True)
    lane_ids = lax.broadcasted_iota(jnp.int32, (heads, 128), 1)
    head_ids = lax.broadcasted_iota(jnp.int32, (heads, 128), 0)
    half, half_width = heads // 2, width // 2
    for core in range(2):
        mine = head_ids - core * half
        keep = (mine >= 0) & (mine < half)
        stats = jnp.where(keep & (lane_ids == mine), row_max, 0.0) + jnp.where(keep & (lane_ids == mine + half), row_sum, 0.0)
        row = jnp.concatenate([o_row[:, core * half_width:(core + 1) * half_width], jnp.sum(stats, axis=0, keepdims=True)], axis=1)
        at_row = lax.broadcasted_iota(jnp.int32, (rows, half_width + 128), 0) == b
        om_ref[core] = jnp.where(at_row, row, om_ref[core])


def attend(positions, q_rows, k_rows, v_rows, k_t, v_t):
    rows, heads, dim, block = k_t.shape
    width = heads * dim
    full = lambda shape: pl.BlockSpec(shape, lambda b, pos: (0, 0))
    cache = pl.BlockSpec((1, heads, dim, block), lambda b, pos: (b, 0, 0, 0))
    return pl.pallas_call(
        attend_kernel,
        out_shape=(jax.ShapeDtypeStruct(k_t.shape, k_t.dtype), jax.ShapeDtypeStruct(v_t.shape, v_t.dtype), jax.ShapeDtypeStruct((2, rows, width // 2 + 128), jnp.float32)),
        grid_spec=pltpu.PrefetchScalarGridSpec(
            num_scalar_prefetch=1,
            grid=(rows,),
            in_specs=[full((rows, width))] * 3 + [cache] * 2,
            out_specs=(cache, cache, pl.BlockSpec((2, rows, width // 2 + 128), lambda b, pos: (0, 0, 0))),
            scratch_shapes=[pltpu.VMEM((width, 128), jnp.float32)] * 2,
        ),
        compiler_params=pltpu.CompilerParams(dimension_semantics=("arbitrary",), vmem_limit_bytes=48 << 20),
        name="attend",
    )(positions, q_rows, k_rows, v_rows, k_t, v_t)


COLS = 512


def tail_kernel(dim, om_ref, hid_ref, gain_ref, wo_hbm, wgu_hbm, wd_hbm, out_ref,
                obuf, wo, wg, wu, wd, o_cat, snd, own, got, ysnd, ygot, x1, r2, act, x2,
                w_sem, gu_sem, o_send, o_recv, p_send, p_recv, y_send, y_recv, g_send, g_recv):
    tp, sp = lax.axis_index('tp'), lax.axis_index('sp')
    core = lax.rem(sp, 2)
    partner = sp + 1 - 2 * core
    rows = hid_ref.shape[0]
    half_width = wo.shape[1]
    n_half = x1.shape[0] // 2
    n_gu, n_wd = wg.shape[0], wd.shape[0]
    units = wd.shape[1]
    ffn = wgu_hbm.shape[1] // 2

    def column(index):
        side = 1 - core if index < n_half else core
        return pl.ds(pl.multiple_of((side * n_half + index % n_half) * COLS, COLS), COLS)

    weight_copies = []
    for i in range(n_wd):
        weight_copies.append(pltpu.make_async_copy(wo_hbm.at[pl.ds(core * half_width, half_width), column(i)], wo.at[i], w_sem.at[i]))
    gate_up_copies = []
    for i in range(n_gu):
        first = core * units + i * COLS
        gate_up_copies.append(pltpu.make_async_copy(wgu_hbm.at[:, pl.ds(pl.multiple_of(first, COLS), COLS)], wg.at[i], gu_sem.at[0, i]))
        gate_up_copies.append(pltpu.make_async_copy(wgu_hbm.at[:, pl.ds(pl.multiple_of(ffn + first, COLS), COLS)], wu.at[i], gu_sem.at[1, i]))
    down_copies = []
    for i in range(n_wd):
        down_copies.append(pltpu.make_async_copy(wd_hbm.at[pl.ds(core * units, units), column(i)], wd.at[i], w_sem.at[n_wd + i]))
    for copy in weight_copies + gate_up_copies + down_copies:
        copy.start()

    barrier = pltpu.get_barrier_semaphore()
    for step in range(1, 4):
        pl.semaphore_signal(barrier, inc=1, device_id={'sp': lax.rem(sp + step, 4)}, device_id_type=MESH)
    pl.semaphore_signal(barrier, inc=1, device_id={'tp': 1 - tp}, device_id_type=MESH)
    pl.semaphore_wait(barrier, 4)

    sent = []

    def send(src, dst, send_sem, recv_sem, where):
        copy = pltpu.make_async_remote_copy(src_ref=src, dst_ref=dst, send_sem=send_sem, recv_sem=recv_sem, device_id=where, device_id_type=MESH)
        copy.start()
        sent.append(copy)
        return copy

    o_copies = []
    for step in (2, 1, 3):
        peer = lax.rem(sp + step, 4)
        o_copies.append(send(om_ref.at[lax.rem(peer, 2)], obuf.at[sp], o_send.at[step - 1], o_recv.at[step - 1], {'sp': peer}))
    obuf[sp] = om_ref[core]
    for copy in o_copies:
        copy.wait_recv()

    heads = half_width // dim
    stats = [obuf[s, :, half_width:] for s in range(4)]
    top = functools.reduce(jnp.maximum, stats)
    alphas = [jnp.exp(st - top) for st in stats]
    total = functools.reduce(lambda a, b: a + b, [al * pltpu.roll(st, 128 - heads, 1) for al, st in zip(alphas, stats)])
    betas = [al / total for al in alphas]
    lane = lax.broadcasted_iota(jnp.int32, (rows, 128), 1)
    for k in range(half_width // 128):
        first, last = 128 * k // dim, (128 * k + 127) // dim
        value = None
        for s in range(4):
            scale = jnp.broadcast_to(betas[s][:, first:first + 1], (rows, 128))
            for h in range(first + 1, last + 1):
                scale = jnp.where(lane >= h * dim - 128 * k, betas[s][:, h:h + 1], scale)
            term = scale * obuf[s, :, 128 * k:128 * (k + 1)]
            value = term if value is None else value + term
        o_cat[:, 128 * k:128 * (k + 1)] = value.astype(jnp.bfloat16)

    def reduce_and_spread(stage, lhs_ref, w_ref, w_waits, base_of, dst):
        lhs = lhs_ref[...]
        first = []
        for j in range(n_half):
            w_waits[j].wait()
            snd[stage, j] = jnp.dot(lhs, w_ref[j], preferred_element_type=jnp.float32)
            first.append(send(snd.at[stage, j], got.at[stage, j], p_send.at[stage, j], p_recv.at[stage, j], {'sp': partner}))
        for j in range(n_half):
            w_waits[n_half + j].wait()
            own[j] = jnp.dot(lhs, w_ref[n_half + j], preferred_element_type=jnp.float32)
        second = []
        for j in range(n_half):
            first[j].wait_recv()
            ysnd[stage, j] = (own[j] + got[stage, j]).astype(jnp.bfloat16).astype(jnp.float32)
            second.append(send(ysnd.at[stage, j], ygot.at[stage, j], y_send.at[stage, j], y_recv.at[stage, j], {'tp': 1 - tp}))
        third = []
        for j in range(n_half):
            second[j].wait_recv()
            dst[core * n_half + j] = base_of(j) + (ysnd[stage, j] + ygot[stage, j])
            third.append(send(dst.at[core * n_half + j], dst.at[core * n_half + j], g_send.at[stage, j], g_recv.at[stage, j], {'sp': partner}))
        for copy in third:
            copy.wait_recv()

    reduce_and_spread(0, o_cat, wo, weight_copies, lambda j: hid_ref[:, column(n_half + j)].astype(jnp.float32), x1)

    square = functools.reduce(lambda a, b: a + b, [x1[i] * x1[i] for i in range(2 * n_half)])
    inv = lax.rsqrt(jnp.sum(square, axis=1, keepdims=True) / (2 * n_half * COLS) + NORM_EPS)
    for i in range(2 * n_half):
        cut = slice(i * COLS, (i + 1) * COLS)
        r2[:, cut] = (x1[i] * inv * gain_ref[:, cut]).astype(jnp.bfloat16)

    for i in range(n_gu):
        gate_up_copies[2 * i].wait()
        gate_up_copies[2 * i + 1].wait()
        gate = jnp.dot(r2[...], wg[i], preferred_element_type=jnp.float32)
        up = jnp.dot(r2[...], wu[i], preferred_element_type=jnp.float32)
        act[:, i * COLS:(i + 1) * COLS] = (gate * jax.nn.sigmoid(gate) * up).astype(jnp.bfloat16)

    reduce_and_spread(1, act, wd, down_copies, lambda j: x1[core * n_half + j], x2)
    for i in range(2 * n_half):
        out_ref[:, i * COLS:(i + 1) * COLS] = x2[i]
    for copy in sent:
        copy.wait_send()


def layer_tail(om, hidden, norm_mlp, w_out, w_gate_up, w_down, dim):
    rows, model = hidden.shape
    half_width, units = w_out.shape[0] // 2, w_down.shape[0] // 2
    n_wd, n_gu = model // COLS, units // COLS
    n_half = n_wd // 2
    f32, bf16 = jnp.float32, jnp.bfloat16
    vmem = pl.BlockSpec(memory_space=pltpu.VMEM)
    hbm = pl.BlockSpec(memory_space=pl.ANY)
    dma = pltpu.SemaphoreType.DMA
    out = pl.pallas_call(
        functools.partial(tail_kernel, dim),
        out_shape=jax.ShapeDtypeStruct((rows, model), f32),
        in_specs=[vmem, vmem, vmem, hbm, hbm, hbm],
        out_specs=vmem,
        scratch_shapes=[
            pltpu.VMEM((4, rows, half_width + 128), f32),
            pltpu.VMEM((n_wd, half_width, COLS), bf16),
            pltpu.VMEM((n_gu, model, COLS), bf16),
            pltpu.VMEM((n_gu, model, COLS), bf16),
            pltpu.VMEM((n_wd, units, COLS), bf16),
            pltpu.VMEM((rows, half_width), bf16),
            pltpu.VMEM((2, n_half, rows, COLS), f32),
            pltpu.VMEM((n_half, rows, COLS), f32),
            pltpu.VMEM((2, n_half, rows, COLS), f32),
            pltpu.VMEM((2, n_half, rows, COLS), f32),
            pltpu.VMEM((2, n_half, rows, COLS), f32),
            pltpu.VMEM((n_wd, rows, COLS), f32),
            pltpu.VMEM((rows, model), bf16),
            pltpu.VMEM((rows, units), bf16),
            pltpu.VMEM((n_wd, rows, COLS), f32),
            dma((2 * n_wd,)), dma((2, n_gu)),
            dma((3,)), dma((3,)),
            dma((2, n_half)), dma((2, n_half)),
            dma((2, n_half)), dma((2, n_half)),
            dma((2, n_half)), dma((2, n_half)),
        ],
        compiler_params=pltpu.CompilerParams(collective_id=0, has_side_effects=True, vmem_limit_bytes=54 << 20),
        name="tail",
    )(om, hidden, norm_mlp[None, :], w_out, w_gate_up, w_down)
    return out.astype(bf16)


def solution(mesh):
    cache_spec = P('dp', 'sp', 'tp', None)

    def local_step(hidden, positions, norm_attn, norm_mlp, w_qkv, w_out, w_gate_up, w_down, k_cache, v_cache):
        num_rows, block_len, kv_local, head_dim = k_cache.shape
        q_rows, k_rows, v_rows = new_entries(hidden, positions, norm_attn, w_qkv, kv_local, head_dim)
        k_upd, v_upd, om = attend(positions, q_rows, k_rows, v_rows, k_cache.transpose(0, 2, 3, 1), v_cache.transpose(0, 2, 3, 1))
        result = layer_tail(om, hidden, norm_mlp, w_out, w_gate_up, w_down, head_dim)
        return result, k_upd.transpose(0, 3, 1, 2), v_upd.transpose(0, 3, 1, 2)

    return jax.shard_map(local_step, mesh=mesh, in_specs=(P('dp', None), P('dp'), P(None), P(None), P(None, 'tp'), P('tp', None), P(None, 'tp'), P('tp', None), cache_spec, cache_spec), out_specs=(P('dp', None), cache_spec, cache_spec), check_vma=False)
```

```python
import functools

import jax
import jax.numpy as jnp
import numpy as np
from jax import lax
from jax.experimental import pallas as pl
from jax.experimental.pallas import tpu as pltpu
from jax.sharding import PartitionSpec as P

WINDOW = 2047
ROPE_BASE = 10000.0
NORM_EPS = 1e-5
NEG = -1e30
MESH = pl.DeviceIdType.MESH


QKV_COLS = 384
SLOTS = 8
W_SLOTS = 4


def attend_kernel(pos_ref, hid_ref, gain_ref, freq_ref, w_hbm, k_hbm, v_hbm, ko_hbm, vo_hbm, om_ref,
                  k_buf, v_buf, w_buf, normed_ref, qkv_t, q_t, q_rows, in_sem, out_sem, w_sem):
    rows, model = hid_ref.shape
    heads, dim, block = k_buf.shape[1:]
    width = heads * dim
    n_w = w_hbm.shape[1] // QKV_COLS
    base = lax.axis_index('sp') * block

    def w_copy(i):
        return pltpu.make_async_copy(w_hbm.at[:, pl.ds(i * QKV_COLS, QKV_COLS)], w_buf.at[i % W_SLOTS], w_sem.at[i % W_SLOTS])

    def load(b, which):
        slot = lax.rem(b, SLOTS)
        src, buf = ((k_hbm, k_buf), (v_hbm, v_buf))[which]
        return pltpu.make_async_copy(src.at[b], buf.at[slot], in_sem.at[which, slot])

    def store(b, which):
        slot = lax.rem(b, SLOTS)
        dst, buf = ((ko_hbm, k_buf), (vo_hbm, v_buf))[which]
        return pltpu.make_async_copy(buf.at[slot], dst.at[b], out_sem.at[which, slot])

    for i in range(W_SLOTS):
        w_copy(i).start()

    resid = hid_ref[...].astype(jnp.float32)
    inv = lax.rsqrt(jnp.sum(resid * resid, axis=1, keepdims=True) / model + NORM_EPS)
    normed_ref[...] = (resid * inv * gain_ref[...]).astype(jnp.bfloat16)
    pad = jnp.zeros((128 - rows, QKV_COLS), jnp.float32)
    for i in range(n_w):
        w_copy(i).wait()
        part = jnp.dot(normed_ref[...], w_buf[i % W_SLOTS], preferred_element_type=jnp.float32)
        if i + W_SLOTS < n_w:
            w_copy(i + W_SLOTS).start()
        elif i + W_SLOTS < n_w + SLOTS:
            load(i + W_SLOTS - n_w, 0).start()
            load(i + W_SLOTS - n_w, 1).start()
        qkv_t[i * QKV_COLS:(i + 1) * QKV_COLS, :] = jnp.concatenate([part, pad], axis=0).T
    for b in range(W_SLOTS, SLOTS):
        load(b, 0).start()
        load(b, 1).start()

    lane = lax.broadcasted_iota(jnp.int32, (1, 128), 1)
    pos_row = jnp.zeros((1, 128), jnp.int32)
    for b in range(rows):
        pos_row = jnp.where(lane == b, pos_ref[b], pos_row)
    angles = pos_row.astype(jnp.float32) * freq_ref[...]
    cos_t, sin_t = jnp.cos(angles), jnp.sin(angles)
    half = dim // 2
    for h in range(heads):
        for part in range(2):
            first = (3 * h + part) * dim
            low, high = qkv_t[first:first + half, :], qkv_t[first + half:first + dim, :]
            dst, at = (q_t, h * dim) if part == 0 else (qkv_t, first)
            dst[at:at + half, :] = low * cos_t - high * sin_t
            dst[at + half:at + dim, :] = high * cos_t + low * sin_t
    q_rows[...] = q_t[...].T[:rows, :]

    own = lax.broadcasted_iota(jnp.int32, (heads, width), 1) // dim == lax.broadcasted_iota(jnp.int32, (heads, width), 0)
    lane_ids = lax.broadcasted_iota(jnp.int32, (heads, 128), 1)
    head_ids = lax.broadcasted_iota(jnp.int32, (heads, 128), 0)
    half_heads, half_width = heads // 2, width // 2

    def patch(buf, slot, which, b, pos):
        at = pos - base

        @pl.when((at >= 0) & (at < block))
        def _():
            inner = lax.rem(at, 128)
            start = pl.multiple_of(at - inner, 128)
            shift = lax.rem(inner - b + 128, 128)
            hit = lax.broadcasted_iota(jnp.int32, (dim, 128), 1) == inner
            for h in range(heads):
                first = (3 * h + 1 + which) * dim
                entry = pltpu.roll(qkv_t[first:first + dim, :], shift, 1)
                old = buf[slot, h, :, pl.ds(start, 128)].astype(jnp.float32)
                buf[slot, h, :, pl.ds(start, 128)] = jnp.where(hit, entry, old).astype(jnp.bfloat16)

    def step(b, carry):
        slot = lax.rem(b, SLOTS)
        pos = pos_ref[b]

        @pl.when((b >= 2) & (b + SLOTS - 2 < rows))
        def _():
            for which in range(2):
                store(b - 2, which).wait()
                load(b + SLOTS - 2, which).start()

        load(b, 0).wait()
        patch(k_buf, slot, 0, b, pos)
        store(b, 0).start()
        q_row = jnp.broadcast_to(q_rows[pl.ds(b, 1), :], (heads, width))
        q_diag = jnp.where(own, q_row, 0.0).astype(jnp.bfloat16)
        scores = jnp.dot(q_diag, k_buf[slot].reshape(width, block), preferred_element_type=jnp.float32) * (dim ** -0.5)
        slot_ids = lax.broadcasted_iota(jnp.int32, (heads, block), 1) + base
        in_window = (slot_ids <= pos) & (slot_ids >= pos - WINDOW)
        scores = jnp.where(in_window, scores, NEG)
        row_max = jnp.max(scores, axis=1, keepdims=True)
        weights = jnp.where(in_window, jnp.exp(scores - row_max), 0.0)
        row_sum = jnp.sum(weights, axis=1, keepdims=True)
        load(b, 1).wait()
        patch(v_buf, slot, 1, b, pos)
        store(b, 1).start()
        acc = lax.dot_general(weights.astype(jnp.bfloat16), v_buf[slot].reshape(width, block), (((1,), (1,)), ((), ())), preferred_element_type=jnp.float32)
        o_row = jnp.sum(jnp.where(own, acc, 0.0), axis=0, keepdims=True)
        for core in range(2):
            mine = head_ids - core * half_heads
            keep = (mine >= 0) & (mine < half_heads)
            stats = jnp.where(keep & (lane_ids == mine), row_max, 0.0) + jnp.where(keep & (lane_ids == mine + half_heads), row_sum, 0.0)
            row = jnp.concatenate([o_row[:, core * half_width:(core + 1) * half_width], jnp.sum(stats, axis=0, keepdims=True)], axis=1)
            at_row = lax.broadcasted_iota(jnp.int32, (rows, half_width + 128), 0) == b
            om_ref[core] = jnp.where(at_row, row, om_ref[core])
        return carry

    lax.fori_loop(0, rows, step, 0)
    for b in range(rows - SLOTS, rows):
        store(b, 0).wait()
        store(b, 1).wait()


def attend(positions, hidden, norm_attn, w_qkv, k_t, v_t):
    rows, heads, dim, block = k_t.shape
    width, model = heads * dim, hidden.shape[1]
    freq = (ROPE_BASE ** (-np.arange(0, dim, 2).astype(np.float64) / dim)).astype(np.float32)
    freq = jnp.asarray(np.broadcast_to(freq[:, None], (dim // 2, 128)))
    vmem = pl.BlockSpec(memory_space=pltpu.VMEM)
    hbm = pl.BlockSpec(memory_space=pl.ANY)
    f32, bf16, dma = jnp.float32, jnp.bfloat16, pltpu.SemaphoreType.DMA
    return pl.pallas_call(
        attend_kernel,
        out_shape=(jax.ShapeDtypeStruct(k_t.shape, k_t.dtype), jax.ShapeDtypeStruct(v_t.shape, v_t.dtype), jax.ShapeDtypeStruct((2, rows, width // 2 + 128), f32)),
        in_specs=[pl.BlockSpec(memory_space=pltpu.SMEM), vmem, vmem, vmem, hbm, hbm, hbm],
        out_specs=(hbm, hbm, vmem),
        scratch_shapes=[
            pltpu.VMEM((SLOTS, heads, dim, block), bf16),
            pltpu.VMEM((SLOTS, heads, dim, block), bf16),
            pltpu.VMEM((W_SLOTS, model, QKV_COLS), bf16),
            pltpu.VMEM((rows, model), bf16),
            pltpu.VMEM((3 * width, 128), f32),
            pltpu.VMEM((width, 128), f32),
            pltpu.VMEM((rows, width), f32),
            dma((2, SLOTS)), dma((2, SLOTS)), dma((W_SLOTS,)),
        ],
        compiler_params=pltpu.CompilerParams(vmem_limit_bytes=58 << 20),
        name="attend",
    )(positions, hidden, norm_attn[None, :], freq, w_qkv, k_t, v_t)


COLS = 512


def tail_kernel(dim, om_ref, hid_ref, gain_ref, wo_hbm, wgu_hbm, wd_hbm, out_ref,
                obuf, wo, wg, wu, wd, o_cat, snd, own, got, ysnd, ygot, x1, r2, act, x2,
                w_sem, gu_sem, o_send, o_recv, p_send, p_recv, y_send, y_recv, g_send, g_recv):
    tp, sp = lax.axis_index('tp'), lax.axis_index('sp')
    core = lax.rem(sp, 2)
    partner = sp + 1 - 2 * core
    rows = hid_ref.shape[0]
    half_width = wo.shape[1]
    n_half = x1.shape[0] // 2
    n_gu, n_wd = wg.shape[0], wd.shape[0]
    units = wd.shape[1]
    ffn = wgu_hbm.shape[1] // 2

    def column(index):
        side = 1 - core if index < n_half else core
        return pl.ds(pl.multiple_of((side * n_half + index % n_half) * COLS, COLS), COLS)

    weight_copies = []
    for i in range(n_wd):
        weight_copies.append(pltpu.make_async_copy(wo_hbm.at[pl.ds(core * half_width, half_width), column(i)], wo.at[i], w_sem.at[i]))
    gate_up_copies = []
    for i in range(n_gu):
        first = core * units + i * COLS
        gate_up_copies.append(pltpu.make_async_copy(wgu_hbm.at[:, pl.ds(pl.multiple_of(first, COLS), COLS)], wg.at[i], gu_sem.at[0, i]))
        gate_up_copies.append(pltpu.make_async_copy(wgu_hbm.at[:, pl.ds(pl.multiple_of(ffn + first, COLS), COLS)], wu.at[i], gu_sem.at[1, i]))
    down_copies = []
    for i in range(n_wd):
        down_copies.append(pltpu.make_async_copy(wd_hbm.at[pl.ds(core * units, units), column(i)], wd.at[i], w_sem.at[n_wd + i]))
    for copy in weight_copies + gate_up_copies + down_copies:
        copy.start()

    barrier = pltpu.get_barrier_semaphore()
    for step in range(1, 4):
        pl.semaphore_signal(barrier, inc=1, device_id={'sp': lax.rem(sp + step, 4)}, device_id_type=MESH)
    pl.semaphore_signal(barrier, inc=1, device_id={'tp': 1 - tp}, device_id_type=MESH)
    pl.semaphore_wait(barrier, 4)

    sent = []

    def send(src, dst, send_sem, recv_sem, where):
        copy = pltpu.make_async_remote_copy(src_ref=src, dst_ref=dst, send_sem=send_sem, recv_sem=recv_sem, device_id=where, device_id_type=MESH)
        copy.start()
        sent.append(copy)
        return copy

    o_copies = []
    for step in (2, 1, 3):
        peer = lax.rem(sp + step, 4)
        o_copies.append(send(om_ref.at[lax.rem(peer, 2)], obuf.at[sp], o_send.at[step - 1], o_recv.at[step - 1], {'sp': peer}))
    obuf[sp] = om_ref[core]
    for copy in o_copies:
        copy.wait_recv()

    heads = half_width // dim
    stats = [obuf[s, :, half_width:] for s in range(4)]
    top = functools.reduce(jnp.maximum, stats)
    alphas = [jnp.exp(st - top) for st in stats]
    total = functools.reduce(lambda a, b: a + b, [al * pltpu.roll(st, 128 - heads, 1) for al, st in zip(alphas, stats)])
    betas = [al / total for al in alphas]
    lane = lax.broadcasted_iota(jnp.int32, (rows, 128), 1)
    for k in range(half_width // 128):
        first, last = 128 * k // dim, (128 * k + 127) // dim
        value = None
        for s in range(4):
            scale = jnp.broadcast_to(betas[s][:, first:first + 1], (rows, 128))
            for h in range(first + 1, last + 1):
                scale = jnp.where(lane >= h * dim - 128 * k, betas[s][:, h:h + 1], scale)
            term = scale * obuf[s, :, 128 * k:128 * (k + 1)]
            value = term if value is None else value + term
        o_cat[:, 128 * k:128 * (k + 1)] = value.astype(jnp.bfloat16)

    def reduce_and_spread(stage, lhs_ref, w_ref, w_waits, base_of, dst):
        lhs = lhs_ref[...]
        first = []
        for j in range(n_half):
            w_waits[j].wait()
            snd[stage, j] = jnp.dot(lhs, w_ref[j], preferred_element_type=jnp.float32)
            first.append(send(snd.at[stage, j], got.at[stage, j], p_send.at[stage, j], p_recv.at[stage, j], {'sp': partner}))
        for j in range(n_half):
            w_waits[n_half + j].wait()
            own[j] = jnp.dot(lhs, w_ref[n_half + j], preferred_element_type=jnp.float32)
        second = []
        for j in range(n_half):
            first[j].wait_recv()
            ysnd[stage, j] = (own[j] + got[stage, j]).astype(jnp.bfloat16).astype(jnp.float32)
            second.append(send(ysnd.at[stage, j], ygot.at[stage, j], y_send.at[stage, j], y_recv.at[stage, j], {'tp': 1 - tp}))
        third = []
        for j in range(n_half):
            second[j].wait_recv()
            dst[core * n_half + j] = base_of(j) + (ysnd[stage, j] + ygot[stage, j])
            third.append(send(dst.at[core * n_half + j], dst.at[core * n_half + j], g_send.at[stage, j], g_recv.at[stage, j], {'sp': partner}))
        for copy in third:
            copy.wait_recv()

    reduce_and_spread(0, o_cat, wo, weight_copies, lambda j: hid_ref[:, column(n_half + j)].astype(jnp.float32), x1)

    square = functools.reduce(lambda a, b: a + b, [x1[i] * x1[i] for i in range(2 * n_half)])
    inv = lax.rsqrt(jnp.sum(square, axis=1, keepdims=True) / (2 * n_half * COLS) + NORM_EPS)
    for i in range(2 * n_half):
        cut = slice(i * COLS, (i + 1) * COLS)
        r2[:, cut] = (x1[i] * inv * gain_ref[:, cut]).astype(jnp.bfloat16)

    for i in range(n_gu):
        gate_up_copies[2 * i].wait()
        gate_up_copies[2 * i + 1].wait()
        gate = jnp.dot(r2[...], wg[i], preferred_element_type=jnp.float32)
        up = jnp.dot(r2[...], wu[i], preferred_element_type=jnp.float32)
        act[:, i * COLS:(i + 1) * COLS] = (gate * jax.nn.sigmoid(gate) * up).astype(jnp.bfloat16)

    reduce_and_spread(1, act, wd, down_copies, lambda j: x1[core * n_half + j], x2)
    for i in range(2 * n_half):
        out_ref[:, i * COLS:(i + 1) * COLS] = x2[i]
    for copy in sent:
        copy.wait_send()


def layer_tail(om, hidden, norm_mlp, w_out, w_gate_up, w_down, dim):
    rows, model = hidden.shape
    half_width, units = w_out.shape[0] // 2, w_down.shape[0] // 2
    n_wd, n_gu = model // COLS, units // COLS
    n_half = n_wd // 2
    f32, bf16 = jnp.float32, jnp.bfloat16
    vmem = pl.BlockSpec(memory_space=pltpu.VMEM)
    hbm = pl.BlockSpec(memory_space=pl.ANY)
    dma = pltpu.SemaphoreType.DMA
    out = pl.pallas_call(
        functools.partial(tail_kernel, dim),
        out_shape=jax.ShapeDtypeStruct((rows, model), f32),
        in_specs=[vmem, vmem, vmem, hbm, hbm, hbm],
        out_specs=vmem,
        scratch_shapes=[
            pltpu.VMEM((4, rows, half_width + 128), f32),
            pltpu.VMEM((n_wd, half_width, COLS), bf16),
            pltpu.VMEM((n_gu, model, COLS), bf16),
            pltpu.VMEM((n_gu, model, COLS), bf16),
            pltpu.VMEM((n_wd, units, COLS), bf16),
            pltpu.VMEM((rows, half_width), bf16),
            pltpu.VMEM((2, n_half, rows, COLS), f32),
            pltpu.VMEM((n_half, rows, COLS), f32),
            pltpu.VMEM((2, n_half, rows, COLS), f32),
            pltpu.VMEM((2, n_half, rows, COLS), f32),
            pltpu.VMEM((2, n_half, rows, COLS), f32),
            pltpu.VMEM((n_wd, rows, COLS), f32),
            pltpu.VMEM((rows, model), bf16),
            pltpu.VMEM((rows, units), bf16),
            pltpu.VMEM((n_wd, rows, COLS), f32),
            dma((2 * n_wd,)), dma((2, n_gu)),
            dma((3,)), dma((3,)),
            dma((2, n_half)), dma((2, n_half)),
            dma((2, n_half)), dma((2, n_half)),
            dma((2, n_half)), dma((2, n_half)),
        ],
        compiler_params=pltpu.CompilerParams(collective_id=0, has_side_effects=True, vmem_limit_bytes=54 << 20),
        name="tail",
    )(om, hidden, norm_mlp[None, :], w_out, w_gate_up, w_down)
    return out.astype(bf16)


def solution(mesh):
    cache_spec = P('dp', 'sp', 'tp', None)

    def local_step(hidden, positions, norm_attn, norm_mlp, w_qkv, w_out, w_gate_up, w_down, k_cache, v_cache):
        num_rows, block_len, kv_local, head_dim = k_cache.shape
        k_upd, v_upd, om = attend(positions, hidden, norm_attn, w_qkv, k_cache.transpose(0, 2, 3, 1), v_cache.transpose(0, 2, 3, 1))
        result = layer_tail(om, hidden, norm_mlp, w_out, w_gate_up, w_down, head_dim)
        return result, k_upd.transpose(0, 3, 1, 2), v_upd.transpose(0, 3, 1, 2)

    return jax.shard_map(local_step, mesh=mesh, in_specs=(P('dp', None), P('dp'), P(None), P(None), P(None, 'tp'), P('tp', None), P(None, 'tp'), P('tp', None), cache_spec, cache_spec), out_specs=(P('dp', None), cache_spec, cache_spec), check_vma=False)
```

```python
import functools
import math

import jax
import jax.numpy as jnp
from jax import lax
from jax.experimental import pallas as pl
from jax.experimental.pallas import tpu as pltpu
from jax.sharding import PartitionSpec as P

WINDOW = 2047
ROPE_BASE = 10000.0
NORM_EPS = 1e-5
NEG = -1e30
MESH = pl.DeviceIdType.MESH


QKV_COLS = 384
SLOTS = 7
PRE = 6


def project_kernel(dim, pos_hbm, hid_hbm, gain_hbm, w_hbm, k_hbm, v_hbm, rows_ref, k_ring, v_ring,
                   pos_ref, hid_ref, gain_ref, w_buf, normed_ref, qkv_t, turned, msg, gath,
                   w_sem, in_sem, side_sem, s_send, s_recv):
    sp = lax.axis_index('sp')
    rows, model = hid_ref.shape
    mine = qkv_t.shape[0]
    n_w = mine // QKV_COLS
    w_copies = []
    for i in range(n_w):
        first = pl.multiple_of(sp * mine + i * QKV_COLS, QKV_COLS)
        w_copies.append(pltpu.make_async_copy(w_hbm.at[:, pl.ds(first, QKV_COLS)], w_buf.at[i], w_sem.at[i]))
    side = [pltpu.make_async_copy(src, dst, side_sem.at[i]) for i, (src, dst) in enumerate(((hid_hbm, hid_ref), (gain_hbm, gain_ref), (pos_hbm, pos_ref)))]
    loads = []
    for b in range(PRE):
        loads.append(pltpu.make_async_copy(k_hbm.at[b], k_ring.at[b], in_sem.at[0, b]))
        loads.append(pltpu.make_async_copy(v_hbm.at[b], v_ring.at[b], in_sem.at[1, b]))
    for copy in side + w_copies + loads:
        copy.start()
    barrier = pltpu.get_barrier_semaphore()
    for step in range(1, 4):
        pl.semaphore_signal(barrier, inc=1, device_id={'sp': lax.rem(sp + step, 4)}, device_id_type=MESH)
    for copy in side:
        copy.wait()

    half = dim // 2
    lane = lax.broadcasted_iota(jnp.int32, (1, 128), 1)
    pos_row = jnp.zeros((1, 128), jnp.int32)
    for b in range(rows):
        pos_row = jnp.where(lane == b, pos_ref[b], pos_row)
    pair = lax.broadcasted_iota(jnp.int32, (half, 128), 0).astype(jnp.float32)
    angles = pos_row.astype(jnp.float32) * jnp.exp(pair * (-2.0 / dim * math.log(ROPE_BASE)))
    cos_t, sin_t = jnp.cos(angles), jnp.sin(angles)

    resid = hid_ref[...].astype(jnp.float32)
    inv = lax.rsqrt(jnp.sum(resid * resid, axis=1, keepdims=True) / model + NORM_EPS)
    normed_ref[...] = (resid * inv * gain_ref[...]).astype(jnp.bfloat16)
    pad = jnp.zeros((128 - rows, QKV_COLS), jnp.float32)
    for i in range(n_w):
        w_copies[i].wait()
        part = jnp.dot(normed_ref[...], w_buf[i], preferred_element_type=jnp.float32)
        qkv_t[i * QKV_COLS:(i + 1) * QKV_COLS, :] = jnp.concatenate([part, pad], axis=0).T
    third = mine // 3
    for h in range(third // dim):
        for part in range(2):
            first = (3 * h + part) * dim
            at = part * third + h * dim
            low, high = qkv_t[first:first + half, :], qkv_t[first + half:first + dim, :]
            turned[at:at + half, :] = low * cos_t - high * sin_t
            turned[at + half:at + dim, :] = high * cos_t + low * sin_t
        turned[2 * third + h * dim:2 * third + (h + 1) * dim, :] = qkv_t[(3 * h + 2) * dim:(3 * h + 3) * dim, :]
    own_rows = turned[...].T[:rows, :]
    msg[...] = own_rows
    pl.semaphore_wait(barrier, 3)
    sends = []
    for step in (2, 1, 3):
        copy = pltpu.make_async_remote_copy(src_ref=msg, dst_ref=gath.at[sp], send_sem=s_send.at[step - 1], recv_sem=s_recv.at[step - 1],
                                            device_id={'sp': lax.rem(sp + step, 4)}, device_id_type=MESH)
        copy.start()
        sends.append(copy)
    gath[sp] = own_rows
    for copy in sends:
        copy.wait_recv()
    rows_ref[...] = gath[...]
    for copy in loads:
        copy.wait()
    for copy in sends:
        copy.wait_send()


def project(positions, hidden, norm_attn, w_qkv, k_t, v_t):
    rows, heads, dim, block = k_t.shape
    model, mine = hidden.shape[1], w_qkv.shape[1] // 4
    vmem = pl.BlockSpec(memory_space=pltpu.VMEM)
    hbm = pl.BlockSpec(memory_space=pl.ANY)
    f32, bf16, dma = jnp.float32, jnp.bfloat16, pltpu.SemaphoreType.DMA
    return pl.pallas_call(
        functools.partial(project_kernel, dim),
        out_shape=(pltpu.VMEM((4, rows, mine), f32), pltpu.VMEM((SLOTS, heads, dim, block), bf16), pltpu.VMEM((SLOTS, heads, dim, block), bf16)),
        in_specs=[hbm] * 6,
        out_specs=(vmem, vmem, vmem),
        scratch_shapes=[
            pltpu.SMEM((rows,), jnp.int32),
            pltpu.VMEM((rows, model), bf16),
            pltpu.VMEM((1, model), f32),
            pltpu.VMEM((mine // QKV_COLS, model, QKV_COLS), bf16),
            pltpu.VMEM((rows, model), bf16),
            pltpu.VMEM((mine, 128), f32),
            pltpu.VMEM((mine, 128), f32),
            pltpu.VMEM((rows, mine), f32),
            pltpu.VMEM((4, rows, mine), f32),
            dma((mine // QKV_COLS,)), dma((2, PRE)), dma((3,)), dma((3,)), dma((3,)),
        ],
        compiler_params=pltpu.CompilerParams(collective_id=1, has_side_effects=True, vmem_limit_bytes=14 << 20),
        name="project",
    )(*(pltpu.with_memory_space_constraint(x, pltpu.HBM) for x in (positions, hidden, norm_attn[None, :])), w_qkv, k_t, v_t)


def attend_kernel(pos_hbm, rows_ref, k_in, v_in, k_hbm, v_hbm, ko_hbm, vo_hbm, om_ref, k_ring, v_ring,
                  pos_ref, new_t, in_sem, out_sem, side_sem):
    rows = rows_ref.shape[1]
    heads, dim, block = k_ring.shape[1:]
    width, third = heads * dim, rows_ref.shape[2] // 3
    base = lax.axis_index('sp') * block

    def load(b, which):
        slot = lax.rem(b, SLOTS)
        src, buf = ((k_hbm, k_ring), (v_hbm, v_ring))[which]
        return pltpu.make_async_copy(src.at[b], buf.at[slot], in_sem.at[which, slot])

    def store(b, which):
        slot = lax.rem(b, SLOTS)
        dst, buf = ((ko_hbm, k_ring), (vo_hbm, v_ring))[which]
        return pltpu.make_async_copy(buf.at[slot], dst.at[b], out_sem.at[which, slot])

    pos_copy = pltpu.make_async_copy(pos_hbm, pos_ref, side_sem)
    pos_copy.start()
    for b in range(PRE, SLOTS):
        load(b, 0).start()
        load(b, 1).start()
    pad = jnp.zeros((128 - rows, third), jnp.float32)
    for which in range(2):
        for s in range(4):
            entry = rows_ref[s, :, (1 + which) * third:(2 + which) * third]
            new_t[which, s * third:(s + 1) * third, :] = jnp.concatenate([entry, pad], axis=0).T
    pos_copy.wait()

    own = lax.broadcasted_iota(jnp.int32, (heads, width), 1) // dim == lax.broadcasted_iota(jnp.int32, (heads, width), 0)
    lane_ids = lax.broadcasted_iota(jnp.int32, (heads, 128), 1)
    head_ids = lax.broadcasted_iota(jnp.int32, (heads, 128), 0)
    half_heads, half_width = heads // 2, width // 2

    def patch(buf, slot, which, b, pos):
        at = pos - base

        @pl.when((at >= 0) & (at < block))
        def _():
            inner = lax.rem(at, 128)
            start = pl.multiple_of(at - inner, 128)
            shift = lax.rem(inner - b + 128, 128)
            hit = lax.broadcasted_iota(jnp.int32, (dim, 128), 1) == inner
            for h in range(heads):
                entry = pltpu.roll(new_t[which, h * dim:(h + 1) * dim, :], shift, 1)
                old = buf[slot, h, :, pl.ds(start, 128)].astype(jnp.float32)
                buf[slot, h, :, pl.ds(start, 128)] = jnp.where(hit, entry, old).astype(jnp.bfloat16)

    def step(b, carry):
        slot = lax.rem(b, SLOTS)
        pos = pos_ref[b]

        @pl.when((b >= 2) & (b + SLOTS - 2 < rows))
        def _():
            for which in range(2):
                store(b - 2, which).wait()
                load(b + SLOTS - 2, which).start()

        @pl.when(b >= PRE)
        def _():
            load(b, 0).wait()

        patch(k_ring, slot, 0, b, pos)
        store(b, 0).start()
        q_row = jnp.concatenate([rows_ref[s, pl.ds(b, 1), :third] for s in range(4)], axis=1)
        q_diag = jnp.where(own, jnp.broadcast_to(q_row, (heads, width)), 0.0).astype(jnp.bfloat16)
        scores = jnp.dot(q_diag, k_ring[slot].reshape(width, block), preferred_element_type=jnp.float32) * (dim ** -0.5)
        slot_ids = lax.broadcasted_iota(jnp.int32, (heads, block), 1) + base
        in_window = (slot_ids <= pos) & (slot_ids >= pos - WINDOW)
        scores = jnp.where(in_window, scores, NEG)
        row_max = jnp.max(scores, axis=1, keepdims=True)
        weights = jnp.where(in_window, jnp.exp(scores - row_max), 0.0)
        row_sum = jnp.sum(weights, axis=1, keepdims=True)

        @pl.when(b >= PRE)
        def _():
            load(b, 1).wait()

        patch(v_ring, slot, 1, b, pos)
        store(b, 1).start()
        acc = lax.dot_general(weights.astype(jnp.bfloat16), v_ring[slot].reshape(width, block), (((1,), (1,)), ((), ())), preferred_element_type=jnp.float32)
        o_row = jnp.sum(jnp.where(own, acc, 0.0), axis=0, keepdims=True)
        for core in range(2):
            local = head_ids - core * half_heads
            keep = (local >= 0) & (local < half_heads)
            stats = jnp.where(keep & (lane_ids == local), row_max, 0.0) + jnp.where(keep & (lane_ids == local + half_heads), row_sum, 0.0)
            row = jnp.concatenate([o_row[:, core * half_width:(core + 1) * half_width], jnp.sum(stats, axis=0, keepdims=True)], axis=1)
            at_row = lax.broadcasted_iota(jnp.int32, (rows, half_width + 128), 0) == b
            om_ref[core] = jnp.where(at_row, row, om_ref[core])
        return carry

    lax.fori_loop(0, rows, step, 0)
    for b in range(rows - SLOTS, rows):
        store(b, 0).wait()
        store(b, 1).wait()


def attend(positions, new_rows, k_ring, v_ring, k_t, v_t):
    rows, heads, dim, block = k_t.shape
    width = heads * dim
    vmem = pl.BlockSpec(memory_space=pltpu.VMEM)
    hbm = pl.BlockSpec(memory_space=pl.ANY)
    f32, bf16, dma = jnp.float32, jnp.bfloat16, pltpu.SemaphoreType.DMA
    ring = pltpu.VMEM((SLOTS, heads, dim, block), bf16)
    k_upd, v_upd, om, _, _ = pl.pallas_call(
        attend_kernel,
        out_shape=(jax.ShapeDtypeStruct(k_t.shape, k_t.dtype), jax.ShapeDtypeStruct(v_t.shape, v_t.dtype), pltpu.VMEM((2, rows, width // 2 + 128), f32), ring, ring),
        in_specs=[hbm, vmem, vmem, vmem, hbm, hbm],
        out_specs=(hbm, hbm, vmem, vmem, vmem),
        scratch_shapes=[
            pltpu.SMEM((rows,), jnp.int32),
            pltpu.VMEM((2, width, 128), f32),
            dma((2, SLOTS)), dma((2, SLOTS)), dma,
        ],
        input_output_aliases={2: 3, 3: 4},
        compiler_params=pltpu.CompilerParams(vmem_limit_bytes=10 << 20),
        name="attend",
    )(pltpu.with_memory_space_constraint(positions, pltpu.HBM), *(pltpu.with_memory_space_constraint(x, pltpu.VMEM) for x in (new_rows, k_ring, v_ring)), k_t, v_t)
    return k_upd, v_upd, om


COLS = 512


def tail_kernel(dim, om_ref, hid_hbm, gain_hbm, wo_hbm, wgu_hbm, wd_hbm, out_ref,
                hid_ref, gain_ref, obuf, wo, wg, wu, wd, o_cat, snd, own, got, ysnd, ygot, x1, r2, act, x2,
                side_sem, w_sem, gu_sem, o_send, o_recv, p_send, p_recv, y_send, y_recv, g_send, g_recv):
    tp, sp = lax.axis_index('tp'), lax.axis_index('sp')
    core = lax.rem(sp, 2)
    partner = sp + 1 - 2 * core
    rows = hid_ref.shape[0]
    half_width = wo.shape[1]
    n_half = x1.shape[0] // 2
    n_gu, n_wd = wg.shape[0], wd.shape[0]
    units = wd.shape[1]
    ffn = wgu_hbm.shape[1] // 2

    def column(index):
        side = 1 - core if index < n_half else core
        return pl.ds(pl.multiple_of((side * n_half + index % n_half) * COLS, COLS), COLS)

    weight_copies = []
    for i in range(n_wd):
        weight_copies.append(pltpu.make_async_copy(wo_hbm.at[pl.ds(core * half_width, half_width), column(i)], wo.at[i], w_sem.at[i]))
    gate_up_copies = []
    for i in range(n_gu):
        first = core * units + i * COLS
        gate_up_copies.append(pltpu.make_async_copy(wgu_hbm.at[:, pl.ds(pl.multiple_of(first, COLS), COLS)], wg.at[i], gu_sem.at[0, i]))
        gate_up_copies.append(pltpu.make_async_copy(wgu_hbm.at[:, pl.ds(pl.multiple_of(ffn + first, COLS), COLS)], wu.at[i], gu_sem.at[1, i]))
    down_copies = []
    for i in range(n_wd):
        down_copies.append(pltpu.make_async_copy(wd_hbm.at[pl.ds(core * units, units), column(i)], wd.at[i], w_sem.at[n_wd + i]))
    side = [pltpu.make_async_copy(hid_hbm, hid_ref, side_sem.at[0]), pltpu.make_async_copy(gain_hbm, gain_ref, side_sem.at[1])]
    for copy in weight_copies + side + gate_up_copies + down_copies:
        copy.start()

    barrier = pltpu.get_barrier_semaphore()
    for step in range(1, 4):
        pl.semaphore_signal(barrier, inc=1, device_id={'sp': lax.rem(sp + step, 4)}, device_id_type=MESH)
    pl.semaphore_signal(barrier, inc=1, device_id={'tp': 1 - tp}, device_id_type=MESH)
    pl.semaphore_wait(barrier, 4)

    sent = []

    def send(src, dst, send_sem, recv_sem, where):
        copy = pltpu.make_async_remote_copy(src_ref=src, dst_ref=dst, send_sem=send_sem, recv_sem=recv_sem, device_id=where, device_id_type=MESH)
        copy.start()
        sent.append(copy)
        return copy

    o_copies = []
    for step in (2, 1, 3):
        peer = lax.rem(sp + step, 4)
        o_copies.append(send(om_ref.at[lax.rem(peer, 2)], obuf.at[sp], o_send.at[step - 1], o_recv.at[step - 1], {'sp': peer}))
    obuf[sp] = om_ref[core]
    for copy in o_copies:
        copy.wait_recv()

    heads = half_width // dim
    stats = [obuf[s, :, half_width:] for s in range(4)]
    top = functools.reduce(jnp.maximum, stats)
    alphas = [jnp.exp(st - top) for st in stats]
    total = functools.reduce(lambda a, b: a + b, [al * pltpu.roll(st, 128 - heads, 1) for al, st in zip(alphas, stats)])
    betas = [al / total for al in alphas]
    lane = lax.broadcasted_iota(jnp.int32, (rows, 128), 1)
    for k in range(half_width // 128):
        first, last = 128 * k // dim, (128 * k + 127) // dim
        value = None
        for s in range(4):
            scale = jnp.broadcast_to(betas[s][:, first:first + 1], (rows, 128))
            for h in range(first + 1, last + 1):
                scale = jnp.where(lane >= h * dim - 128 * k, betas[s][:, h:h + 1], scale)
            term = scale * obuf[s, :, 128 * k:128 * (k + 1)]
            value = term if value is None else value + term
        o_cat[:, 128 * k:128 * (k + 1)] = value.astype(jnp.bfloat16)

    def reduce_and_spread(stage, lhs_ref, w_ref, w_waits, base_of, dst):
        lhs = lhs_ref[...]
        first = []
        for j in range(n_half):
            w_waits[j].wait()
            snd[stage, j] = jnp.dot(lhs, w_ref[j], preferred_element_type=jnp.float32)
            first.append(send(snd.at[stage, j], got.at[stage, j], p_send.at[stage, j], p_recv.at[stage, j], {'sp': partner}))
        for j in range(n_half):
            w_waits[n_half + j].wait()
            own[j] = jnp.dot(lhs, w_ref[n_half + j], preferred_element_type=jnp.float32)
        second = []
        for j in range(n_half):
            first[j].wait_recv()
            ysnd[stage, j] = (own[j] + got[stage, j]).astype(jnp.bfloat16).astype(jnp.float32)
            second.append(send(ysnd.at[stage, j], ygot.at[stage, j], y_send.at[stage, j], y_recv.at[stage, j], {'tp': 1 - tp}))
        third = []
        for j in range(n_half):
            second[j].wait_recv()
            dst[core * n_half + j] = base_of(j) + (ysnd[stage, j] + ygot[stage, j])
            third.append(send(dst.at[core * n_half + j], dst.at[core * n_half + j], g_send.at[stage, j], g_recv.at[stage, j], {'sp': partner}))
        for copy in third:
            copy.wait_recv()

    for copy in side:
        copy.wait()
    reduce_and_spread(0, o_cat, wo, weight_copies, lambda j: hid_ref[:, column(n_half + j)].astype(jnp.float32), x1)

    square = functools.reduce(lambda a, b: a + b, [x1[i] * x1[i] for i in range(2 * n_half)])
    inv = lax.rsqrt(jnp.sum(square, axis=1, keepdims=True) / (2 * n_half * COLS) + NORM_EPS)
    for i in range(2 * n_half):
        cut = slice(i * COLS, (i + 1) * COLS)
        r2[:, cut] = (x1[i] * inv * gain_ref[:, cut]).astype(jnp.bfloat16)

    for i in range(n_gu):
        gate_up_copies[2 * i].wait()
        gate_up_copies[2 * i + 1].wait()
        gate = jnp.dot(r2[...], wg[i], preferred_element_type=jnp.float32)
        up = jnp.dot(r2[...], wu[i], preferred_element_type=jnp.float32)
        act[:, i * COLS:(i + 1) * COLS] = (gate * jax.nn.sigmoid(gate) * up).astype(jnp.bfloat16)

    reduce_and_spread(1, act, wd, down_copies, lambda j: x1[core * n_half + j], x2)
    for i in range(2 * n_half):
        out_ref[:, i * COLS:(i + 1) * COLS] = x2[i]
    for copy in sent:
        copy.wait_send()


def layer_tail(om, hidden, norm_mlp, w_out, w_gate_up, w_down, dim):
    rows, model = hidden.shape
    half_width, units = w_out.shape[0] // 2, w_down.shape[0] // 2
    n_wd, n_gu = model // COLS, units // COLS
    n_half = n_wd // 2
    f32, bf16 = jnp.float32, jnp.bfloat16
    vmem = pl.BlockSpec(memory_space=pltpu.VMEM)
    hbm = pl.BlockSpec(memory_space=pl.ANY)
    dma = pltpu.SemaphoreType.DMA
    out = pl.pallas_call(
        functools.partial(tail_kernel, dim),
        out_shape=pltpu.VMEM((rows, model), f32),
        in_specs=[vmem, hbm, hbm, hbm, hbm, hbm],
        out_specs=vmem,
        scratch_shapes=[
            pltpu.VMEM((rows, model), bf16),
            pltpu.VMEM((1, model), f32),
            pltpu.VMEM((4, rows, half_width + 128), f32),
            pltpu.VMEM((n_wd, half_width, COLS), bf16),
            pltpu.VMEM((n_gu, model, COLS), bf16),
            pltpu.VMEM((n_gu, model, COLS), bf16),
            pltpu.VMEM((n_wd, units, COLS), bf16),
            pltpu.VMEM((rows, half_width), bf16),
            pltpu.VMEM((2, n_half, rows, COLS), f32),
            pltpu.VMEM((n_half, rows, COLS), f32),
            pltpu.VMEM((2, n_half, rows, COLS), f32),
            pltpu.VMEM((2, n_half, rows, COLS), f32),
            pltpu.VMEM((2, n_half, rows, COLS), f32),
            pltpu.VMEM((n_wd, rows, COLS), f32),
            pltpu.VMEM((rows, model), bf16),
            pltpu.VMEM((rows, units), bf16),
            pltpu.VMEM((n_wd, rows, COLS), f32),
            dma((2,)), dma((2 * n_wd,)), dma((2, n_gu)),
            dma((3,)), dma((3,)),
            dma((2, n_half)), dma((2, n_half)),
            dma((2, n_half)), dma((2, n_half)),
            dma((2, n_half)), dma((2, n_half)),
        ],
        compiler_params=pltpu.CompilerParams(collective_id=0, has_side_effects=True, vmem_limit_bytes=54 << 20),
        name="tail",
    )(pltpu.with_memory_space_constraint(om, pltpu.VMEM), *(pltpu.with_memory_space_constraint(x, pltpu.HBM) for x in (hidden, norm_mlp[None, :])), w_out, w_gate_up, w_down)
    return out.astype(bf16)


def solution(mesh):
    cache_spec = P('dp', 'sp', 'tp', None)

    def local_step(hidden, positions, norm_attn, norm_mlp, w_qkv, w_out, w_gate_up, w_down, k_cache, v_cache):
        num_rows, block_len, kv_local, head_dim = k_cache.shape
        k_t, v_t = k_cache.transpose(0, 2, 3, 1), v_cache.transpose(0, 2, 3, 1)
        new_rows, k_ring, v_ring = project(positions, hidden, norm_attn, w_qkv, k_t, v_t)
        k_upd, v_upd, om = attend(positions, new_rows, k_ring, v_ring, k_t, v_t)
        result = layer_tail(om, hidden, norm_mlp, w_out, w_gate_up, w_down, head_dim)
        return result, k_upd.transpose(0, 3, 1, 2), v_upd.transpose(0, 3, 1, 2)

    return jax.shard_map(local_step, mesh=mesh, in_specs=(P('dp', None), P('dp'), P(None), P(None), P(None, 'tp'), P('tp', None), P(None, 'tp'), P('tp', None), cache_spec, cache_spec), out_specs=(P('dp', None), cache_spec, cache_spec), check_vma=False)
```

```python
import functools
import math

import jax
import jax.numpy as jnp
from jax import lax
from jax.experimental import pallas as pl
from jax.experimental.pallas import tpu as pltpu
from jax.sharding import PartitionSpec as P

WINDOW = 2047
ROPE_BASE = 10000.0
NORM_EPS = 1e-5
NEG = -1e30
MESH = pl.DeviceIdType.MESH


QKV_COLS = 384
SLOTS = 7
PRE = 5


def project_kernel(dim, pos_hbm, hid_hbm, gain_hbm, w_hbm, k_hbm, v_hbm, rows_ref, k_ring, v_ring,
                   pos_ref, hid_ref, gain_ref, w_buf, normed_ref, qkv_t, turned, msg, gath,
                   w_sem, in_sem, side_sem, s_send, s_recv):
    sp = lax.axis_index('sp')
    rows, model = hid_ref.shape
    mine = qkv_t.shape[0]
    n_w = mine // QKV_COLS
    w_copies = []
    for i in range(n_w):
        first = pl.multiple_of(sp * mine + i * QKV_COLS, QKV_COLS)
        w_copies.append(pltpu.make_async_copy(w_hbm.at[:, pl.ds(first, QKV_COLS)], w_buf.at[i], w_sem.at[i]))
    side = [pltpu.make_async_copy(src, dst, side_sem.at[i]) for i, (src, dst) in enumerate(((hid_hbm, hid_ref), (gain_hbm, gain_ref), (pos_hbm, pos_ref)))]
    loads = []
    for b in range(PRE):
        loads.append(pltpu.make_async_copy(k_hbm.at[b], k_ring.at[b], in_sem.at[0, b]))
        loads.append(pltpu.make_async_copy(v_hbm.at[b], v_ring.at[b], in_sem.at[1, b]))
    for copy in side + w_copies:
        copy.start()
    barrier = pltpu.get_barrier_semaphore()
    for step in range(1, 4):
        pl.semaphore_signal(barrier, inc=1, device_id={'sp': lax.rem(sp + step, 4)}, device_id_type=MESH)
    for copy in side:
        copy.wait()

    half = dim // 2
    lane = lax.broadcasted_iota(jnp.int32, (1, 128), 1)
    pos_row = jnp.zeros((1, 128), jnp.int32)
    for b in range(rows):
        pos_row = jnp.where(lane == b, pos_ref[b], pos_row)
    pair = lax.broadcasted_iota(jnp.int32, (half, 128), 0).astype(jnp.float32)
    angles = pos_row.astype(jnp.float32) * jnp.exp(pair * (-2.0 / dim * math.log(ROPE_BASE)))
    cos_t, sin_t = jnp.cos(angles), jnp.sin(angles)

    resid = hid_ref[...].astype(jnp.float32)
    inv = lax.rsqrt(jnp.sum(resid * resid, axis=1, keepdims=True) / model + NORM_EPS)
    normed_ref[...] = (resid * inv * gain_ref[...]).astype(jnp.bfloat16)
    pad = jnp.zeros((128 - rows, QKV_COLS), jnp.float32)
    for i in range(n_w):
        w_copies[i].wait()
        for copy in loads[i * len(loads) // n_w:(i + 1) * len(loads) // n_w]:
            copy.start()
        part = jnp.dot(normed_ref[...], w_buf[i], preferred_element_type=jnp.float32)
        qkv_t[i * QKV_COLS:(i + 1) * QKV_COLS, :] = jnp.concatenate([part, pad], axis=0).T
    third = mine // 3
    for h in range(third // dim):
        for part in range(2):
            first = (3 * h + part) * dim
            at = part * third + h * dim
            low, high = qkv_t[first:first + half, :], qkv_t[first + half:first + dim, :]
            turned[at:at + half, :] = low * cos_t - high * sin_t
            turned[at + half:at + dim, :] = high * cos_t + low * sin_t
        turned[2 * third + h * dim:2 * third + (h + 1) * dim, :] = qkv_t[(3 * h + 2) * dim:(3 * h + 3) * dim, :]
    own_rows = turned[...].T[:rows, :]
    msg[...] = own_rows
    pl.semaphore_wait(barrier, 3)
    sends = []
    for step in (2, 1, 3):
        copy = pltpu.make_async_remote_copy(src_ref=msg, dst_ref=gath.at[sp], send_sem=s_send.at[step - 1], recv_sem=s_recv.at[step - 1],
                                            device_id={'sp': lax.rem(sp + step, 4)}, device_id_type=MESH)
        copy.start()
        sends.append(copy)
    gath[sp] = own_rows
    for copy in sends:
        copy.wait_recv()
    rows_ref[...] = gath[...]
    for copy in loads:
        copy.wait()
    for copy in sends:
        copy.wait_send()


def project(positions, hidden, norm_attn, w_qkv, k_t, v_t):
    rows, heads, dim, block = k_t.shape
    model, mine = hidden.shape[1], w_qkv.shape[1] // 4
    vmem = pl.BlockSpec(memory_space=pltpu.VMEM)
    hbm = pl.BlockSpec(memory_space=pl.ANY)
    f32, bf16, dma = jnp.float32, jnp.bfloat16, pltpu.SemaphoreType.DMA
    return pl.pallas_call(
        functools.partial(project_kernel, dim),
        out_shape=(pltpu.VMEM((4, rows, mine), f32), pltpu.VMEM((SLOTS, heads, dim, block), bf16), pltpu.VMEM((SLOTS, heads, dim, block), bf16)),
        in_specs=[hbm] * 6,
        out_specs=(vmem, vmem, vmem),
        scratch_shapes=[
            pltpu.SMEM((rows,), jnp.int32),
            pltpu.VMEM((rows, model), bf16),
            pltpu.VMEM((1, model), f32),
            pltpu.VMEM((mine // QKV_COLS, model, QKV_COLS), bf16),
            pltpu.VMEM((rows, model), bf16),
            pltpu.VMEM((mine, 128), f32),
            pltpu.VMEM((mine, 128), f32),
            pltpu.VMEM((rows, mine), f32),
            pltpu.VMEM((4, rows, mine), f32),
            dma((mine // QKV_COLS,)), dma((2, PRE)), dma((3,)), dma((3,)), dma((3,)),
        ],
        compiler_params=pltpu.CompilerParams(collective_id=1, has_side_effects=True, vmem_limit_bytes=14 << 20),
        name="project",
    )(*(pltpu.with_memory_space_constraint(x, pltpu.HBM) for x in (positions, hidden, norm_attn[None, :])), w_qkv, k_t, v_t)


def attend_kernel(pos_hbm, rows_ref, k_in, v_in, k_hbm, v_hbm, ko_hbm, vo_hbm, om_ref, k_ring, v_ring,
                  pos_ref, new_t, in_sem, out_sem, side_sem):
    rows = rows_ref.shape[1]
    heads, dim, block = k_ring.shape[1:]
    width, third = heads * dim, rows_ref.shape[2] // 3
    base = lax.axis_index('sp') * block

    def load(b, which):
        slot = lax.rem(b, SLOTS)
        src, buf = ((k_hbm, k_ring), (v_hbm, v_ring))[which]
        return pltpu.make_async_copy(src.at[b], buf.at[slot], in_sem.at[which, slot])

    def store(b, which):
        slot = lax.rem(b, SLOTS)
        dst, buf = ((ko_hbm, k_ring), (vo_hbm, v_ring))[which]
        return pltpu.make_async_copy(buf.at[slot], dst.at[b], out_sem.at[which, slot])

    pos_copy = pltpu.make_async_copy(pos_hbm, pos_ref, side_sem)
    pos_copy.start()
    for b in range(PRE, SLOTS):
        load(b, 0).start()
        load(b, 1).start()
    pad = jnp.zeros((128 - rows, third), jnp.float32)
    for which in range(2):
        for s in range(4):
            entry = rows_ref[s, :, (1 + which) * third:(2 + which) * third]
            new_t[which, s * third:(s + 1) * third, :] = jnp.concatenate([entry, pad], axis=0).T
    pos_copy.wait()

    own = lax.broadcasted_iota(jnp.int32, (heads, width), 1) // dim == lax.broadcasted_iota(jnp.int32, (heads, width), 0)
    lane_ids = lax.broadcasted_iota(jnp.int32, (heads, 128), 1)
    head_ids = lax.broadcasted_iota(jnp.int32, (heads, 128), 0)
    half_heads, half_width = heads // 2, width // 2

    def patch(buf, slot, which, b, pos):
        at = pos - base

        @pl.when((at >= 0) & (at < block))
        def _():
            inner = lax.rem(at, 128)
            start = pl.multiple_of(at - inner, 128)
            shift = lax.rem(inner - b + 128, 128)
            hit = lax.broadcasted_iota(jnp.int32, (dim, 128), 1) == inner
            for h in range(heads):
                entry = pltpu.roll(new_t[which, h * dim:(h + 1) * dim, :], shift, 1)
                old = buf[slot, h, :, pl.ds(start, 128)].astype(jnp.float32)
                buf[slot, h, :, pl.ds(start, 128)] = jnp.where(hit, entry, old).astype(jnp.bfloat16)

    def step(b, carry):
        slot = lax.rem(b, SLOTS)
        pos = pos_ref[b]

        @pl.when((b >= 2) & (b + SLOTS - 2 < rows))
        def _():
            for which in range(2):
                store(b - 2, which).wait()
                load(b + SLOTS - 2, which).start()

        @pl.when(b >= PRE)
        def _():
            load(b, 0).wait()

        patch(k_ring, slot, 0, b, pos)
        store(b, 0).start()
        q_row = jnp.concatenate([rows_ref[s, pl.ds(b, 1), :third] for s in range(4)], axis=1)
        q_diag = jnp.where(own, jnp.broadcast_to(q_row, (heads, width)), 0.0).astype(jnp.bfloat16)
        scores = jnp.dot(q_diag, k_ring[slot].reshape(width, block), preferred_element_type=jnp.float32) * (dim ** -0.5)
        slot_ids = lax.broadcasted_iota(jnp.int32, (heads, block), 1) + base
        in_window = (slot_ids <= pos) & (slot_ids >= pos - WINDOW)
        scores = jnp.where(in_window, scores, NEG)
        row_max = jnp.max(scores, axis=1, keepdims=True)
        weights = jnp.where(in_window, jnp.exp(scores - row_max), 0.0)
        row_sum = jnp.sum(weights, axis=1, keepdims=True)

        @pl.when(b >= PRE)
        def _():
            load(b, 1).wait()

        patch(v_ring, slot, 1, b, pos)
        store(b, 1).start()
        acc = lax.dot_general(weights.astype(jnp.bfloat16), v_ring[slot].reshape(width, block), (((1,), (1,)), ((), ())), preferred_element_type=jnp.float32)
        o_row = jnp.sum(jnp.where(own, acc, 0.0), axis=0, keepdims=True)
        for core in range(2):
            local = head_ids - core * half_heads
            keep = (local >= 0) & (local < half_heads)
            stats = jnp.where(keep & (lane_ids == local), row_max, 0.0) + jnp.where(keep & (lane_ids == local + half_heads), row_sum, 0.0)
            row = jnp.concatenate([o_row[:, core * half_width:(core + 1) * half_width], jnp.sum(stats, axis=0, keepdims=True)], axis=1)
            at_row = lax.broadcasted_iota(jnp.int32, (rows, half_width + 128), 0) == b
            om_ref[core] = jnp.where(at_row, row, om_ref[core])
        return carry

    lax.fori_loop(0, rows, step, 0)
    for b in range(rows - SLOTS, rows):
        store(b, 0).wait()
        store(b, 1).wait()


def attend(positions, new_rows, k_ring, v_ring, k_t, v_t):
    rows, heads, dim, block = k_t.shape
    width = heads * dim
    vmem = pl.BlockSpec(memory_space=pltpu.VMEM)
    hbm = pl.BlockSpec(memory_space=pl.ANY)
    f32, bf16, dma = jnp.float32, jnp.bfloat16, pltpu.SemaphoreType.DMA
    ring = pltpu.VMEM((SLOTS, heads, dim, block), bf16)
    k_upd, v_upd, om, _, _ = pl.pallas_call(
        attend_kernel,
        out_shape=(jax.ShapeDtypeStruct(k_t.shape, k_t.dtype), jax.ShapeDtypeStruct(v_t.shape, v_t.dtype), pltpu.VMEM((2, rows, width // 2 + 128), f32), ring, ring),
        in_specs=[hbm, vmem, vmem, vmem, hbm, hbm],
        out_specs=(hbm, hbm, vmem, vmem, vmem),
        scratch_shapes=[
            pltpu.SMEM((rows,), jnp.int32),
            pltpu.VMEM((2, width, 128), f32),
            dma((2, SLOTS)), dma((2, SLOTS)), dma,
        ],
        input_output_aliases={2: 3, 3: 4},
        compiler_params=pltpu.CompilerParams(vmem_limit_bytes=10 << 20),
        name="attend",
    )(pltpu.with_memory_space_constraint(positions, pltpu.HBM), *(pltpu.with_memory_space_constraint(x, pltpu.VMEM) for x in (new_rows, k_ring, v_ring)), k_t, v_t)
    return k_upd, v_upd, om


COLS = 512


def tail_kernel(dim, om_ref, hid_hbm, gain_hbm, wo_hbm, wgu_hbm, wd_hbm, out_ref,
                hid_ref, gain_ref, obuf, wo, wg, wu, wd, o_cat, snd, own, got, ysnd, ygot, x1, r2, act, x2,
                side_sem, w_sem, gu_sem, o_send, o_recv, p_send, p_recv, y_send, y_recv, g_send, g_recv):
    tp, sp = lax.axis_index('tp'), lax.axis_index('sp')
    core = lax.rem(sp, 2)
    partner = sp + 1 - 2 * core
    rows = hid_ref.shape[0]
    half_width = wo.shape[1]
    n_half = x1.shape[0] // 2
    n_gu, n_wd = wg.shape[0], wd.shape[0]
    units = wd.shape[1]
    ffn = wgu_hbm.shape[1] // 2

    def column(index):
        side = 1 - core if index < n_half else core
        return pl.ds(pl.multiple_of((side * n_half + index % n_half) * COLS, COLS), COLS)

    weight_copies = []
    for i in range(n_wd):
        weight_copies.append(pltpu.make_async_copy(wo_hbm.at[pl.ds(core * half_width, half_width), column(i)], wo.at[i], w_sem.at[i]))
    gate_up_copies = []
    for i in range(n_gu):
        first = core * units + i * COLS
        gate_up_copies.append(pltpu.make_async_copy(wgu_hbm.at[:, pl.ds(pl.multiple_of(first, COLS), COLS)], wg.at[i], gu_sem.at[0, i]))
        gate_up_copies.append(pltpu.make_async_copy(wgu_hbm.at[:, pl.ds(pl.multiple_of(ffn + first, COLS), COLS)], wu.at[i], gu_sem.at[1, i]))
    down_copies = []
    for i in range(n_wd):
        down_copies.append(pltpu.make_async_copy(wd_hbm.at[pl.ds(core * units, units), column(i)], wd.at[i], w_sem.at[n_wd + i]))
    side = [pltpu.make_async_copy(hid_hbm, hid_ref, side_sem.at[0]), pltpu.make_async_copy(gain_hbm, gain_ref, side_sem.at[1])]
    for copy in side + weight_copies:
        copy.start()

    barrier = pltpu.get_barrier_semaphore()
    for step in range(1, 4):
        pl.semaphore_signal(barrier, inc=1, device_id={'sp': lax.rem(sp + step, 4)}, device_id_type=MESH)
    pl.semaphore_signal(barrier, inc=1, device_id={'tp': 1 - tp}, device_id_type=MESH)
    pl.semaphore_wait(barrier, 4)

    sent = []

    def send(src, dst, send_sem, recv_sem, where):
        copy = pltpu.make_async_remote_copy(src_ref=src, dst_ref=dst, send_sem=send_sem, recv_sem=recv_sem, device_id=where, device_id_type=MESH)
        copy.start()
        sent.append(copy)
        return copy

    o_copies = []
    for step in (2, 1, 3):
        peer = lax.rem(sp + step, 4)
        o_copies.append(send(om_ref.at[lax.rem(peer, 2)], obuf.at[sp], o_send.at[step - 1], o_recv.at[step - 1], {'sp': peer}))
    obuf[sp] = om_ref[core]
    for copy in gate_up_copies:
        copy.start()
    for copy in o_copies:
        copy.wait_recv()
    for copy in down_copies:
        copy.start()

    heads = half_width // dim
    stats = [obuf[s, :, half_width:] for s in range(4)]
    top = functools.reduce(jnp.maximum, stats)
    alphas = [jnp.exp(st - top) for st in stats]
    total = functools.reduce(lambda a, b: a + b, [al * pltpu.roll(st, 128 - heads, 1) for al, st in zip(alphas, stats)])
    betas = [al / total for al in alphas]
    lane = lax.broadcasted_iota(jnp.int32, (rows, 128), 1)
    for k in range(half_width // 128):
        first, last = 128 * k // dim, (128 * k + 127) // dim
        value = None
        for s in range(4):
            scale = jnp.broadcast_to(betas[s][:, first:first + 1], (rows, 128))
            for h in range(first + 1, last + 1):
                scale = jnp.where(lane >= h * dim - 128 * k, betas[s][:, h:h + 1], scale)
            term = scale * obuf[s, :, 128 * k:128 * (k + 1)]
            value = term if value is None else value + term
        o_cat[:, 128 * k:128 * (k + 1)] = value.astype(jnp.bfloat16)

    def reduce_and_spread(stage, lhs_ref, w_ref, w_waits, base_of, dst):
        lhs = lhs_ref[...]
        first = []
        for j in range(n_half):
            w_waits[j].wait()
            snd[stage, j] = jnp.dot(lhs, w_ref[j], preferred_element_type=jnp.float32)
            first.append(send(snd.at[stage, j], got.at[stage, j], p_send.at[stage, j], p_recv.at[stage, j], {'sp': partner}))
        for j in range(n_half):
            w_waits[n_half + j].wait()
            own[j] = jnp.dot(lhs, w_ref[n_half + j], preferred_element_type=jnp.float32)
        second = []
        for j in range(n_half):
            first[j].wait_recv()
            ysnd[stage, j] = (own[j] + got[stage, j]).astype(jnp.bfloat16).astype(jnp.float32)
            second.append(send(ysnd.at[stage, j], ygot.at[stage, j], y_send.at[stage, j], y_recv.at[stage, j], {'tp': 1 - tp}))
        third = []
        for j in range(n_half):
            second[j].wait_recv()
            dst[core * n_half + j] = base_of(j) + (ysnd[stage, j] + ygot[stage, j])
            third.append(send(dst.at[core * n_half + j], dst.at[core * n_half + j], g_send.at[stage, j], g_recv.at[stage, j], {'sp': partner}))
        for copy in third:
            copy.wait_recv()

    for copy in side:
        copy.wait()
    reduce_and_spread(0, o_cat, wo, weight_copies, lambda j: hid_ref[:, column(n_half + j)].astype(jnp.float32), x1)

    square = functools.reduce(lambda a, b: a + b, [x1[i] * x1[i] for i in range(2 * n_half)])
    inv = lax.rsqrt(jnp.sum(square, axis=1, keepdims=True) / (2 * n_half * COLS) + NORM_EPS)
    for i in range(2 * n_half):
        cut = slice(i * COLS, (i + 1) * COLS)
        r2[:, cut] = (x1[i] * inv * gain_ref[:, cut]).astype(jnp.bfloat16)

    for i in range(n_gu):
        gate_up_copies[2 * i].wait()
        gate_up_copies[2 * i + 1].wait()
        gate = jnp.dot(r2[...], wg[i], preferred_element_type=jnp.float32)
        up = jnp.dot(r2[...], wu[i], preferred_element_type=jnp.float32)
        act[:, i * COLS:(i + 1) * COLS] = (gate * jax.nn.sigmoid(gate) * up).astype(jnp.bfloat16)

    reduce_and_spread(1, act, wd, down_copies, lambda j: x1[core * n_half + j], x2)
    for i in range(2 * n_half):
        out_ref[:, i * COLS:(i + 1) * COLS] = x2[i]
    for copy in sent:
        copy.wait_send()


def layer_tail(om, hidden, norm_mlp, w_out, w_gate_up, w_down, dim):
    rows, model = hidden.shape
    half_width, units = w_out.shape[0] // 2, w_down.shape[0] // 2
    n_wd, n_gu = model // COLS, units // COLS
    n_half = n_wd // 2
    f32, bf16 = jnp.float32, jnp.bfloat16
    vmem = pl.BlockSpec(memory_space=pltpu.VMEM)
    hbm = pl.BlockSpec(memory_space=pl.ANY)
    dma = pltpu.SemaphoreType.DMA
    out = pl.pallas_call(
        functools.partial(tail_kernel, dim),
        out_shape=pltpu.VMEM((rows, model), f32),
        in_specs=[vmem, hbm, hbm, hbm, hbm, hbm],
        out_specs=vmem,
        scratch_shapes=[
            pltpu.VMEM((rows, model), bf16),
            pltpu.VMEM((1, model), f32),
            pltpu.VMEM((4, rows, half_width + 128), f32),
            pltpu.VMEM((n_wd, half_width, COLS), bf16),
            pltpu.VMEM((n_gu, model, COLS), bf16),
            pltpu.VMEM((n_gu, model, COLS), bf16),
            pltpu.VMEM((n_wd, units, COLS), bf16),
            pltpu.VMEM((rows, half_width), bf16),
            pltpu.VMEM((2, n_half, rows, COLS), f32),
            pltpu.VMEM((n_half, rows, COLS), f32),
            pltpu.VMEM((2, n_half, rows, COLS), f32),
            pltpu.VMEM((2, n_half, rows, COLS), f32),
            pltpu.VMEM((2, n_half, rows, COLS), f32),
            pltpu.VMEM((n_wd, rows, COLS), f32),
            pltpu.VMEM((rows, model), bf16),
            pltpu.VMEM((rows, units), bf16),
            pltpu.VMEM((n_wd, rows, COLS), f32),
            dma((2,)), dma((2 * n_wd,)), dma((2, n_gu)),
            dma((3,)), dma((3,)),
            dma((2, n_half)), dma((2, n_half)),
            dma((2, n_half)), dma((2, n_half)),
            dma((2, n_half)), dma((2, n_half)),
        ],
        compiler_params=pltpu.CompilerParams(collective_id=0, has_side_effects=True, vmem_limit_bytes=54 << 20),
        name="tail",
    )(pltpu.with_memory_space_constraint(om, pltpu.VMEM), *(pltpu.with_memory_space_constraint(x, pltpu.HBM) for x in (hidden, norm_mlp[None, :])), w_out, w_gate_up, w_down)
    return out.astype(bf16)


def solution(mesh):
    cache_spec = P('dp', 'sp', 'tp', None)

    def local_step(hidden, positions, norm_attn, norm_mlp, w_qkv, w_out, w_gate_up, w_down, k_cache, v_cache):
        num_rows, block_len, kv_local, head_dim = k_cache.shape
        k_t, v_t = k_cache.transpose(0, 2, 3, 1), v_cache.transpose(0, 2, 3, 1)
        new_rows, k_ring, v_ring = project(positions, hidden, norm_attn, w_qkv, k_t, v_t)
        k_upd, v_upd, om = attend(positions, new_rows, k_ring, v_ring, k_t, v_t)
        result = layer_tail(om, hidden, norm_mlp, w_out, w_gate_up, w_down, head_dim)
        return result, k_upd.transpose(0, 3, 1, 2), v_upd.transpose(0, 3, 1, 2)

    return jax.shard_map(local_step, mesh=mesh, in_specs=(P('dp', None), P('dp'), P(None), P(None), P(None, 'tp'), P('tp', None), P(None, 'tp'), P('tp', None), cache_spec, cache_spec), out_specs=(P('dp', None), cache_spec, cache_spec), check_vma=False)
```

```python
import functools
import math

import jax
import jax.numpy as jnp
from jax import lax
from jax.experimental import pallas as pl
from jax.experimental.pallas import tpu as pltpu
from jax.sharding import PartitionSpec as P

WINDOW = 2047
ROPE_BASE = 10000.0
NORM_EPS = 1e-5
NEG = -1e30
MESH = pl.DeviceIdType.MESH


QKV_COLS = 384
SLOTS = 8
PRE = 5
DRAIN = 3


def project_kernel(dim, pos_hbm, hid_hbm, gain_hbm, w_hbm, k_hbm, v_hbm, rows_ref, k_ring, v_ring,
                   pos_ref, hid_ref, gain_ref, w_buf, normed_ref, qkv_t, turned, msg, gath,
                   w_sem, in_sem, side_sem, s_send, s_recv):
    sp = lax.axis_index('sp')
    rows, model = hid_ref.shape
    mine = qkv_t.shape[0]
    n_w = mine // QKV_COLS
    w_copies = []
    for i in range(n_w):
        first = pl.multiple_of(sp * mine + i * QKV_COLS, QKV_COLS)
        w_copies.append(pltpu.make_async_copy(w_hbm.at[:, pl.ds(first, QKV_COLS)], w_buf.at[i], w_sem.at[i]))
    side = [pltpu.make_async_copy(src, dst, side_sem.at[i]) for i, (src, dst) in enumerate(((hid_hbm, hid_ref), (gain_hbm, gain_ref), (pos_hbm, pos_ref)))]
    loads = []
    for b in range(PRE):
        loads.append(pltpu.make_async_copy(k_hbm.at[b], k_ring.at[b], in_sem.at[0, b]))
        loads.append(pltpu.make_async_copy(v_hbm.at[b], v_ring.at[b], in_sem.at[1, b]))
    for copy in side + w_copies:
        copy.start()
    barrier = pltpu.get_barrier_semaphore()
    for step in range(1, 4):
        pl.semaphore_signal(barrier, inc=1, device_id={'sp': lax.rem(sp + step, 4)}, device_id_type=MESH)
    for copy in side:
        copy.wait()

    half = dim // 2
    lane = lax.broadcasted_iota(jnp.int32, (1, 128), 1)
    pos_row = jnp.zeros((1, 128), jnp.int32)
    for b in range(rows):
        pos_row = jnp.where(lane == b, pos_ref[b], pos_row)
    pair = lax.broadcasted_iota(jnp.int32, (half, 128), 0).astype(jnp.float32)
    angles = pos_row.astype(jnp.float32) * jnp.exp(pair * (-2.0 / dim * math.log(ROPE_BASE)))
    cos_t, sin_t = jnp.cos(angles), jnp.sin(angles)

    resid = hid_ref[...].astype(jnp.float32)
    inv = lax.rsqrt(jnp.sum(resid * resid, axis=1, keepdims=True) / model + NORM_EPS)
    normed_ref[...] = (resid * inv * gain_ref[...]).astype(jnp.bfloat16)
    pad = jnp.zeros((128 - rows, QKV_COLS), jnp.float32)
    for i in range(n_w):
        w_copies[i].wait()
        for copy in loads[i * len(loads) // n_w:(i + 1) * len(loads) // n_w]:
            copy.start()
        part = jnp.dot(normed_ref[...], w_buf[i], preferred_element_type=jnp.float32)
        qkv_t[i * QKV_COLS:(i + 1) * QKV_COLS, :] = jnp.concatenate([part, pad], axis=0).T
    third = mine // 3
    for h in range(third // dim):
        for part in range(2):
            first = (3 * h + part) * dim
            at = part * third + h * dim
            low, high = qkv_t[first:first + half, :], qkv_t[first + half:first + dim, :]
            turned[at:at + half, :] = low * cos_t - high * sin_t
            turned[at + half:at + dim, :] = high * cos_t + low * sin_t
        turned[2 * third + h * dim:2 * third + (h + 1) * dim, :] = qkv_t[(3 * h + 2) * dim:(3 * h + 3) * dim, :]
    own_rows = turned[...].T[:rows, :]
    msg[...] = own_rows
    pl.semaphore_wait(barrier, 3)
    sends = []
    for step in (2, 1, 3):
        copy = pltpu.make_async_remote_copy(src_ref=msg, dst_ref=gath.at[sp], send_sem=s_send.at[step - 1], recv_sem=s_recv.at[step - 1],
                                            device_id={'sp': lax.rem(sp + step, 4)}, device_id_type=MESH)
        copy.start()
        sends.append(copy)
    gath[sp] = own_rows
    for copy in sends:
        copy.wait_recv()
    rows_ref[...] = gath[...]
    for copy in loads:
        copy.wait()
    for copy in sends:
        copy.wait_send()


def project(positions, hidden, norm_attn, w_qkv, k_t, v_t):
    rows, heads, dim, block = k_t.shape
    model, mine = hidden.shape[1], w_qkv.shape[1] // 4
    vmem = pl.BlockSpec(memory_space=pltpu.VMEM)
    hbm = pl.BlockSpec(memory_space=pl.ANY)
    f32, bf16, dma = jnp.float32, jnp.bfloat16, pltpu.SemaphoreType.DMA
    return pl.pallas_call(
        functools.partial(project_kernel, dim),
        out_shape=(pltpu.VMEM((4, rows, mine), f32), pltpu.VMEM((SLOTS, heads, dim, block), bf16), pltpu.VMEM((SLOTS, heads, dim, block), bf16)),
        in_specs=[hbm] * 6,
        out_specs=(vmem, vmem, vmem),
        scratch_shapes=[
            pltpu.SMEM((rows,), jnp.int32),
            pltpu.VMEM((rows, model), bf16),
            pltpu.VMEM((1, model), f32),
            pltpu.VMEM((mine // QKV_COLS, model, QKV_COLS), bf16),
            pltpu.VMEM((rows, model), bf16),
            pltpu.VMEM((mine, 128), f32),
            pltpu.VMEM((mine, 128), f32),
            pltpu.VMEM((rows, mine), f32),
            pltpu.VMEM((4, rows, mine), f32),
            dma((mine // QKV_COLS,)), dma((2, PRE)), dma((3,)), dma((3,)), dma((3,)),
        ],
        compiler_params=pltpu.CompilerParams(collective_id=1, has_side_effects=True, vmem_limit_bytes=9 << 20),
        name="project",
    )(*(pltpu.with_memory_space_constraint(x, pltpu.HBM) for x in (positions, hidden, norm_attn[None, :])), w_qkv, k_t, v_t)


def attend_kernel(pos_hbm, rows_ref, k_in, v_in, k_hbm, v_hbm, ko_hbm, vo_hbm, om_ref, k_ring, v_ring,
                  pos_ref, new_t, in_sem, out_sem, side_sem):
    rows = rows_ref.shape[1]
    heads, dim, block = k_ring.shape[1:]
    width, third = heads * dim, rows_ref.shape[2] // 3
    base = lax.axis_index('sp') * block

    def load(b, which):
        slot = lax.rem(b, SLOTS)
        src, buf = ((k_hbm, k_ring), (v_hbm, v_ring))[which]
        return pltpu.make_async_copy(src.at[b], buf.at[slot], in_sem.at[which, slot])

    def store(b, which):
        slot = lax.rem(b, SLOTS)
        dst, buf = ((ko_hbm, k_ring), (vo_hbm, v_ring))[which]
        return pltpu.make_async_copy(buf.at[slot], dst.at[b], out_sem.at[which, slot])

    pos_copy = pltpu.make_async_copy(pos_hbm, pos_ref, side_sem)
    pos_copy.start()
    for b in range(PRE, SLOTS):
        load(b, 0).start()
        load(b, 1).start()
    pad = jnp.zeros((128 - rows, third), jnp.float32)
    for which in range(2):
        for s in range(4):
            entry = rows_ref[s, :, (1 + which) * third:(2 + which) * third]
            new_t[which, s * third:(s + 1) * third, :] = jnp.concatenate([entry, pad], axis=0).T
    pos_copy.wait()

    own = lax.broadcasted_iota(jnp.int32, (heads, width), 1) // dim == lax.broadcasted_iota(jnp.int32, (heads, width), 0)
    lane_ids = lax.broadcasted_iota(jnp.int32, (heads, 128), 1)
    head_ids = lax.broadcasted_iota(jnp.int32, (heads, 128), 0)
    half_heads, half_width = heads // 2, width // 2

    def patch(buf, slot, which, b, pos):
        at = pos - base

        @pl.when((at >= 0) & (at < block))
        def _():
            inner = lax.rem(at, 128)
            start = pl.multiple_of(at - inner, 128)
            shift = lax.rem(inner - b + 128, 128)
            hit = lax.broadcasted_iota(jnp.int32, (dim, 128), 1) == inner
            for h in range(heads):
                entry = pltpu.roll(new_t[which, h * dim:(h + 1) * dim, :], shift, 1)
                old = buf[slot, h, :, pl.ds(start, 128)].astype(jnp.float32)
                buf[slot, h, :, pl.ds(start, 128)] = jnp.where(hit, entry, old).astype(jnp.bfloat16)

    def step(b, carry):
        slot = lax.rem(b, SLOTS)
        pos = pos_ref[b]

        @pl.when((b >= DRAIN) & (b + SLOTS - DRAIN < rows))
        def _():
            for which in range(2):
                store(b - DRAIN, which).wait()
                load(b + SLOTS - DRAIN, which).start()

        @pl.when(b >= PRE)
        def _():
            load(b, 0).wait()

        patch(k_ring, slot, 0, b, pos)
        store(b, 0).start()
        q_row = jnp.concatenate([rows_ref[s, pl.ds(b, 1), :third] for s in range(4)], axis=1)
        q_diag = jnp.where(own, jnp.broadcast_to(q_row, (heads, width)), 0.0).astype(jnp.bfloat16)
        scores = jnp.dot(q_diag, k_ring[slot].reshape(width, block), preferred_element_type=jnp.float32) * (dim ** -0.5)
        slot_ids = lax.broadcasted_iota(jnp.int32, (heads, block), 1) + base
        in_window = (slot_ids <= pos) & (slot_ids >= pos - WINDOW)
        scores = jnp.where(in_window, scores, NEG)
        row_max = jnp.max(scores, axis=1, keepdims=True)
        weights = jnp.where(in_window, jnp.exp(scores - row_max), 0.0)
        row_sum = jnp.sum(weights, axis=1, keepdims=True)

        @pl.when(b >= PRE)
        def _():
            load(b, 1).wait()

        patch(v_ring, slot, 1, b, pos)
        store(b, 1).start()
        acc = lax.dot_general(weights.astype(jnp.bfloat16), v_ring[slot].reshape(width, block), (((1,), (1,)), ((), ())), preferred_element_type=jnp.float32)
        o_row = jnp.sum(jnp.where(own, acc, 0.0), axis=0, keepdims=True)
        for core in range(2):
            local = head_ids - core * half_heads
            keep = (local >= 0) & (local < half_heads)
            stats = jnp.where(keep & (lane_ids == local), row_max, 0.0) + jnp.where(keep & (lane_ids == local + half_heads), row_sum, 0.0)
            row = jnp.concatenate([o_row[:, core * half_width:(core + 1) * half_width], jnp.sum(stats, axis=0, keepdims=True)], axis=1)
            at_row = lax.broadcasted_iota(jnp.int32, (rows, half_width + 128), 0) == b
            om_ref[core] = jnp.where(at_row, row, om_ref[core])
        return carry

    lax.fori_loop(0, rows, step, 0)
    for b in range(rows - SLOTS, rows):
        store(b, 0).wait()
        store(b, 1).wait()


def attend(positions, new_rows, k_ring, v_ring, k_t, v_t):
    rows, heads, dim, block = k_t.shape
    width = heads * dim
    vmem = pl.BlockSpec(memory_space=pltpu.VMEM)
    hbm = pl.BlockSpec(memory_space=pl.ANY)
    f32, bf16, dma = jnp.float32, jnp.bfloat16, pltpu.SemaphoreType.DMA
    ring = pltpu.VMEM((SLOTS, heads, dim, block), bf16)
    k_upd, v_upd, om, _, _ = pl.pallas_call(
        attend_kernel,
        out_shape=(jax.ShapeDtypeStruct(k_t.shape, k_t.dtype), jax.ShapeDtypeStruct(v_t.shape, v_t.dtype), pltpu.VMEM((2, rows, width // 2 + 128), f32), ring, ring),
        in_specs=[hbm, vmem, vmem, vmem, hbm, hbm],
        out_specs=(hbm, hbm, vmem, vmem, vmem),
        scratch_shapes=[
            pltpu.SMEM((rows,), jnp.int32),
            pltpu.VMEM((2, width, 128), f32),
            dma((2, SLOTS)), dma((2, SLOTS)), dma,
        ],
        input_output_aliases={2: 3, 3: 4},
        compiler_params=pltpu.CompilerParams(vmem_limit_bytes=6 << 20),
        name="attend",
    )(pltpu.with_memory_space_constraint(positions, pltpu.HBM), *(pltpu.with_memory_space_constraint(x, pltpu.VMEM) for x in (new_rows, k_ring, v_ring)), k_t, v_t)
    return k_upd, v_upd, om


COLS = 512


def tail_kernel(dim, om_ref, hid_hbm, gain_hbm, wo_hbm, wgu_hbm, wd_hbm, out_ref,
                hid_ref, gain_ref, obuf, wo, wg, wu, wd, o_cat, o_snd, o_got, acc, ysnd, ygot, x1, r2, act, a_snd, a_got, x2,
                side_sem, wo_sem, wd_sem, gu_sem, o_send, o_recv, p_send, p_recv, a_send, a_recv, y_send, y_recv, g_send, g_recv):
    tp, sp = lax.axis_index('tp'), lax.axis_index('sp')
    core = lax.rem(sp, 2)
    partner = sp + 1 - 2 * core
    rows = hid_ref.shape[0]
    half_width = wo.shape[2]
    n_half = x1.shape[0] // 2
    n_gu = wg.shape[0]
    units = wd.shape[2]
    ffn = wgu_hbm.shape[1] // 2

    def column(j):
        return pl.ds(pl.multiple_of((core * n_half + j) * COLS, COLS), COLS)

    side = [pltpu.make_async_copy(hid_hbm, hid_ref, side_sem.at[0]), pltpu.make_async_copy(gain_hbm, gain_ref, side_sem.at[1])]
    out_copies, down_copies, gate_up_copies = [[], []], [[], []], []
    for k, owner in enumerate((core, 1 - core)):
        for j in range(n_half):
            out_copies[k].append(pltpu.make_async_copy(wo_hbm.at[pl.ds(owner * half_width, half_width), column(j)], wo.at[k, j], wo_sem.at[k, j]))
            down_copies[k].append(pltpu.make_async_copy(wd_hbm.at[pl.ds(owner * units, units), column(j)], wd.at[k, j], wd_sem.at[k, j]))
    for i in range(n_gu):
        first = core * units + i * COLS
        gate_up_copies.append(pltpu.make_async_copy(wgu_hbm.at[:, pl.ds(pl.multiple_of(first, COLS), COLS)], wg.at[i], gu_sem.at[0, i]))
        gate_up_copies.append(pltpu.make_async_copy(wgu_hbm.at[:, pl.ds(pl.multiple_of(ffn + first, COLS), COLS)], wu.at[i], gu_sem.at[1, i]))
    barrier = pltpu.get_barrier_semaphore()
    for step in range(1, 4):
        pl.semaphore_signal(barrier, inc=1, device_id={'sp': lax.rem(sp + step, 4)}, device_id_type=MESH)
    pl.semaphore_signal(barrier, inc=1, device_id={'tp': 1 - tp}, device_id_type=MESH)
    for copy in side + out_copies[0] + out_copies[1]:
        copy.start()
    pl.semaphore_wait(barrier, 4)

    sent = []

    def send(src, dst, send_sem, recv_sem, where):
        copy = pltpu.make_async_remote_copy(src_ref=src, dst_ref=dst, send_sem=send_sem, recv_sem=recv_sem, device_id=where, device_id_type=MESH)
        copy.start()
        sent.append(copy)
        return copy

    first_copies = []
    for step in (2, 1, 3):
        peer = lax.rem(sp + step, 4)
        first_copies.append(send(om_ref.at[lax.rem(peer, 2)], obuf.at[sp], o_send.at[step - 1], o_recv.at[step - 1], {'sp': peer}))
    obuf[sp] = om_ref[core]
    for copy in gate_up_copies:
        copy.start()
    for copy in first_copies:
        copy.wait_recv()
    for copy in down_copies[0] + down_copies[1]:
        copy.start()

    heads = half_width // dim
    stats = [obuf[s, :, half_width:] for s in range(4)]
    top = functools.reduce(jnp.maximum, stats)
    alphas = [jnp.exp(st - top) for st in stats]
    total = functools.reduce(lambda a, b: a + b, [al * pltpu.roll(st, 128 - heads, 1) for al, st in zip(alphas, stats)])
    betas = [al / total for al in alphas]
    lane = lax.broadcasted_iota(jnp.int32, (rows, 128), 1)
    for k in range(half_width // 128):
        first, last = 128 * k // dim, (128 * k + 127) // dim
        value = None
        for s in range(4):
            scale = jnp.broadcast_to(betas[s][:, first:first + 1], (rows, 128))
            for h in range(first + 1, last + 1):
                scale = jnp.where(lane >= h * dim - 128 * k, betas[s][:, h:h + 1], scale)
            term = scale * obuf[s, :, 128 * k:128 * (k + 1)]
            value = term if value is None else value + term
        value = value.astype(jnp.bfloat16)
        o_cat[:, 128 * k:128 * (k + 1)] = value
        o_snd[:, 128 * k:128 * (k + 1)] = value.astype(jnp.float32)

    def product(lhs, w_ref, copies, j):
        copies[j].wait()
        return jnp.dot(lhs, w_ref[j], preferred_element_type=jnp.float32)

    def spread(stage, part_of, base_of, dst):
        second = []
        for j in range(n_half):
            ysnd[stage, j] = part_of(j).astype(jnp.bfloat16).astype(jnp.float32)
            second.append(send(ysnd.at[stage, j], ygot.at[stage, j], y_send.at[stage, j], y_recv.at[stage, j], {'tp': 1 - tp}))
        third = []
        for j in range(n_half):
            second[j].wait_recv()
            dst[core * n_half + j] = base_of(j) + (ysnd[stage, j] + ygot[stage, j])
            third.append(send(dst.at[core * n_half + j], dst.at[core * n_half + j], g_send.at[stage, j], g_recv.at[stage, j], {'sp': partner}))
        for copy in third:
            copy.wait_recv()

    o_copy = send(o_snd, o_got, p_send, p_recv, {'sp': partner})
    for j in range(n_half):
        acc[j] = product(o_cat[...], wo.at[0], out_copies[0], j)
    for copy in side:
        copy.wait()
    o_copy.wait_recv()
    o_other = o_got[...].astype(jnp.bfloat16)
    spread(0, lambda j: acc[j] + product(o_other, wo.at[1], out_copies[1], j), lambda j: hid_ref[:, column(j)].astype(jnp.float32), x1)

    square = functools.reduce(lambda a, b: a + b, [x1[i] * x1[i] for i in range(2 * n_half)])
    inv = lax.rsqrt(jnp.sum(square, axis=1, keepdims=True) / (2 * n_half * COLS) + NORM_EPS)
    for i in range(2 * n_half):
        cut = slice(i * COLS, (i + 1) * COLS)
        r2[:, cut] = (x1[i] * inv * gain_ref[:, cut]).astype(jnp.bfloat16)

    a_copies = []
    for i in range(n_gu):
        gate_up_copies[2 * i].wait()
        gate_up_copies[2 * i + 1].wait()
        gate = jnp.dot(r2[...], wg[i], preferred_element_type=jnp.float32)
        up = jnp.dot(r2[...], wu[i], preferred_element_type=jnp.float32)
        value = (gate * jax.nn.sigmoid(gate) * up).astype(jnp.bfloat16)
        act[0, :, i * COLS:(i + 1) * COLS] = value
        a_snd[i] = value.astype(jnp.float32)
        a_copies.append(send(a_snd.at[i], a_got.at[i], a_send.at[i], a_recv.at[i], {'sp': partner}))
    for j in range(n_half):
        acc[j] = product(act[0], wd.at[0], down_copies[0], j)
    for i in range(n_gu):
        a_copies[i].wait_recv()
        act[1, :, i * COLS:(i + 1) * COLS] = a_got[i].astype(jnp.bfloat16)
    spread(1, lambda j: acc[j] + product(act[1], wd.at[1], down_copies[1], j), lambda j: x1[core * n_half + j], x2)
    for i in range(2 * n_half):
        out_ref[:, i * COLS:(i + 1) * COLS] = x2[i]
    for copy in sent:
        copy.wait_send()


def layer_tail(om, hidden, norm_mlp, w_out, w_gate_up, w_down, dim):
    rows, model = hidden.shape
    half_width, units = w_out.shape[0] // 2, w_down.shape[0] // 2
    n_wd, n_gu = model // COLS, units // COLS
    n_half = n_wd // 2
    f32, bf16 = jnp.float32, jnp.bfloat16
    vmem = pl.BlockSpec(memory_space=pltpu.VMEM)
    hbm = pl.BlockSpec(memory_space=pl.ANY)
    dma = pltpu.SemaphoreType.DMA
    out = pl.pallas_call(
        functools.partial(tail_kernel, dim),
        out_shape=pltpu.VMEM((rows, model), f32),
        in_specs=[vmem, hbm, hbm, hbm, hbm, hbm],
        out_specs=vmem,
        scratch_shapes=[
            pltpu.VMEM((rows, model), bf16),
            pltpu.VMEM((1, model), f32),
            pltpu.VMEM((4, rows, half_width + 128), f32),
            pltpu.VMEM((2, n_half, half_width, COLS), bf16),
            pltpu.VMEM((n_gu, model, COLS), bf16),
            pltpu.VMEM((n_gu, model, COLS), bf16),
            pltpu.VMEM((2, n_half, units, COLS), bf16),
            pltpu.VMEM((rows, half_width), bf16),
            pltpu.VMEM((rows, half_width), f32),
            pltpu.VMEM((rows, half_width), f32),
            pltpu.VMEM((n_half, rows, COLS), f32),
            pltpu.VMEM((2, n_half, rows, COLS), f32),
            pltpu.VMEM((2, n_half, rows, COLS), f32),
            pltpu.VMEM((n_wd, rows, COLS), f32),
            pltpu.VMEM((rows, model), bf16),
            pltpu.VMEM((2, rows, units), bf16),
            pltpu.VMEM((n_gu, rows, COLS), f32),
            pltpu.VMEM((n_gu, rows, COLS), f32),
            pltpu.VMEM((n_wd, rows, COLS), f32),
            dma((2,)), dma((2, n_half)), dma((2, n_half)), dma((2, n_gu)),
            dma((3,)), dma((3,)),
            dma, dma,
            dma((n_gu,)), dma((n_gu,)),
            dma((2, n_half)), dma((2, n_half)),
            dma((2, n_half)), dma((2, n_half)),
        ],
        compiler_params=pltpu.CompilerParams(collective_id=0, has_side_effects=True, vmem_limit_bytes=54 << 20),
        name="tail",
    )(pltpu.with_memory_space_constraint(om, pltpu.VMEM), *(pltpu.with_memory_space_constraint(x, pltpu.HBM) for x in (hidden, norm_mlp[None, :])), w_out, w_gate_up, w_down)
    return out.astype(bf16)


def solution(mesh):
    cache_spec = P('dp', 'sp', 'tp', None)

    def local_step(hidden, positions, norm_attn, norm_mlp, w_qkv, w_out, w_gate_up, w_down, k_cache, v_cache):
        num_rows, block_len, kv_local, head_dim = k_cache.shape
        k_t, v_t = k_cache.transpose(0, 2, 3, 1), v_cache.transpose(0, 2, 3, 1)
        new_rows, k_ring, v_ring = project(positions, hidden, norm_attn, w_qkv, k_t, v_t)
        k_upd, v_upd, om = attend(positions, new_rows, k_ring, v_ring, k_t, v_t)
        result = layer_tail(om, hidden, norm_mlp, w_out, w_gate_up, w_down, head_dim)
        return result, k_upd.transpose(0, 3, 1, 2), v_upd.transpose(0, 3, 1, 2)

    return jax.shard_map(local_step, mesh=mesh, in_specs=(P('dp', None), P('dp'), P(None), P(None), P(None, 'tp'), P('tp', None), P(None, 'tp'), P('tp', None), cache_spec, cache_spec), out_specs=(P('dp', None), cache_spec, cache_spec), check_vma=False)
```

```python
import functools
import math

import jax
import jax.numpy as jnp
from jax import lax
from jax.experimental import pallas as pl
from jax.experimental.pallas import tpu as pltpu
from jax.sharding import PartitionSpec as P

WINDOW = 2047
ROPE_BASE = 10000.0
NORM_EPS = 1e-5
NEG = -1e30
MESH = pl.DeviceIdType.MESH


QKV_COLS = 384
SLOTS = 8
PRE = 7
DRAIN = 3


def project_kernel(dim, pos_hbm, hid_hbm, gain_hbm, w_hbm, k_hbm, v_hbm, q_ref, new_t, k_ring, v_ring,
                   pos_ref, hid_ref, gain_ref, w_buf, normed_ref, qkv_t, turned, msg, gath,
                   w_sem, in_sem, side_sem, s_send, s_recv):
    sp = lax.axis_index('sp')
    rows, model = hid_ref.shape
    mine = qkv_t.shape[0]
    n_w = mine // QKV_COLS
    w_copies = []
    for i in range(n_w):
        first = pl.multiple_of(sp * mine + i * QKV_COLS, QKV_COLS)
        w_copies.append(pltpu.make_async_copy(w_hbm.at[:, pl.ds(first, QKV_COLS)], w_buf.at[i], w_sem.at[i]))
    side = [pltpu.make_async_copy(src, dst, side_sem.at[i]) for i, (src, dst) in enumerate(((hid_hbm, hid_ref), (gain_hbm, gain_ref), (pos_hbm, pos_ref)))]
    loads = []
    for b in range(PRE):
        loads.append(pltpu.make_async_copy(k_hbm.at[b], k_ring.at[b], in_sem.at[0, b]))
        loads.append(pltpu.make_async_copy(v_hbm.at[b], v_ring.at[b], in_sem.at[1, b]))
    for copy in side + w_copies:
        copy.start()
    barrier = pltpu.get_barrier_semaphore()
    for step in range(1, 4):
        pl.semaphore_signal(barrier, inc=1, device_id={'sp': lax.rem(sp + step, 4)}, device_id_type=MESH)
    for copy in side:
        copy.wait()

    half = dim // 2
    lane = lax.broadcasted_iota(jnp.int32, (1, 128), 1)
    pos_row = jnp.zeros((1, 128), jnp.int32)
    for b in range(rows):
        pos_row = jnp.where(lane == b, pos_ref[b], pos_row)
    pair = lax.broadcasted_iota(jnp.int32, (half, 128), 0).astype(jnp.float32)
    angles = pos_row.astype(jnp.float32) * jnp.exp(pair * (-2.0 / dim * math.log(ROPE_BASE)))
    cos_t, sin_t = jnp.cos(angles), jnp.sin(angles)

    resid = hid_ref[...].astype(jnp.float32)
    inv = lax.rsqrt(jnp.sum(resid * resid, axis=1, keepdims=True) / model + NORM_EPS)
    normed_ref[...] = (resid * inv * gain_ref[...]).astype(jnp.bfloat16)
    pad = jnp.zeros((128 - rows, QKV_COLS), jnp.float32)
    for i in range(n_w):
        w_copies[i].wait()
        for copy in loads[i * len(loads) // n_w:(i + 1) * len(loads) // n_w]:
            copy.start()
        part = jnp.dot(normed_ref[...], w_buf[i], preferred_element_type=jnp.float32)
        qkv_t[i * QKV_COLS:(i + 1) * QKV_COLS, :] = jnp.concatenate([part, pad], axis=0).T
    third = mine // 3
    for h in range(third // dim):
        for part in range(2):
            first = (3 * h + part) * dim
            at = part * third + h * dim
            low, high = qkv_t[first:first + half, :], qkv_t[first + half:first + dim, :]
            turned[at:at + half, :] = low * cos_t - high * sin_t
            turned[at + half:at + dim, :] = high * cos_t + low * sin_t
        turned[2 * third + h * dim:2 * third + (h + 1) * dim, :] = qkv_t[(3 * h + 2) * dim:(3 * h + 3) * dim, :]
    own_rows = turned[...].T[:rows, :]
    msg[...] = own_rows
    pl.semaphore_wait(barrier, 3)
    sends = []
    for step in (2, 1, 3):
        copy = pltpu.make_async_remote_copy(src_ref=msg, dst_ref=gath.at[sp], send_sem=s_send.at[step - 1], recv_sem=s_recv.at[step - 1],
                                            device_id={'sp': lax.rem(sp + step, 4)}, device_id_type=MESH)
        copy.start()
        sends.append(copy)
    gath[sp] = own_rows
    for copy in sends:
        copy.wait_recv()
    q_ref[...] = gath[:, :, :third]
    pad = jnp.zeros((128 - rows, third), jnp.float32)
    for which in range(2):
        for s in range(4):
            entry = gath[s, :, (1 + which) * third:(2 + which) * third]
            new_t[which, s * third:(s + 1) * third, :] = jnp.concatenate([entry, pad], axis=0).T
    for copy in loads:
        copy.wait()
    for copy in sends:
        copy.wait_send()


def project(positions, hidden, norm_attn, w_qkv, k_t, v_t):
    rows, heads, dim, block = k_t.shape
    model, mine = hidden.shape[1], w_qkv.shape[1] // 4
    vmem = pl.BlockSpec(memory_space=pltpu.VMEM)
    hbm = pl.BlockSpec(memory_space=pl.ANY)
    f32, bf16, dma = jnp.float32, jnp.bfloat16, pltpu.SemaphoreType.DMA
    return pl.pallas_call(
        functools.partial(project_kernel, dim),
        out_shape=(pltpu.VMEM((4, rows, mine // 3), f32), pltpu.VMEM((2, heads * dim, 128), f32), pltpu.VMEM((SLOTS, heads, dim, block), bf16), pltpu.VMEM((SLOTS, heads, dim, block), bf16)),
        in_specs=[hbm] * 6,
        out_specs=(vmem, vmem, vmem, vmem),
        scratch_shapes=[
            pltpu.SMEM((rows,), jnp.int32),
            pltpu.VMEM((rows, model), bf16),
            pltpu.VMEM((1, model), f32),
            pltpu.VMEM((mine // QKV_COLS, model, QKV_COLS), bf16),
            pltpu.VMEM((rows, model), bf16),
            pltpu.VMEM((mine, 128), f32),
            pltpu.VMEM((mine, 128), f32),
            pltpu.VMEM((rows, mine), f32),
            pltpu.VMEM((4, rows, mine), f32),
            dma((mine // QKV_COLS,)), dma((2, PRE)), dma((3,)), dma((3,)), dma((3,)),
        ],
        compiler_params=pltpu.CompilerParams(collective_id=1, has_side_effects=True, vmem_limit_bytes=8200 << 10),
        name="project",
    )(*(pltpu.with_memory_space_constraint(x, pltpu.HBM) for x in (positions, hidden, norm_attn[None, :])), w_qkv, k_t, v_t)


def attend_kernel(pos_hbm, q_ref, new_t, k_in, v_in, k_hbm, v_hbm, ko_hbm, vo_hbm, om_ref, k_ring, v_ring,
                  pos_ref, in_sem, out_sem, side_sem):
    rows, third = q_ref.shape[1:]
    heads, dim, block = k_ring.shape[1:]
    width = heads * dim
    base = lax.axis_index('sp') * block

    def load(b, which):
        slot = lax.rem(b, SLOTS)
        src, buf = ((k_hbm, k_ring), (v_hbm, v_ring))[which]
        return pltpu.make_async_copy(src.at[b], buf.at[slot], in_sem.at[which, slot])

    def store(b, which):
        slot = lax.rem(b, SLOTS)
        dst, buf = ((ko_hbm, k_ring), (vo_hbm, v_ring))[which]
        return pltpu.make_async_copy(buf.at[slot], dst.at[b], out_sem.at[which, slot])

    pos_copy = pltpu.make_async_copy(pos_hbm, pos_ref, side_sem)
    pos_copy.start()
    for b in range(PRE, SLOTS):
        load(b, 0).start()
        load(b, 1).start()
    pos_copy.wait()

    own = lax.broadcasted_iota(jnp.int32, (heads, width), 1) // dim == lax.broadcasted_iota(jnp.int32, (heads, width), 0)
    lane_ids = lax.broadcasted_iota(jnp.int32, (heads, 128), 1)
    head_ids = lax.broadcasted_iota(jnp.int32, (heads, 128), 0)
    half_heads, half_width = heads // 2, width // 2

    def patch(buf, slot, which, b, pos):
        at = pos - base

        @pl.when((at >= 0) & (at < block))
        def _():
            inner = lax.rem(at, 128)
            start = pl.multiple_of(at - inner, 128)
            shift = lax.rem(inner - b + 128, 128)
            hit = lax.broadcasted_iota(jnp.int32, (dim, 128), 1) == inner
            for h in range(heads):
                entry = pltpu.roll(new_t[which, h * dim:(h + 1) * dim, :], shift, 1)
                old = buf[slot, h, :, pl.ds(start, 128)].astype(jnp.float32)
                buf[slot, h, :, pl.ds(start, 128)] = jnp.where(hit, entry, old).astype(jnp.bfloat16)

    def step(b, carry):
        slot = lax.rem(b, SLOTS)
        pos = pos_ref[b]

        @pl.when((b >= DRAIN) & (b + SLOTS - DRAIN < rows))
        def _():
            for which in range(2):
                store(b - DRAIN, which).wait()
                load(b + SLOTS - DRAIN, which).start()

        @pl.when(b >= PRE)
        def _():
            load(b, 0).wait()

        patch(k_ring, slot, 0, b, pos)
        store(b, 0).start()
        q_row = jnp.concatenate([q_ref[s, pl.ds(b, 1), :] for s in range(4)], axis=1)
        q_diag = jnp.where(own, jnp.broadcast_to(q_row, (heads, width)), 0.0).astype(jnp.bfloat16)
        scores = jnp.dot(q_diag, k_ring[slot].reshape(width, block), preferred_element_type=jnp.float32) * (dim ** -0.5)
        slot_ids = lax.broadcasted_iota(jnp.int32, (heads, block), 1) + base
        in_window = (slot_ids <= pos) & (slot_ids >= pos - WINDOW)
        scores = jnp.where(in_window, scores, NEG)
        row_max = jnp.max(scores, axis=1, keepdims=True)
        weights = jnp.where(in_window, jnp.exp(scores - row_max), 0.0)
        row_sum = jnp.sum(weights, axis=1, keepdims=True)

        @pl.when(b >= PRE)
        def _():
            load(b, 1).wait()

        patch(v_ring, slot, 1, b, pos)
        store(b, 1).start()
        acc = lax.dot_general(weights.astype(jnp.bfloat16), v_ring[slot].reshape(width, block), (((1,), (1,)), ((), ())), preferred_element_type=jnp.float32)
        o_row = jnp.sum(jnp.where(own, acc, 0.0), axis=0, keepdims=True)
        for core in range(2):
            local = head_ids - core * half_heads
            keep = (local >= 0) & (local < half_heads)
            stats = jnp.where(keep & (lane_ids == local), row_max, 0.0) + jnp.where(keep & (lane_ids == local + half_heads), row_sum, 0.0)
            row = jnp.concatenate([o_row[:, core * half_width:(core + 1) * half_width], jnp.sum(stats, axis=0, keepdims=True)], axis=1)
            at_row = lax.broadcasted_iota(jnp.int32, (rows, half_width + 128), 0) == b
            om_ref[core] = jnp.where(at_row, row, om_ref[core])
        return carry

    lax.fori_loop(0, rows, step, 0)
    for b in range(rows - SLOTS, rows):
        store(b, 0).wait()
        store(b, 1).wait()


def attend(positions, q_rows, new_t, k_ring, v_ring, k_t, v_t):
    rows, heads, dim, block = k_t.shape
    width = heads * dim
    vmem = pl.BlockSpec(memory_space=pltpu.VMEM)
    hbm = pl.BlockSpec(memory_space=pl.ANY)
    f32, bf16, dma = jnp.float32, jnp.bfloat16, pltpu.SemaphoreType.DMA
    ring = pltpu.VMEM((SLOTS, heads, dim, block), bf16)
    k_upd, v_upd, om, _, _ = pl.pallas_call(
        attend_kernel,
        out_shape=(jax.ShapeDtypeStruct(k_t.shape, k_t.dtype), jax.ShapeDtypeStruct(v_t.shape, v_t.dtype), pltpu.VMEM((2, rows, width // 2 + 128), f32), ring, ring),
        in_specs=[hbm, vmem, vmem, vmem, vmem, hbm, hbm],
        out_specs=(hbm, hbm, vmem, vmem, vmem),
        scratch_shapes=[
            pltpu.SMEM((rows,), jnp.int32),
            dma((2, SLOTS)), dma((2, SLOTS)), dma,
        ],
        input_output_aliases={3: 3, 4: 4},
        compiler_params=pltpu.CompilerParams(vmem_limit_bytes=5 << 20),
        name="attend",
    )(pltpu.with_memory_space_constraint(positions, pltpu.HBM), *(pltpu.with_memory_space_constraint(x, pltpu.VMEM) for x in (q_rows, new_t, k_ring, v_ring)), k_t, v_t)
    return k_upd, v_upd, om


COLS = 512


def tail_kernel(dim, om_ref, hid_hbm, gain_hbm, wo_hbm, wgu_hbm, wd_hbm, out_ref,
                hid_ref, gain_ref, obuf, wo, wg, wu, wd, o_cat, o_snd, o_got, acc, ysnd, ygot, x1, r2, act, a_snd, a_got, x2,
                side_sem, wo_sem, wd_sem, gu_sem, o_send, o_recv, p_send, p_recv, a_send, a_recv, y_send, y_recv, g_send, g_recv):
    tp, sp = lax.axis_index('tp'), lax.axis_index('sp')
    core = lax.rem(sp, 2)
    partner = sp + 1 - 2 * core
    rows = hid_ref.shape[0]
    half_width = wo.shape[2]
    n_half = x1.shape[0] // 2
    n_gu = wg.shape[0]
    units = wd.shape[2]
    ffn = wgu_hbm.shape[1] // 2

    def column(j):
        return pl.ds(pl.multiple_of((core * n_half + j) * COLS, COLS), COLS)

    side = [pltpu.make_async_copy(hid_hbm, hid_ref, side_sem.at[0]), pltpu.make_async_copy(gain_hbm, gain_ref, side_sem.at[1])]
    out_copies, down_copies, gate_up_copies = [[], []], [[], []], []
    for k, owner in enumerate((core, 1 - core)):
        for j in range(n_half):
            out_copies[k].append(pltpu.make_async_copy(wo_hbm.at[pl.ds(owner * half_width, half_width), column(j)], wo.at[k, j], wo_sem.at[k, j]))
            down_copies[k].append(pltpu.make_async_copy(wd_hbm.at[pl.ds(owner * units, units), column(j)], wd.at[k, j], wd_sem.at[k, j]))
    for i in range(n_gu):
        first = core * units + i * COLS
        gate_up_copies.append(pltpu.make_async_copy(wgu_hbm.at[:, pl.ds(pl.multiple_of(first, COLS), COLS)], wg.at[i], gu_sem.at[0, i]))
        gate_up_copies.append(pltpu.make_async_copy(wgu_hbm.at[:, pl.ds(pl.multiple_of(ffn + first, COLS), COLS)], wu.at[i], gu_sem.at[1, i]))
    barrier = pltpu.get_barrier_semaphore()
    for step in range(1, 4):
        pl.semaphore_signal(barrier, inc=1, device_id={'sp': lax.rem(sp + step, 4)}, device_id_type=MESH)
    pl.semaphore_signal(barrier, inc=1, device_id={'tp': 1 - tp}, device_id_type=MESH)
    for copy in side + out_copies[0] + out_copies[1]:
        copy.start()
    pl.semaphore_wait(barrier, 4)

    sent = []

    def send(src, dst, send_sem, recv_sem, where):
        copy = pltpu.make_async_remote_copy(src_ref=src, dst_ref=dst, send_sem=send_sem, recv_sem=recv_sem, device_id=where, device_id_type=MESH)
        copy.start()
        sent.append(copy)
        return copy

    first_copies = []
    for step in (2, 1, 3):
        peer = lax.rem(sp + step, 4)
        first_copies.append(send(om_ref.at[lax.rem(peer, 2)], obuf.at[sp], o_send.at[step - 1], o_recv.at[step - 1], {'sp': peer}))
    obuf[sp] = om_ref[core]
    for copy in gate_up_copies:
        copy.start()
    for copy in first_copies:
        copy.wait_recv()
    for copy in down_copies[0] + down_copies[1]:
        copy.start()

    heads = half_width // dim
    stats = [obuf[s, :, half_width:] for s in range(4)]
    top = functools.reduce(jnp.maximum, stats)
    alphas = [jnp.exp(st - top) for st in stats]
    total = functools.reduce(lambda a, b: a + b, [al * pltpu.roll(st, 128 - heads, 1) for al, st in zip(alphas, stats)])
    betas = [al / total for al in alphas]
    lane = lax.broadcasted_iota(jnp.int32, (rows, 128), 1)
    for k in range(half_width // 128):
        first, last = 128 * k // dim, (128 * k + 127) // dim
        value = None
        for s in range(4):
            scale = jnp.broadcast_to(betas[s][:, first:first + 1], (rows, 128))
            for h in range(first + 1, last + 1):
                scale = jnp.where(lane >= h * dim - 128 * k, betas[s][:, h:h + 1], scale)
            term = scale * obuf[s, :, 128 * k:128 * (k + 1)]
            value = term if value is None else value + term
        value = value.astype(jnp.bfloat16)
        o_cat[:, 128 * k:128 * (k + 1)] = value
        o_snd[:, 128 * k:128 * (k + 1)] = value.astype(jnp.float32)

    def product(lhs, w_ref, copies, j):
        copies[j].wait()
        return jnp.dot(lhs, w_ref[j], preferred_element_type=jnp.float32)

    def spread(stage, part_of, base_of, dst):
        second = []
        for j in range(n_half):
            ysnd[stage, j] = part_of(j).astype(jnp.bfloat16).astype(jnp.float32)
            second.append(send(ysnd.at[stage, j], ygot.at[stage, j], y_send.at[stage, j], y_recv.at[stage, j], {'tp': 1 - tp}))
        third = []
        for j in range(n_half):
            second[j].wait_recv()
            dst[core * n_half + j] = base_of(j) + (ysnd[stage, j] + ygot[stage, j])
            third.append(send(dst.at[core * n_half + j], dst.at[core * n_half + j], g_send.at[stage, j], g_recv.at[stage, j], {'sp': partner}))
        for copy in third:
            copy.wait_recv()

    o_copy = send(o_snd, o_got, p_send, p_recv, {'sp': partner})
    for j in range(n_half):
        acc[j] = product(o_cat[...], wo.at[0], out_copies[0], j)
    for copy in side:
        copy.wait()
    o_copy.wait_recv()
    o_other = o_got[...].astype(jnp.bfloat16)
    spread(0, lambda j: acc[j] + product(o_other, wo.at[1], out_copies[1], j), lambda j: hid_ref[:, column(j)].astype(jnp.float32), x1)

    square = functools.reduce(lambda a, b: a + b, [x1[i] * x1[i] for i in range(2 * n_half)])
    inv = lax.rsqrt(jnp.sum(square, axis=1, keepdims=True) / (2 * n_half * COLS) + NORM_EPS)
    for i in range(2 * n_half):
        cut = slice(i * COLS, (i + 1) * COLS)
        r2[:, cut] = (x1[i] * inv * gain_ref[:, cut]).astype(jnp.bfloat16)

    a_copies = []
    for i in range(n_gu):
        gate_up_copies[2 * i].wait()
        gate_up_copies[2 * i + 1].wait()
        gate = jnp.dot(r2[...], wg[i], preferred_element_type=jnp.float32)
        up = jnp.dot(r2[...], wu[i], preferred_element_type=jnp.float32)
        value = (gate * jax.nn.sigmoid(gate) * up).astype(jnp.bfloat16)
        act[0, :, i * COLS:(i + 1) * COLS] = value
        a_snd[i] = value.astype(jnp.float32)
        a_copies.append(send(a_snd.at[i], a_got.at[i], a_send.at[i], a_recv.at[i], {'sp': partner}))
    for j in range(n_half):
        acc[j] = product(act[0], wd.at[0], down_copies[0], j)
    for i in range(n_gu):
        a_copies[i].wait_recv()
        act[1, :, i * COLS:(i + 1) * COLS] = a_got[i].astype(jnp.bfloat16)
    spread(1, lambda j: acc[j] + product(act[1], wd.at[1], down_copies[1], j), lambda j: x1[core * n_half + j], x2)
    for i in range(2 * n_half):
        out_ref[:, i * COLS:(i + 1) * COLS] = x2[i]
    for copy in sent:
        copy.wait_send()


def layer_tail(om, hidden, norm_mlp, w_out, w_gate_up, w_down, dim):
    rows, model = hidden.shape
    half_width, units = w_out.shape[0] // 2, w_down.shape[0] // 2
    n_wd, n_gu = model // COLS, units // COLS
    n_half = n_wd // 2
    f32, bf16 = jnp.float32, jnp.bfloat16
    vmem = pl.BlockSpec(memory_space=pltpu.VMEM)
    hbm = pl.BlockSpec(memory_space=pl.ANY)
    dma = pltpu.SemaphoreType.DMA
    out = pl.pallas_call(
        functools.partial(tail_kernel, dim),
        out_shape=pltpu.VMEM((rows, model), f32),
        in_specs=[vmem, hbm, hbm, hbm, hbm, hbm],
        out_specs=vmem,
        scratch_shapes=[
            pltpu.VMEM((rows, model), bf16),
            pltpu.VMEM((1, model), f32),
            pltpu.VMEM((4, rows, half_width + 128), f32),
            pltpu.VMEM((2, n_half, half_width, COLS), bf16),
            pltpu.VMEM((n_gu, model, COLS), bf16),
            pltpu.VMEM((n_gu, model, COLS), bf16),
            pltpu.VMEM((2, n_half, units, COLS), bf16),
            pltpu.VMEM((rows, half_width), bf16),
            pltpu.VMEM((rows, half_width), f32),
            pltpu.VMEM((rows, half_width), f32),
            pltpu.VMEM((n_half, rows, COLS), f32),
            pltpu.VMEM((2, n_half, rows, COLS), f32),
            pltpu.VMEM((2, n_half, rows, COLS), f32),
            pltpu.VMEM((n_wd, rows, COLS), f32),
            pltpu.VMEM((rows, model), bf16),
            pltpu.VMEM((2, rows, units), bf16),
            pltpu.VMEM((n_gu, rows, COLS), f32),
            pltpu.VMEM((n_gu, rows, COLS), f32),
            pltpu.VMEM((n_wd, rows, COLS), f32),
            dma((2,)), dma((2, n_half)), dma((2, n_half)), dma((2, n_gu)),
            dma((3,)), dma((3,)),
            dma, dma,
            dma((n_gu,)), dma((n_gu,)),
            dma((2, n_half)), dma((2, n_half)),
            dma((2, n_half)), dma((2, n_half)),
        ],
        compiler_params=pltpu.CompilerParams(collective_id=0, has_side_effects=True, vmem_limit_bytes=54 << 20),
        name="tail",
    )(pltpu.with_memory_space_constraint(om, pltpu.VMEM), *(pltpu.with_memory_space_constraint(x, pltpu.HBM) for x in (hidden, norm_mlp[None, :])), w_out, w_gate_up, w_down)
    return out.astype(bf16)


def solution(mesh):
    cache_spec = P('dp', 'sp', 'tp', None)

    def local_step(hidden, positions, norm_attn, norm_mlp, w_qkv, w_out, w_gate_up, w_down, k_cache, v_cache):
        num_rows, block_len, kv_local, head_dim = k_cache.shape
        k_t, v_t = k_cache.transpose(0, 2, 3, 1), v_cache.transpose(0, 2, 3, 1)
        q_rows, new_t, k_ring, v_ring = project(positions, hidden, norm_attn, w_qkv, k_t, v_t)
        k_upd, v_upd, om = attend(positions, q_rows, new_t, k_ring, v_ring, k_t, v_t)
        result = layer_tail(om, hidden, norm_mlp, w_out, w_gate_up, w_down, head_dim)
        return result, k_upd.transpose(0, 3, 1, 2), v_upd.transpose(0, 3, 1, 2)

    return jax.shard_map(local_step, mesh=mesh, in_specs=(P('dp', None), P('dp'), P(None), P(None), P(None, 'tp'), P('tp', None), P(None, 'tp'), P('tp', None), cache_spec, cache_spec), out_specs=(P('dp', None), cache_spec, cache_spec), check_vma=False)
```

```python
import functools
import math

import jax
import jax.numpy as jnp
from jax import lax
from jax.experimental import pallas as pl
from jax.experimental.pallas import tpu as pltpu
from jax.sharding import PartitionSpec as P

WINDOW = 2047
ROPE_BASE = 10000.0
NORM_EPS = 1e-5
NEG = -1e30
MESH = pl.DeviceIdType.MESH


QKV_COLS = 384
SLOTS = 8
PRE = 7
DRAIN = 3


def project_kernel(dim, pos_hbm, hid_hbm, gain_hbm, w_hbm, k_hbm, v_hbm, q_ref, new_t, k_ring, v_ring,
                   pos_ref, hid_ref, gain_ref, w_buf, normed_ref, qkv_t, turned, msg, gath,
                   w_sem, in_sem, side_sem, s_send, s_recv):
    sp = lax.axis_index('sp')
    rows, model = hid_ref.shape
    mine = qkv_t.shape[0]
    n_w = mine // QKV_COLS
    w_copies = []
    for i in range(n_w):
        first = pl.multiple_of(sp * mine + i * QKV_COLS, QKV_COLS)
        w_copies.append(pltpu.make_async_copy(w_hbm.at[:, pl.ds(first, QKV_COLS)], w_buf.at[i], w_sem.at[i]))
    side = [pltpu.make_async_copy(src, dst, side_sem.at[i]) for i, (src, dst) in enumerate(((hid_hbm, hid_ref), (gain_hbm, gain_ref), (pos_hbm, pos_ref)))]
    loads = []
    for b in range(PRE):
        loads.append(pltpu.make_async_copy(k_hbm.at[b], k_ring.at[b], in_sem.at[0, b]))
        loads.append(pltpu.make_async_copy(v_hbm.at[b], v_ring.at[b], in_sem.at[1, b]))
    for copy in side + w_copies + loads[:2]:
        copy.start()
    barrier = pltpu.get_barrier_semaphore()
    for step in range(1, 4):
        pl.semaphore_signal(barrier, inc=1, device_id={'sp': lax.rem(sp + step, 4)}, device_id_type=MESH)
    for copy in side:
        copy.wait()

    half = dim // 2
    lane = lax.broadcasted_iota(jnp.int32, (1, 128), 1)
    pos_row = jnp.zeros((1, 128), jnp.int32)
    for b in range(rows):
        pos_row = jnp.where(lane == b, pos_ref[b], pos_row)
    pair = lax.broadcasted_iota(jnp.int32, (half, 128), 0).astype(jnp.float32)
    angles = pos_row.astype(jnp.float32) * jnp.exp(pair * (-2.0 / dim * math.log(ROPE_BASE)))
    cos_t, sin_t = jnp.cos(angles), jnp.sin(angles)

    resid = hid_ref[...].astype(jnp.float32)
    inv = lax.rsqrt(jnp.sum(resid * resid, axis=1, keepdims=True) / model + NORM_EPS)
    normed_ref[...] = (resid * inv * gain_ref[...]).astype(jnp.bfloat16)
    pad = jnp.zeros((128 - rows, QKV_COLS), jnp.float32)
    for i in range(n_w):
        w_copies[i].wait()
        for copy in loads[2 + 4 * i:6 + 4 * i]:
            copy.start()
        part = jnp.dot(normed_ref[...], w_buf[i], preferred_element_type=jnp.float32)
        qkv_t[i * QKV_COLS:(i + 1) * QKV_COLS, :] = jnp.concatenate([part, pad], axis=0).T
    third = mine // 3
    for h in range(third // dim):
        for part in range(2):
            first = (3 * h + part) * dim
            at = part * third + h * dim
            low, high = qkv_t[first:first + half, :], qkv_t[first + half:first + dim, :]
            turned[at:at + half, :] = low * cos_t - high * sin_t
            turned[at + half:at + dim, :] = high * cos_t + low * sin_t
        turned[2 * third + h * dim:2 * third + (h + 1) * dim, :] = qkv_t[(3 * h + 2) * dim:(3 * h + 3) * dim, :]
    own_rows = turned[...].T[:rows, :]
    msg[...] = own_rows
    pl.semaphore_wait(barrier, 3)
    sends = []
    for step in (2, 1, 3):
        copy = pltpu.make_async_remote_copy(src_ref=msg, dst_ref=gath.at[sp], send_sem=s_send.at[step - 1], recv_sem=s_recv.at[step - 1],
                                            device_id={'sp': lax.rem(sp + step, 4)}, device_id_type=MESH)
        copy.start()
        sends.append(copy)
    gath[sp] = own_rows
    for copy in sends:
        copy.wait_recv()
    q_ref[...] = gath[:, :, :third]
    pad = jnp.zeros((128 - rows, third), jnp.float32)
    for which in range(2):
        for s in range(4):
            entry = gath[s, :, (1 + which) * third:(2 + which) * third]
            new_t[which, s * third:(s + 1) * third, :] = jnp.concatenate([entry, pad], axis=0).T
    for copy in loads:
        copy.wait()
    for copy in sends:
        copy.wait_send()


def project(positions, hidden, norm_attn, w_qkv, k_t, v_t):
    rows, heads, dim, block = k_t.shape
    model, mine = hidden.shape[1], w_qkv.shape[1] // 4
    vmem = pl.BlockSpec(memory_space=pltpu.VMEM)
    hbm = pl.BlockSpec(memory_space=pl.ANY)
    f32, bf16, dma = jnp.float32, jnp.bfloat16, pltpu.SemaphoreType.DMA
    return pl.pallas_call(
        functools.partial(project_kernel, dim),
        out_shape=(pltpu.VMEM((4, rows, mine // 3), f32), pltpu.VMEM((2, heads * dim, 128), f32), pltpu.VMEM((SLOTS, heads, dim, block), bf16), pltpu.VMEM((SLOTS, heads, dim, block), bf16)),
        in_specs=[hbm] * 6,
        out_specs=(vmem, vmem, vmem, vmem),
        scratch_shapes=[
            pltpu.SMEM((rows,), jnp.int32),
            pltpu.VMEM((rows, model), bf16),
            pltpu.VMEM((1, model), f32),
            pltpu.VMEM((mine // QKV_COLS, model, QKV_COLS), bf16),
            pltpu.VMEM((rows, model), bf16),
            pltpu.VMEM((mine, 128), f32),
            pltpu.VMEM((mine, 128), f32),
            pltpu.VMEM((rows, mine), f32),
            pltpu.VMEM((4, rows, mine), f32),
            dma((mine // QKV_COLS,)), dma((2, PRE)), dma((3,)), dma((3,)), dma((3,)),
        ],
        compiler_params=pltpu.CompilerParams(collective_id=1, has_side_effects=True, vmem_limit_bytes=8200 << 10),
        name="project",
    )(*(pltpu.with_memory_space_constraint(x, pltpu.HBM) for x in (positions, hidden, norm_attn[None, :])), w_qkv, k_t, v_t)


def attend_kernel(pos_hbm, q_ref, new_t, k_in, v_in, k_hbm, v_hbm, ko_hbm, vo_hbm, om_ref, k_ring, v_ring,
                  pos_ref, in_sem, out_sem, side_sem):
    rows, third = q_ref.shape[1:]
    heads, dim, block = k_ring.shape[1:]
    width = heads * dim
    base = lax.axis_index('sp') * block

    def load(b, which):
        slot = lax.rem(b, SLOTS)
        src, buf = ((k_hbm, k_ring), (v_hbm, v_ring))[which]
        return pltpu.make_async_copy(src.at[b], buf.at[slot], in_sem.at[which, slot])

    def store(b, which):
        slot = lax.rem(b, SLOTS)
        dst, buf = ((ko_hbm, k_ring), (vo_hbm, v_ring))[which]
        return pltpu.make_async_copy(buf.at[slot], dst.at[b], out_sem.at[which, slot])

    pos_copy = pltpu.make_async_copy(pos_hbm, pos_ref, side_sem)
    pos_copy.start()
    for b in range(PRE, SLOTS):
        load(b, 0).start()
        load(b, 1).start()
    pos_copy.wait()

    own = lax.broadcasted_iota(jnp.int32, (heads, width), 1) // dim == lax.broadcasted_iota(jnp.int32, (heads, width), 0)
    lane_ids = lax.broadcasted_iota(jnp.int32, (heads, 128), 1)
    head_ids = lax.broadcasted_iota(jnp.int32, (heads, 128), 0)
    half_heads, half_width = heads // 2, width // 2

    def patch(buf, slot, which, b, pos):
        at = pos - base

        @pl.when((at >= 0) & (at < block))
        def _():
            inner = lax.rem(at, 128)
            start = pl.multiple_of(at - inner, 128)
            shift = lax.rem(inner - b + 128, 128)
            hit = lax.broadcasted_iota(jnp.int32, (dim, 128), 1) == inner
            for h in range(heads):
                entry = pltpu.roll(new_t[which, h * dim:(h + 1) * dim, :], shift, 1)
                old = buf[slot, h, :, pl.ds(start, 128)].astype(jnp.float32)
                buf[slot, h, :, pl.ds(start, 128)] = jnp.where(hit, entry, old).astype(jnp.bfloat16)

    def step(b, carry):
        slot = lax.rem(b, SLOTS)
        pos = pos_ref[b]

        @pl.when((b >= DRAIN) & (b + SLOTS - DRAIN < rows))
        def _():
            for which in range(2):
                store(b - DRAIN, which).wait()
                load(b + SLOTS - DRAIN, which).start()

        @pl.when(b >= PRE)
        def _():
            load(b, 0).wait()

        patch(k_ring, slot, 0, b, pos)
        store(b, 0).start(priority=1)
        q_row = jnp.concatenate([q_ref[s, pl.ds(b, 1), :] for s in range(4)], axis=1)
        q_diag = jnp.where(own, jnp.broadcast_to(q_row, (heads, width)), 0.0).astype(jnp.bfloat16)
        scores = jnp.dot(q_diag, k_ring[slot].reshape(width, block), preferred_element_type=jnp.float32) * (dim ** -0.5)
        slot_ids = lax.broadcasted_iota(jnp.int32, (heads, block), 1) + base
        in_window = (slot_ids <= pos) & (slot_ids >= pos - WINDOW)
        scores = jnp.where(in_window, scores, NEG)
        row_max = jnp.max(scores, axis=1, keepdims=True)
        weights = jnp.where(in_window, jnp.exp(scores - row_max), 0.0)
        row_sum = jnp.sum(weights, axis=1, keepdims=True)

        @pl.when(b >= PRE)
        def _():
            load(b, 1).wait()

        patch(v_ring, slot, 1, b, pos)
        store(b, 1).start(priority=1)
        acc = lax.dot_general(weights.astype(jnp.bfloat16), v_ring[slot].reshape(width, block), (((1,), (1,)), ((), ())), preferred_element_type=jnp.float32)
        o_row = jnp.sum(jnp.where(own, acc, 0.0), axis=0, keepdims=True)
        for core in range(2):
            local = head_ids - core * half_heads
            keep = (local >= 0) & (local < half_heads)
            stats = jnp.where(keep & (lane_ids == local), row_max, 0.0) + jnp.where(keep & (lane_ids == local + half_heads), row_sum, 0.0)
            row = jnp.concatenate([o_row[:, core * half_width:(core + 1) * half_width], jnp.sum(stats, axis=0, keepdims=True)], axis=1)
            at_row = lax.broadcasted_iota(jnp.int32, (rows, half_width + 128), 0) == b
            om_ref[core] = jnp.where(at_row, row, om_ref[core])
        return carry

    lax.fori_loop(0, rows, step, 0)
    for b in range(rows - SLOTS, rows):
        store(b, 0).wait()
        store(b, 1).wait()


def attend(positions, q_rows, new_t, k_ring, v_ring, k_t, v_t):
    rows, heads, dim, block = k_t.shape
    width = heads * dim
    vmem = pl.BlockSpec(memory_space=pltpu.VMEM)
    hbm = pl.BlockSpec(memory_space=pl.ANY)
    f32, bf16, dma = jnp.float32, jnp.bfloat16, pltpu.SemaphoreType.DMA
    ring = pltpu.VMEM((SLOTS, heads, dim, block), bf16)
    k_upd, v_upd, om, _, _ = pl.pallas_call(
        attend_kernel,
        out_shape=(jax.ShapeDtypeStruct(k_t.shape, k_t.dtype), jax.ShapeDtypeStruct(v_t.shape, v_t.dtype), pltpu.VMEM((2, rows, width // 2 + 128), f32), ring, ring),
        in_specs=[hbm, vmem, vmem, vmem, vmem, hbm, hbm],
        out_specs=(hbm, hbm, vmem, vmem, vmem),
        scratch_shapes=[
            pltpu.SMEM((rows,), jnp.int32),
            dma((2, SLOTS)), dma((2, SLOTS)), dma,
        ],
        input_output_aliases={3: 3, 4: 4},
        compiler_params=pltpu.CompilerParams(vmem_limit_bytes=5 << 20),
        name="attend",
    )(pltpu.with_memory_space_constraint(positions, pltpu.HBM), *(pltpu.with_memory_space_constraint(x, pltpu.VMEM) for x in (q_rows, new_t, k_ring, v_ring)), k_t, v_t)
    return k_upd, v_upd, om


COLS = 512


def tail_kernel(dim, om_ref, hid_hbm, gain_hbm, wo_hbm, wgu_hbm, wd_hbm, out_ref,
                hid_ref, gain_ref, obuf, wo, wg, wu, wd, o_cat, o_snd, o_got, acc, ysnd, ygot, x1, r2, act, a_snd, a_got, x2,
                side_sem, wo_sem, wd_sem, gu_sem, o_send, o_recv, p_send, p_recv, a_send, a_recv, y_send, y_recv, g_send, g_recv):
    tp, sp = lax.axis_index('tp'), lax.axis_index('sp')
    core = lax.rem(sp, 2)
    partner = sp + 1 - 2 * core
    rows = hid_ref.shape[0]
    half_width = wo.shape[2]
    n_half = x1.shape[0] // 2
    n_gu = wg.shape[0]
    units = wd.shape[2]
    ffn = wgu_hbm.shape[1] // 2

    def column(j):
        return pl.ds(pl.multiple_of((core * n_half + j) * COLS, COLS), COLS)

    side = [pltpu.make_async_copy(hid_hbm, hid_ref, side_sem.at[0]), pltpu.make_async_copy(gain_hbm, gain_ref, side_sem.at[1])]
    out_copies, down_copies, gate_up_copies = [[], []], [[], []], []
    for k, owner in enumerate((core, 1 - core)):
        for j in range(n_half):
            out_copies[k].append(pltpu.make_async_copy(wo_hbm.at[pl.ds(owner * half_width, half_width), column(j)], wo.at[k, j], wo_sem.at[k, j]))
            down_copies[k].append(pltpu.make_async_copy(wd_hbm.at[pl.ds(owner * units, units), column(j)], wd.at[k, j], wd_sem.at[k, j]))
    for i in range(n_gu):
        first = core * units + i * COLS
        gate_up_copies.append(pltpu.make_async_copy(wgu_hbm.at[:, pl.ds(pl.multiple_of(first, COLS), COLS)], wg.at[i], gu_sem.at[0, i]))
        gate_up_copies.append(pltpu.make_async_copy(wgu_hbm.at[:, pl.ds(pl.multiple_of(ffn + first, COLS), COLS)], wu.at[i], gu_sem.at[1, i]))
    barrier = pltpu.get_barrier_semaphore()
    for step in range(1, 4):
        pl.semaphore_signal(barrier, inc=1, device_id={'sp': lax.rem(sp + step, 4)}, device_id_type=MESH)
    pl.semaphore_signal(barrier, inc=1, device_id={'tp': 1 - tp}, device_id_type=MESH)
    for copy in side + out_copies[0] + out_copies[1]:
        copy.start()
    pl.semaphore_wait(barrier, 4)

    sent = []

    def send(src, dst, send_sem, recv_sem, where):
        copy = pltpu.make_async_remote_copy(src_ref=src, dst_ref=dst, send_sem=send_sem, recv_sem=recv_sem, device_id=where, device_id_type=MESH)
        copy.start()
        sent.append(copy)
        return copy

    first_copies = []
    for step in (2, 1, 3):
        peer = lax.rem(sp + step, 4)
        first_copies.append(send(om_ref.at[lax.rem(peer, 2)], obuf.at[sp], o_send.at[step - 1], o_recv.at[step - 1], {'sp': peer}))
    obuf[sp] = om_ref[core]
    for copy in gate_up_copies:
        copy.start()
    for copy in first_copies:
        copy.wait_recv()
    for copy in down_copies[0] + down_copies[1]:
        copy.start()

    heads = half_width // dim
    stats = [obuf[s, :, half_width:] for s in range(4)]
    top = functools.reduce(jnp.maximum, stats)
    alphas = [jnp.exp(st - top) for st in stats]
    total = functools.reduce(lambda a, b: a + b, [al * pltpu.roll(st, 128 - heads, 1) for al, st in zip(alphas, stats)])
    betas = [al / total for al in alphas]
    lane = lax.broadcasted_iota(jnp.int32, (rows, 128), 1)
    for k in range(half_width // 128):
        first, last = 128 * k // dim, (128 * k + 127) // dim
        value = None
        for s in range(4):
            scale = jnp.broadcast_to(betas[s][:, first:first + 1], (rows, 128))
            for h in range(first + 1, last + 1):
                scale = jnp.where(lane >= h * dim - 128 * k, betas[s][:, h:h + 1], scale)
            term = scale * obuf[s, :, 128 * k:128 * (k + 1)]
            value = term if value is None else value + term
        value = value.astype(jnp.bfloat16)
        o_cat[:, 128 * k:128 * (k + 1)] = value
        o_snd[:, 128 * k:128 * (k + 1)] = value.astype(jnp.float32)

    def product(lhs, w_ref, copies, j):
        copies[j].wait()
        return jnp.dot(lhs, w_ref[j], preferred_element_type=jnp.float32)

    def spread(stage, part_of, base_of, dst):
        second = []
        for j in range(n_half):
            ysnd[stage, j] = part_of(j).astype(jnp.bfloat16).astype(jnp.float32)
            second.append(send(ysnd.at[stage, j], ygot.at[stage, j], y_send.at[stage, j], y_recv.at[stage, j], {'tp': 1 - tp}))
        third = []
        for j in range(n_half):
            second[j].wait_recv()
            dst[core * n_half + j] = base_of(j) + (ysnd[stage, j] + ygot[stage, j])
            third.append(send(dst.at[core * n_half + j], dst.at[core * n_half + j], g_send.at[stage, j], g_recv.at[stage, j], {'sp': partner}))
        for copy in third:
            copy.wait_recv()

    o_copy = send(o_snd, o_got, p_send, p_recv, {'sp': partner})
    for j in range(n_half):
        acc[j] = product(o_cat[...], wo.at[0], out_copies[0], j)
    for copy in side:
        copy.wait()
    o_copy.wait_recv()
    o_other = o_got[...].astype(jnp.bfloat16)
    spread(0, lambda j: acc[j] + product(o_other, wo.at[1], out_copies[1], j), lambda j: hid_ref[:, column(j)].astype(jnp.float32), x1)

    square = functools.reduce(lambda a, b: a + b, [x1[i] * x1[i] for i in range(2 * n_half)])
    inv = lax.rsqrt(jnp.sum(square, axis=1, keepdims=True) / (2 * n_half * COLS) + NORM_EPS)
    for i in range(2 * n_half):
        cut = slice(i * COLS, (i + 1) * COLS)
        r2[:, cut] = (x1[i] * inv * gain_ref[:, cut]).astype(jnp.bfloat16)

    a_copies = []
    for i in range(n_gu):
        gate_up_copies[2 * i].wait()
        gate_up_copies[2 * i + 1].wait()
        gate = jnp.dot(r2[...], wg[i], preferred_element_type=jnp.float32)
        up = jnp.dot(r2[...], wu[i], preferred_element_type=jnp.float32)
        value = (gate * jax.nn.sigmoid(gate) * up).astype(jnp.bfloat16)
        act[0, :, i * COLS:(i + 1) * COLS] = value
        a_snd[i] = value.astype(jnp.float32)
        a_copies.append(send(a_snd.at[i], a_got.at[i], a_send.at[i], a_recv.at[i], {'sp': partner}))
    for j in range(n_half):
        acc[j] = product(act[0], wd.at[0], down_copies[0], j)
    for i in range(n_gu):
        a_copies[i].wait_recv()
        act[1, :, i * COLS:(i + 1) * COLS] = a_got[i].astype(jnp.bfloat16)
    spread(1, lambda j: acc[j] + product(act[1], wd.at[1], down_copies[1], j), lambda j: x1[core * n_half + j], x2)
    for i in range(2 * n_half):
        out_ref[:, i * COLS:(i + 1) * COLS] = x2[i]
    for copy in sent:
        copy.wait_send()


def layer_tail(om, hidden, norm_mlp, w_out, w_gate_up, w_down, dim):
    rows, model = hidden.shape
    half_width, units = w_out.shape[0] // 2, w_down.shape[0] // 2
    n_wd, n_gu = model // COLS, units // COLS
    n_half = n_wd // 2
    f32, bf16 = jnp.float32, jnp.bfloat16
    vmem = pl.BlockSpec(memory_space=pltpu.VMEM)
    hbm = pl.BlockSpec(memory_space=pl.ANY)
    dma = pltpu.SemaphoreType.DMA
    out = pl.pallas_call(
        functools.partial(tail_kernel, dim),
        out_shape=pltpu.VMEM((rows, model), f32),
        in_specs=[vmem, hbm, hbm, hbm, hbm, hbm],
        out_specs=vmem,
        scratch_shapes=[
            pltpu.VMEM((rows, model), bf16),
            pltpu.VMEM((1, model), f32),
            pltpu.VMEM((4, rows, half_width + 128), f32),
            pltpu.VMEM((2, n_half, half_width, COLS), bf16),
            pltpu.VMEM((n_gu, model, COLS), bf16),
            pltpu.VMEM((n_gu, model, COLS), bf16),
            pltpu.VMEM((2, n_half, units, COLS), bf16),
            pltpu.VMEM((rows, half_width), bf16),
            pltpu.VMEM((rows, half_width), f32),
            pltpu.VMEM((rows, half_width), f32),
            pltpu.VMEM((n_half, rows, COLS), f32),
            pltpu.VMEM((2, n_half, rows, COLS), f32),
            pltpu.VMEM((2, n_half, rows, COLS), f32),
            pltpu.VMEM((n_wd, rows, COLS), f32),
            pltpu.VMEM((rows, model), bf16),
            pltpu.VMEM((2, rows, units), bf16),
            pltpu.VMEM((n_gu, rows, COLS), f32),
            pltpu.VMEM((n_gu, rows, COLS), f32),
            pltpu.VMEM((n_wd, rows, COLS), f32),
            dma((2,)), dma((2, n_half)), dma((2, n_half)), dma((2, n_gu)),
            dma((3,)), dma((3,)),
            dma, dma,
            dma((n_gu,)), dma((n_gu,)),
            dma((2, n_half)), dma((2, n_half)),
            dma((2, n_half)), dma((2, n_half)),
        ],
        compiler_params=pltpu.CompilerParams(collective_id=0, has_side_effects=True, vmem_limit_bytes=54 << 20),
        name="tail",
    )(pltpu.with_memory_space_constraint(om, pltpu.VMEM), *(pltpu.with_memory_space_constraint(x, pltpu.HBM) for x in (hidden, norm_mlp[None, :])), w_out, w_gate_up, w_down)
    return out.astype(bf16)


def solution(mesh):
    cache_spec = P('dp', 'sp', 'tp', None)

    def local_step(hidden, positions, norm_attn, norm_mlp, w_qkv, w_out, w_gate_up, w_down, k_cache, v_cache):
        num_rows, block_len, kv_local, head_dim = k_cache.shape
        k_t, v_t = k_cache.transpose(0, 2, 3, 1), v_cache.transpose(0, 2, 3, 1)
        q_rows, new_t, k_ring, v_ring = project(positions, hidden, norm_attn, w_qkv, k_t, v_t)
        k_upd, v_upd, om = attend(positions, q_rows, new_t, k_ring, v_ring, k_t, v_t)
        result = layer_tail(om, hidden, norm_mlp, w_out, w_gate_up, w_down, head_dim)
        return result, k_upd.transpose(0, 3, 1, 2), v_upd.transpose(0, 3, 1, 2)

    return jax.shard_map(local_step, mesh=mesh, in_specs=(P('dp', None), P('dp'), P(None), P(None), P(None, 'tp'), P('tp', None), P(None, 'tp'), P('tp', None), cache_spec, cache_spec), out_specs=(P('dp', None), cache_spec, cache_spec), check_vma=False)
```

```python
import functools
import math

import jax
import jax.numpy as jnp
from jax import lax
from jax.experimental import pallas as pl
from jax.experimental.pallas import tpu as pltpu
from jax.sharding import PartitionSpec as P

WINDOW = 2047
ROPE_BASE = 10000.0
NORM_EPS = 1e-5
NEG = -1e30
MESH = pl.DeviceIdType.MESH


QKV_COLS = 384
SLOTS = 8
PRE = 7
DRAIN = 3
LEFT = 4


def project_kernel(dim, pos_hbm, hid_hbm, gain_hbm, w_hbm, k_hbm, v_hbm, q_ref, new_t, k_ring, v_ring,
                   pos_ref, hid_ref, gain_ref, w_buf, normed_ref, qkv_t, turned, msg, gath,
                   w_sem, in_sem, side_sem, s_send, s_recv):
    sp = lax.axis_index('sp')
    rows, model = hid_ref.shape
    mine = qkv_t.shape[0]
    n_w = mine // QKV_COLS
    w_copies = []
    for i in range(n_w):
        first = pl.multiple_of(sp * mine + i * QKV_COLS, QKV_COLS)
        w_copies.append(pltpu.make_async_copy(w_hbm.at[:, pl.ds(first, QKV_COLS)], w_buf.at[i], w_sem.at[i]))
    side = [pltpu.make_async_copy(src, dst, side_sem.at[i]) for i, (src, dst) in enumerate(((hid_hbm, hid_ref), (gain_hbm, gain_ref), (pos_hbm, pos_ref)))]
    loads = []
    for b in range(PRE):
        loads.append(pltpu.make_async_copy(k_hbm.at[b], k_ring.at[b], in_sem.at[0, b]))
        loads.append(pltpu.make_async_copy(v_hbm.at[b], v_ring.at[b], in_sem.at[1, b]))
    for copy in side + w_copies:
        copy.start()
    barrier = pltpu.get_barrier_semaphore()
    for step in range(1, 4):
        pl.semaphore_signal(barrier, inc=1, device_id={'sp': lax.rem(sp + step, 4)}, device_id_type=MESH)
    for copy in side:
        copy.wait()

    half = dim // 2
    lane = lax.broadcasted_iota(jnp.int32, (1, 128), 1)
    pos_row = jnp.zeros((1, 128), jnp.int32)
    for b in range(rows):
        pos_row = jnp.where(lane == b, pos_ref[b], pos_row)
    pair = lax.broadcasted_iota(jnp.int32, (half, 128), 0).astype(jnp.float32)
    angles = pos_row.astype(jnp.float32) * jnp.exp(pair * (-2.0 / dim * math.log(ROPE_BASE)))
    cos_t, sin_t = jnp.cos(angles), jnp.sin(angles)

    resid = hid_ref[...].astype(jnp.float32)
    inv = lax.rsqrt(jnp.sum(resid * resid, axis=1, keepdims=True) / model + NORM_EPS)
    normed_ref[...] = (resid * inv * gain_ref[...]).astype(jnp.bfloat16)
    pad = jnp.zeros((128 - rows, QKV_COLS), jnp.float32)
    for i in range(n_w):
        w_copies[i].wait()
        for copy in loads[i * len(loads) // n_w:(i + 1) * len(loads) // n_w]:
            copy.start()
        part = jnp.dot(normed_ref[...], w_buf[i], preferred_element_type=jnp.float32)
        qkv_t[i * QKV_COLS:(i + 1) * QKV_COLS, :] = jnp.concatenate([part, pad], axis=0).T
    third = mine // 3
    for h in range(third // dim):
        for part in range(2):
            first = (3 * h + part) * dim
            at = part * third + h * dim
            low, high = qkv_t[first:first + half, :], qkv_t[first + half:first + dim, :]
            turned[at:at + half, :] = low * cos_t - high * sin_t
            turned[at + half:at + dim, :] = high * cos_t + low * sin_t
        turned[2 * third + h * dim:2 * third + (h + 1) * dim, :] = qkv_t[(3 * h + 2) * dim:(3 * h + 3) * dim, :]
    own_rows = turned[...].T[:rows, :]
    msg[...] = own_rows
    pl.semaphore_wait(barrier, 3)
    sends = []
    for step in (2, 1, 3):
        copy = pltpu.make_async_remote_copy(src_ref=msg, dst_ref=gath.at[sp], send_sem=s_send.at[step - 1], recv_sem=s_recv.at[step - 1],
                                            device_id={'sp': lax.rem(sp + step, 4)}, device_id_type=MESH)
        copy.start()
        sends.append(copy)
    gath[sp] = own_rows
    for copy in sends:
        copy.wait_recv()
    q_ref[...] = gath[:, :, :third]
    pad = jnp.zeros((128 - rows, third), jnp.float32)
    for which in range(2):
        for s in range(4):
            entry = gath[s, :, (1 + which) * third:(2 + which) * third]
            new_t[which, s * third:(s + 1) * third, :] = jnp.concatenate([entry, pad], axis=0).T
    for copy in loads:
        copy.wait()
    for copy in sends:
        copy.wait_send()


def project(positions, hidden, norm_attn, w_qkv, k_t, v_t):
    rows, heads, dim, block = k_t.shape
    model, mine = hidden.shape[1], w_qkv.shape[1] // 4
    vmem = pl.BlockSpec(memory_space=pltpu.VMEM)
    hbm = pl.BlockSpec(memory_space=pl.ANY)
    f32, bf16, dma = jnp.float32, jnp.bfloat16, pltpu.SemaphoreType.DMA
    return pl.pallas_call(
        functools.partial(project_kernel, dim),
        out_shape=(pltpu.VMEM((4, rows, mine // 3), f32), pltpu.VMEM((2, heads * dim, 128), f32), pltpu.VMEM((SLOTS, heads, dim, block), bf16), pltpu.VMEM((SLOTS, heads, dim, block), bf16)),
        in_specs=[hbm] * 6,
        out_specs=(vmem, vmem, vmem, vmem),
        scratch_shapes=[
            pltpu.SMEM((rows,), jnp.int32),
            pltpu.VMEM((rows, model), bf16),
            pltpu.VMEM((1, model), f32),
            pltpu.VMEM((mine // QKV_COLS, model, QKV_COLS), bf16),
            pltpu.VMEM((rows, model), bf16),
            pltpu.VMEM((mine, 128), f32),
            pltpu.VMEM((mine, 128), f32),
            pltpu.VMEM((rows, mine), f32),
            pltpu.VMEM((4, rows, mine), f32),
            dma((mine // QKV_COLS,)), dma((2, PRE)), dma((3,)), dma((3,)), dma((3,)),
        ],
        compiler_params=pltpu.CompilerParams(collective_id=1, has_side_effects=True, vmem_limit_bytes=8200 << 10),
        name="project",
    )(*(pltpu.with_memory_space_constraint(x, pltpu.HBM) for x in (positions, hidden, norm_attn[None, :])), w_qkv, k_t, v_t)


def attend_kernel(pos_hbm, q_ref, new_t, k_in, v_in, k_hbm, v_hbm, ko_hbm, vo_hbm, own_ref, other_ref, k_ring, v_ring,
                  pos_ref, in_sem, out_sem, side_sem):
    rows, third = q_ref.shape[1:]
    heads, dim, block = k_ring.shape[1:]
    width = heads * dim
    base = lax.axis_index('sp') * block
    core = lax.rem(lax.axis_index('sp'), 2)

    def load(b, which):
        slot = lax.rem(b, SLOTS)
        src, buf = ((k_hbm, k_ring), (v_hbm, v_ring))[which]
        return pltpu.make_async_copy(src.at[b], buf.at[slot], in_sem.at[which, slot])

    def store(b, which):
        slot = lax.rem(b, SLOTS)
        dst, buf = ((ko_hbm, k_ring), (vo_hbm, v_ring))[which]
        return pltpu.make_async_copy(buf.at[slot], dst.at[b], out_sem.at[which, slot])

    pos_copy = pltpu.make_async_copy(pos_hbm, pos_ref, side_sem)
    pos_copy.start()
    for b in range(PRE, SLOTS):
        load(b, 0).start()
        load(b, 1).start()
    pos_copy.wait()

    own = lax.broadcasted_iota(jnp.int32, (heads, width), 1) // dim == lax.broadcasted_iota(jnp.int32, (heads, width), 0)
    lane_ids = lax.broadcasted_iota(jnp.int32, (heads, 128), 1)
    head_ids = lax.broadcasted_iota(jnp.int32, (heads, 128), 0)
    half_heads, half_width = heads // 2, width // 2

    def patch(buf, slot, which, b, pos):
        at = pos - base

        @pl.when((at >= 0) & (at < block))
        def _():
            inner = lax.rem(at, 128)
            start = pl.multiple_of(at - inner, 128)
            shift = lax.rem(inner - b + 128, 128)
            hit = lax.broadcasted_iota(jnp.int32, (dim, 128), 1) == inner
            for h in range(heads):
                entry = pltpu.roll(new_t[which, h * dim:(h + 1) * dim, :], shift, 1)
                old = buf[slot, h, :, pl.ds(start, 128)].astype(jnp.float32)
                buf[slot, h, :, pl.ds(start, 128)] = jnp.where(hit, entry, old).astype(jnp.bfloat16)

    def step(b, carry):
        slot = lax.rem(b, SLOTS)
        pos = pos_ref[b]

        @pl.when((b >= DRAIN) & (b + SLOTS - DRAIN < rows))
        def _():
            for which in range(2):
                store(b - DRAIN, which).wait()
                load(b + SLOTS - DRAIN, which).start()

        @pl.when(b >= PRE)
        def _():
            load(b, 0).wait()

        patch(k_ring, slot, 0, b, pos)
        pl.when(b < rows - LEFT)(lambda: store(b, 0).start())
        q_row = jnp.concatenate([q_ref[s, pl.ds(b, 1), :] for s in range(4)], axis=1)
        q_diag = jnp.where(own, jnp.broadcast_to(q_row, (heads, width)), 0.0).astype(jnp.bfloat16)
        scores = jnp.dot(q_diag, k_ring[slot].reshape(width, block), preferred_element_type=jnp.float32) * (dim ** -0.5)
        slot_ids = lax.broadcasted_iota(jnp.int32, (heads, block), 1) + base
        in_window = (slot_ids <= pos) & (slot_ids >= pos - WINDOW)
        scores = jnp.where(in_window, scores, NEG)
        row_max = jnp.max(scores, axis=1, keepdims=True)
        weights = jnp.where(in_window, jnp.exp(scores - row_max), 0.0)
        row_sum = jnp.sum(weights, axis=1, keepdims=True)

        @pl.when(b >= PRE)
        def _():
            load(b, 1).wait()

        patch(v_ring, slot, 1, b, pos)
        pl.when(b < rows - LEFT)(lambda: store(b, 1).start())
        acc = lax.dot_general(weights.astype(jnp.bfloat16), v_ring[slot].reshape(width, block), (((1,), (1,)), ((), ())), preferred_element_type=jnp.float32)
        o_row = jnp.sum(jnp.where(own, acc, 0.0), axis=0, keepdims=True)
        pieces = []
        for half in range(2):
            local = head_ids - half * half_heads
            keep = (local >= 0) & (local < half_heads)
            stats = jnp.where(keep & (lane_ids == local), row_max, 0.0) + jnp.where(keep & (lane_ids == local + half_heads), row_sum, 0.0)
            pieces.append(jnp.concatenate([o_row[:, half * half_width:(half + 1) * half_width], jnp.sum(stats, axis=0, keepdims=True)], axis=1))
        at_row = lax.broadcasted_iota(jnp.int32, (rows, half_width + 128), 0) == b
        own_ref[...] = jnp.where(at_row, jnp.where(core == 0, pieces[0], pieces[1]), own_ref[...])
        other_ref[...] = jnp.where(at_row, jnp.where(core == 0, pieces[1], pieces[0]), other_ref[...])
        return carry

    lax.fori_loop(0, rows, step, 0)
    for b in range(rows - SLOTS, rows - LEFT):
        store(b, 0).wait()
        store(b, 1).wait()


def attend(positions, q_rows, new_t, k_ring, v_ring, k_t, v_t):
    rows, heads, dim, block = k_t.shape
    width = heads * dim
    vmem = pl.BlockSpec(memory_space=pltpu.VMEM)
    hbm = pl.BlockSpec(memory_space=pl.ANY)
    f32, bf16, dma = jnp.float32, jnp.bfloat16, pltpu.SemaphoreType.DMA
    ring = pltpu.VMEM((SLOTS, heads, dim, block), bf16)
    part = jax.ShapeDtypeStruct((rows, width // 2 + 128), f32)
    return pl.pallas_call(
        attend_kernel,
        out_shape=(jax.ShapeDtypeStruct(k_t.shape, k_t.dtype), jax.ShapeDtypeStruct(v_t.shape, v_t.dtype), part, part, ring, ring),
        in_specs=[hbm, vmem, vmem, vmem, vmem, hbm, hbm],
        out_specs=(hbm, hbm, vmem, vmem, vmem, vmem),
        scratch_shapes=[
            pltpu.SMEM((rows,), jnp.int32),
            dma((2, SLOTS)), dma((2, SLOTS)), dma,
        ],
        input_output_aliases={3: 4, 4: 5},
        compiler_params=pltpu.CompilerParams(vmem_limit_bytes=5 << 20),
        name="attend",
    )(pltpu.with_memory_space_constraint(positions, pltpu.HBM), *(pltpu.with_memory_space_constraint(x, pltpu.VMEM) for x in (q_rows, new_t, k_ring, v_ring)), k_t, v_t)


def write_kernel(k_ring, v_ring, k_in, v_in, ko_hbm, vo_hbm, sem):
    rows = ko_hbm.shape[0]
    copies = []
    for b in range(rows - LEFT, rows):
        for which, (ring, dst) in enumerate(((k_ring, ko_hbm), (v_ring, vo_hbm))):
            copies.append(pltpu.make_async_copy(ring.at[b % SLOTS], dst.at[b], sem.at[which, b - rows + LEFT]))
    for copy in copies:
        copy.start()
    for copy in copies:
        copy.wait()


def write_rest(k_ring, v_ring, k_upd, v_upd):
    vmem = pl.BlockSpec(memory_space=pltpu.VMEM)
    hbm = pl.BlockSpec(memory_space=pl.ANY)
    return pl.pallas_call(
        write_kernel,
        out_shape=(jax.ShapeDtypeStruct(k_upd.shape, k_upd.dtype), jax.ShapeDtypeStruct(v_upd.shape, v_upd.dtype)),
        in_specs=[vmem, vmem, hbm, hbm],
        out_specs=(hbm, hbm),
        scratch_shapes=[pltpu.SemaphoreType.DMA((2, LEFT))],
        input_output_aliases={2: 0, 3: 1},
        cost_estimate=pl.CostEstimate(flops=10 ** 10, bytes_accessed=19 << 20, transcendentals=0),
        compiler_params=pltpu.CompilerParams(vmem_limit_bytes=1 << 20),
        name="write_rest",
    )(*(pltpu.with_memory_space_constraint(x, pltpu.VMEM) for x in (k_ring, v_ring)), k_upd, v_upd)


COLS = 512


def tail_kernel(dim, own_ref, in1_ref, in2_ref, in3_ref, hid_hbm, gain_hbm, wo_hbm, wgu_hbm, wd_hbm, out_ref,
                hid_ref, gain_ref, obuf, wo, wg, wu, wd, o_cat, o_snd, o_got, acc, ysnd, ygot, x1, r2, act, a_snd, a_got, x2,
                side_sem, wo_sem, wd_sem, gu_sem, p_send, p_recv, a_send, a_recv, y_send, y_recv, g_send, g_recv):
    tp, sp = lax.axis_index('tp'), lax.axis_index('sp')
    core = lax.rem(sp, 2)
    partner = sp + 1 - 2 * core
    rows = hid_ref.shape[0]
    half_width = wo.shape[2]
    n_half = x1.shape[0] // 2
    n_gu = wg.shape[0]
    units = wd.shape[2]
    ffn = wgu_hbm.shape[1] // 2

    def column(j):
        return pl.ds(pl.multiple_of((core * n_half + j) * COLS, COLS), COLS)

    side = [pltpu.make_async_copy(hid_hbm, hid_ref, side_sem.at[0]), pltpu.make_async_copy(gain_hbm, gain_ref, side_sem.at[1])]
    out_copies, down_copies, gate_up_copies = [[], []], [[], []], []
    for k, owner in enumerate((core, 1 - core)):
        for j in range(n_half):
            out_copies[k].append(pltpu.make_async_copy(wo_hbm.at[pl.ds(owner * half_width, half_width), column(j)], wo.at[k, j], wo_sem.at[k, j]))
            down_copies[k].append(pltpu.make_async_copy(wd_hbm.at[pl.ds(owner * units, units), column(j)], wd.at[k, j], wd_sem.at[k, j]))
    for i in range(n_gu):
        first = core * units + i * COLS
        gate_up_copies.append(pltpu.make_async_copy(wgu_hbm.at[:, pl.ds(pl.multiple_of(first, COLS), COLS)], wg.at[i], gu_sem.at[0, i]))
        gate_up_copies.append(pltpu.make_async_copy(wgu_hbm.at[:, pl.ds(pl.multiple_of(ffn + first, COLS), COLS)], wu.at[i], gu_sem.at[1, i]))
    barrier = pltpu.get_barrier_semaphore()
    pl.semaphore_signal(barrier, inc=1, device_id={'sp': partner}, device_id_type=MESH)
    pl.semaphore_signal(barrier, inc=1, device_id={'tp': 1 - tp}, device_id_type=MESH)
    for copy in side + out_copies[0] + out_copies[1] + gate_up_copies:
        copy.start()

    sent = []

    def send(src, dst, send_sem, recv_sem, where):
        copy = pltpu.make_async_remote_copy(src_ref=src, dst_ref=dst, send_sem=send_sem, recv_sem=recv_sem, device_id=where, device_id_type=MESH)
        copy.start()
        sent.append(copy)
        return copy

    for source, ref in ((sp, own_ref), (partner, in1_ref), (lax.rem(sp + 2, 4), in2_ref), (lax.rem(partner + 2, 4), in3_ref)):
        obuf[source] = ref[...]

    heads = half_width // dim
    stats = [obuf[s, :, half_width:] for s in range(4)]
    top = functools.reduce(jnp.maximum, stats)
    alphas = [jnp.exp(st - top) for st in stats]
    total = functools.reduce(lambda a, b: a + b, [al * pltpu.roll(st, 128 - heads, 1) for al, st in zip(alphas, stats)])
    betas = [al / total for al in alphas]
    lane = lax.broadcasted_iota(jnp.int32, (rows, 128), 1)
    for k in range(half_width // 128):
        first, last = 128 * k // dim, (128 * k + 127) // dim
        value = None
        for s in range(4):
            scale = jnp.broadcast_to(betas[s][:, first:first + 1], (rows, 128))
            for h in range(first + 1, last + 1):
                scale = jnp.where(lane >= h * dim - 128 * k, betas[s][:, h:h + 1], scale)
            term = scale * obuf[s, :, 128 * k:128 * (k + 1)]
            value = term if value is None else value + term
        value = value.astype(jnp.bfloat16)
        o_cat[:, 128 * k:128 * (k + 1)] = value
        o_snd[:, 128 * k:128 * (k + 1)] = value.astype(jnp.float32)

    def product(lhs, w_ref, copies, j):
        copies[j].wait()
        return jnp.dot(lhs, w_ref[j], preferred_element_type=jnp.float32)

    def spread(stage, part_of, base_of, dst):
        second = []
        for j in range(n_half):
            ysnd[stage, j] = part_of(j).astype(jnp.bfloat16).astype(jnp.float32)
            second.append(send(ysnd.at[stage, j], ygot.at[stage, j], y_send.at[stage, j], y_recv.at[stage, j], {'tp': 1 - tp}))
        third = []
        for j in range(n_half):
            second[j].wait_recv()
            dst[core * n_half + j] = base_of(j) + (ysnd[stage, j] + ygot[stage, j])
            third.append(send(dst.at[core * n_half + j], dst.at[core * n_half + j], g_send.at[stage, j], g_recv.at[stage, j], {'sp': partner}))
        for copy in third:
            copy.wait_recv()

    for copy in down_copies[0] + down_copies[1]:
        copy.start()
    pl.semaphore_wait(barrier, 2)
    o_copy = send(o_snd, o_got, p_send, p_recv, {'sp': partner})
    for j in range(n_half):
        acc[j] = product(o_cat[...], wo.at[0], out_copies[0], j)
    for copy in side:
        copy.wait()
    o_copy.wait_recv()
    o_other = o_got[...].astype(jnp.bfloat16)
    spread(0, lambda j: acc[j] + product(o_other, wo.at[1], out_copies[1], j), lambda j: hid_ref[:, column(j)].astype(jnp.float32), x1)

    square = functools.reduce(lambda a, b: a + b, [x1[i] * x1[i] for i in range(2 * n_half)])
    inv = lax.rsqrt(jnp.sum(square, axis=1, keepdims=True) / (2 * n_half * COLS) + NORM_EPS)
    for i in range(2 * n_half):
        cut = slice(i * COLS, (i + 1) * COLS)
        r2[:, cut] = (x1[i] * inv * gain_ref[:, cut]).astype(jnp.bfloat16)

    a_copies = []
    for i in range(n_gu):
        gate_up_copies[2 * i].wait()
        gate_up_copies[2 * i + 1].wait()
        gate = jnp.dot(r2[...], wg[i], preferred_element_type=jnp.float32)
        up = jnp.dot(r2[...], wu[i], preferred_element_type=jnp.float32)
        value = (gate * jax.nn.sigmoid(gate) * up).astype(jnp.bfloat16)
        act[0, :, i * COLS:(i + 1) * COLS] = value
        a_snd[i] = value.astype(jnp.float32)
        a_copies.append(send(a_snd.at[i], a_got.at[i], a_send.at[i], a_recv.at[i], {'sp': partner}))
    for j in range(n_half):
        acc[j] = product(act[0], wd.at[0], down_copies[0], j)
    for i in range(n_gu):
        a_copies[i].wait_recv()
        act[1, :, i * COLS:(i + 1) * COLS] = a_got[i].astype(jnp.bfloat16)
    spread(1, lambda j: acc[j] + product(act[1], wd.at[1], down_copies[1], j), lambda j: x1[core * n_half + j], x2)
    for i in range(2 * n_half):
        out_ref[:, i * COLS:(i + 1) * COLS] = x2[i]
    for copy in sent:
        copy.wait_send()


def layer_tail(parts, hidden, norm_mlp, w_out, w_gate_up, w_down, dim):
    rows, model = hidden.shape
    half_width, units = w_out.shape[0] // 2, w_down.shape[0] // 2
    n_wd, n_gu = model // COLS, units // COLS
    n_half = n_wd // 2
    f32, bf16 = jnp.float32, jnp.bfloat16
    vmem = pl.BlockSpec(memory_space=pltpu.VMEM)
    hbm = pl.BlockSpec(memory_space=pl.ANY)
    dma = pltpu.SemaphoreType.DMA
    out = pl.pallas_call(
        functools.partial(tail_kernel, dim),
        out_shape=pltpu.VMEM((rows, model), f32),
        in_specs=[vmem] * 4 + [hbm] * 5,
        out_specs=vmem,
        scratch_shapes=[
            pltpu.VMEM((rows, model), bf16),
            pltpu.VMEM((1, model), f32),
            pltpu.VMEM((4, rows, half_width + 128), f32),
            pltpu.VMEM((2, n_half, half_width, COLS), bf16),
            pltpu.VMEM((n_gu, model, COLS), bf16),
            pltpu.VMEM((n_gu, model, COLS), bf16),
            pltpu.VMEM((2, n_half, units, COLS), bf16),
            pltpu.VMEM((rows, half_width), bf16),
            pltpu.VMEM((rows, half_width), f32),
            pltpu.VMEM((rows, half_width), f32),
            pltpu.VMEM((n_half, rows, COLS), f32),
            pltpu.VMEM((2, n_half, rows, COLS), f32),
            pltpu.VMEM((2, n_half, rows, COLS), f32),
            pltpu.VMEM((n_wd, rows, COLS), f32),
            pltpu.VMEM((rows, model), bf16),
            pltpu.VMEM((2, rows, units), bf16),
            pltpu.VMEM((n_gu, rows, COLS), f32),
            pltpu.VMEM((n_gu, rows, COLS), f32),
            pltpu.VMEM((n_wd, rows, COLS), f32),
            dma((2,)), dma((2, n_half)), dma((2, n_half)), dma((2, n_gu)),
            dma, dma,
            dma((n_gu,)), dma((n_gu,)),
            dma((2, n_half)), dma((2, n_half)),
            dma((2, n_half)), dma((2, n_half)),
        ],
        compiler_params=pltpu.CompilerParams(collective_id=0, has_side_effects=True, vmem_limit_bytes=54 << 20),
        name="tail",
    )(*(pltpu.with_memory_space_constraint(x, pltpu.VMEM) for x in parts), *(pltpu.with_memory_space_constraint(x, pltpu.HBM) for x in (hidden, norm_mlp[None, :])), w_out, w_gate_up, w_down)
    return out.astype(bf16)


def solution(mesh):
    cache_spec = P('dp', 'sp', 'tp', None)

    def local_step(hidden, positions, norm_attn, norm_mlp, w_qkv, w_out, w_gate_up, w_down, k_cache, v_cache):
        num_rows, block_len, kv_local, head_dim = k_cache.shape
        k_t, v_t = k_cache.transpose(0, 2, 3, 1), v_cache.transpose(0, 2, 3, 1)
        q_rows, new_t, k_ring, v_ring = project(positions, hidden, norm_attn, w_qkv, k_t, v_t)
        k_upd, v_upd, own, other, k_ring, v_ring = attend(positions, q_rows, new_t, k_ring, v_ring, k_t, v_t)
        swap = lambda value, mask: lax.ppermute(value, 'sp', [(i, i ^ mask) for i in range(4)])
        parts = (own, swap(other, 1), swap(own, 2), swap(other, 3))
        k_upd, v_upd = write_rest(k_ring, v_ring, k_upd, v_upd)
        result = layer_tail(parts, hidden, norm_mlp, w_out, w_gate_up, w_down, head_dim)
        return result, k_upd.transpose(0, 3, 1, 2), v_upd.transpose(0, 3, 1, 2)

    return jax.shard_map(local_step, mesh=mesh, in_specs=(P('dp', None), P('dp'), P(None), P(None), P(None, 'tp'), P('tp', None), P(None, 'tp'), P('tp', None), cache_spec, cache_spec), out_specs=(P('dp', None), cache_spec, cache_spec), check_vma=False)
```

```python
import functools
import math

import jax
import jax.numpy as jnp
from jax import lax
from jax.experimental import pallas as pl
from jax.experimental.pallas import tpu as pltpu
from jax.sharding import PartitionSpec as P

WINDOW = 2047
ROPE_BASE = 10000.0
NORM_EPS = 1e-5
NEG = -1e30
MESH = pl.DeviceIdType.MESH


QKV_COLS = 384
SLOTS = 8
PRE = 7
DRAIN = 3


def project_kernel(dim, pos_hbm, hid_hbm, gain_hbm, w_hbm, k_hbm, v_hbm, q_ref, new_t, k_ring, v_ring,
                   pos_ref, hid_ref, gain_ref, w_buf, normed_ref, qkv_t, turned, msg, gath,
                   w_sem, in_sem, side_sem, s_send, s_recv):
    sp = lax.axis_index('sp')
    rows, model = hid_ref.shape
    mine = qkv_t.shape[0]
    n_w = mine // QKV_COLS
    w_copies = []
    for i in range(n_w):
        first = pl.multiple_of(sp * mine + i * QKV_COLS, QKV_COLS)
        w_copies.append(pltpu.make_async_copy(w_hbm.at[:, pl.ds(first, QKV_COLS)], w_buf.at[i], w_sem.at[i]))
    side = [pltpu.make_async_copy(src, dst, side_sem.at[i]) for i, (src, dst) in enumerate(((hid_hbm, hid_ref), (gain_hbm, gain_ref), (pos_hbm, pos_ref)))]
    loads = []
    for b in range(PRE):
        loads.append(pltpu.make_async_copy(k_hbm.at[b], k_ring.at[b], in_sem.at[0, b]))
        loads.append(pltpu.make_async_copy(v_hbm.at[b], v_ring.at[b], in_sem.at[1, b]))
    for copy in side + w_copies:
        copy.start()
    barrier = pltpu.get_barrier_semaphore()
    for step in range(1, 4):
        pl.semaphore_signal(barrier, inc=1, device_id={'sp': lax.rem(sp + step, 4)}, device_id_type=MESH)
    for copy in side:
        copy.wait()

    half = dim // 2
    lane = lax.broadcasted_iota(jnp.int32, (1, 128), 1)
    pos_row = jnp.zeros((1, 128), jnp.int32)
    for b in range(rows):
        pos_row = jnp.where(lane == b, pos_ref[b], pos_row)
    pair = lax.broadcasted_iota(jnp.int32, (half, 128), 0).astype(jnp.float32)
    angles = pos_row.astype(jnp.float32) * jnp.exp(pair * (-2.0 / dim * math.log(ROPE_BASE)))
    cos_t, sin_t = jnp.cos(angles), jnp.sin(angles)

    resid = hid_ref[...].astype(jnp.float32)
    inv = lax.rsqrt(jnp.sum(resid * resid, axis=1, keepdims=True) / model + NORM_EPS)
    normed_ref[...] = (resid * inv * gain_ref[...]).astype(jnp.bfloat16)
    pad = jnp.zeros((128 - rows, QKV_COLS), jnp.float32)
    for i in range(n_w):
        w_copies[i].wait()
        for copy in loads[i * len(loads) // n_w:(i + 1) * len(loads) // n_w]:
            copy.start()
        part = jnp.dot(normed_ref[...], w_buf[i], preferred_element_type=jnp.float32)
        qkv_t[i * QKV_COLS:(i + 1) * QKV_COLS, :] = jnp.concatenate([part, pad], axis=0).T
    third = mine // 3
    for h in range(third // dim):
        for part in range(2):
            first = (3 * h + part) * dim
            at = part * third + h * dim
            low, high = qkv_t[first:first + half, :], qkv_t[first + half:first + dim, :]
            turned[at:at + half, :] = low * cos_t - high * sin_t
            turned[at + half:at + dim, :] = high * cos_t + low * sin_t
        turned[2 * third + h * dim:2 * third + (h + 1) * dim, :] = qkv_t[(3 * h + 2) * dim:(3 * h + 3) * dim, :]
    own_rows = turned[...].T[:rows, :]
    msg[...] = own_rows
    pl.semaphore_wait(barrier, 3)
    sends = []
    for step in (2, 1, 3):
        copy = pltpu.make_async_remote_copy(src_ref=msg, dst_ref=gath.at[sp], send_sem=s_send.at[step - 1], recv_sem=s_recv.at[step - 1],
                                            device_id={'sp': lax.rem(sp + step, 4)}, device_id_type=MESH)
        copy.start()
        sends.append(copy)
    gath[sp] = own_rows
    for copy in sends:
        copy.wait_recv()
    q_ref[...] = gath[:, :, :third]
    pad = jnp.zeros((128 - rows, third), jnp.float32)
    for which in range(2):
        for s in range(4):
            entry = gath[s, :, (1 + which) * third:(2 + which) * third]
            new_t[which, s * third:(s + 1) * third, :] = jnp.concatenate([entry, pad], axis=0).T
    for copy in loads:
        copy.wait()
    for copy in sends:
        copy.wait_send()


def project(positions, hidden, norm_attn, w_qkv, k_t, v_t):
    rows, heads, dim, block = k_t.shape
    model, mine = hidden.shape[1], w_qkv.shape[1] // 4
    vmem = pl.BlockSpec(memory_space=pltpu.VMEM)
    hbm = pl.BlockSpec(memory_space=pl.ANY)
    f32, bf16, dma = jnp.float32, jnp.bfloat16, pltpu.SemaphoreType.DMA
    return pl.pallas_call(
        functools.partial(project_kernel, dim),
        out_shape=(pltpu.VMEM((4, rows, mine // 3), f32), pltpu.VMEM((2, heads * dim, 128), f32), pltpu.VMEM((SLOTS, heads, dim, block), bf16), pltpu.VMEM((SLOTS, heads, dim, block), bf16)),
        in_specs=[hbm] * 6,
        out_specs=(vmem, vmem, vmem, vmem),
        scratch_shapes=[
            pltpu.SMEM((rows,), jnp.int32),
            pltpu.VMEM((rows, model), bf16),
            pltpu.VMEM((1, model), f32),
            pltpu.VMEM((mine // QKV_COLS, model, QKV_COLS), bf16),
            pltpu.VMEM((rows, model), bf16),
            pltpu.VMEM((mine, 128), f32),
            pltpu.VMEM((mine, 128), f32),
            pltpu.VMEM((rows, mine), f32),
            pltpu.VMEM((4, rows, mine), f32),
            dma((mine // QKV_COLS,)), dma((2, PRE)), dma((3,)), dma((3,)), dma((3,)),
        ],
        compiler_params=pltpu.CompilerParams(collective_id=1, has_side_effects=True, vmem_limit_bytes=8200 << 10),
        name="project",
    )(*(pltpu.with_memory_space_constraint(x, pltpu.HBM) for x in (positions, hidden, norm_attn[None, :])), w_qkv, k_t, v_t)


def attend_kernel(pos_hbm, q_ref, new_t, k_in, v_in, k_hbm, v_hbm, ko_hbm, vo_hbm, om_ref, k_ring, v_ring,
                  pos_ref, in_sem, out_sem, side_sem):
    rows, third = q_ref.shape[1:]
    heads, dim, block = k_ring.shape[1:]
    width = heads * dim
    base = lax.axis_index('sp') * block

    def load(b, which):
        slot = lax.rem(b, SLOTS)
        src, buf = ((k_hbm, k_ring), (v_hbm, v_ring))[which]
        return pltpu.make_async_copy(src.at[b], buf.at[slot], in_sem.at[which, slot])

    def store(b, which):
        slot = lax.rem(b, SLOTS)
        dst, buf = ((ko_hbm, k_ring), (vo_hbm, v_ring))[which]
        return pltpu.make_async_copy(buf.at[slot], dst.at[b], out_sem.at[which, slot])

    pos_copy = pltpu.make_async_copy(pos_hbm, pos_ref, side_sem)
    pos_copy.start()
    for b in range(PRE, SLOTS):
        load(b, 0).start()
        load(b, 1).start()
    pos_copy.wait()

    own = lax.broadcasted_iota(jnp.int32, (heads, width), 1) // dim == lax.broadcasted_iota(jnp.int32, (heads, width), 0)
    lane_ids = lax.broadcasted_iota(jnp.int32, (heads, 128), 1)
    head_ids = lax.broadcasted_iota(jnp.int32, (heads, 128), 0)
    half_heads, half_width = heads // 2, width // 2

    def patch(buf, slot, which, b, pos):
        at = pos - base

        @pl.when((at >= 0) & (at < block))
        def _():
            inner = lax.rem(at, 128)
            start = pl.multiple_of(at - inner, 128)
            shift = lax.rem(inner - b + 128, 128)
            hit = lax.broadcasted_iota(jnp.int32, (dim, 128), 1) == inner
            for h in range(heads):
                entry = pltpu.roll(new_t[which, h * dim:(h + 1) * dim, :], shift, 1)
                old = buf[slot, h, :, pl.ds(start, 128)].astype(jnp.float32)
                buf[slot, h, :, pl.ds(start, 128)] = jnp.where(hit, entry, old).astype(jnp.bfloat16)

    def step(b, carry):
        slot = lax.rem(b, SLOTS)
        pos = pos_ref[b]

        @pl.when((b >= DRAIN) & (b + SLOTS - DRAIN < rows))
        def _():
            for which in range(2):
                store(b - DRAIN, which).wait()
                load(b + SLOTS - DRAIN, which).start()

        @pl.when(b >= PRE)
        def _():
            load(b, 0).wait()

        patch(k_ring, slot, 0, b, pos)
        store(b, 0).start()
        q_row = jnp.concatenate([q_ref[s, pl.ds(b, 1), :] for s in range(4)], axis=1)
        q_diag = jnp.where(own, jnp.broadcast_to(q_row, (heads, width)), 0.0).astype(jnp.bfloat16)
        scores = jnp.dot(q_diag, k_ring[slot].reshape(width, block), preferred_element_type=jnp.float32) * (dim ** -0.5)
        slot_ids = lax.broadcasted_iota(jnp.int32, (heads, block), 1) + base
        in_window = (slot_ids <= pos) & (slot_ids >= pos - WINDOW)
        scores = jnp.where(in_window, scores, NEG)
        row_max = jnp.max(scores, axis=1, keepdims=True)
        weights = jnp.where(in_window, jnp.exp(scores - row_max), 0.0)
        row_sum = jnp.sum(weights, axis=1, keepdims=True)

        @pl.when(b >= PRE)
        def _():
            load(b, 1).wait()

        patch(v_ring, slot, 1, b, pos)
        store(b, 1).start()
        acc = lax.dot_general(weights.astype(jnp.bfloat16), v_ring[slot].reshape(width, block), (((1,), (1,)), ((), ())), preferred_element_type=jnp.float32)
        o_row = jnp.sum(jnp.where(own, acc, 0.0), axis=0, keepdims=True)
        for core in range(2):
            local = head_ids - core * half_heads
            keep = (local >= 0) & (local < half_heads)
            stats = jnp.where(keep & (lane_ids == local), row_max, 0.0) + jnp.where(keep & (lane_ids == local + half_heads), row_sum, 0.0)
            row = jnp.concatenate([o_row[:, core * half_width:(core + 1) * half_width], jnp.sum(stats, axis=0, keepdims=True)], axis=1)
            at_row = lax.broadcasted_iota(jnp.int32, (rows, half_width + 128), 0) == b
            om_ref[core] = jnp.where(at_row, row, om_ref[core])
        return carry

    lax.fori_loop(0, rows, step, 0)
    for b in range(rows - SLOTS, rows):
        store(b, 0).wait()
        store(b, 1).wait()


def attend(positions, q_rows, new_t, k_ring, v_ring, k_t, v_t):
    rows, heads, dim, block = k_t.shape
    width = heads * dim
    vmem = pl.BlockSpec(memory_space=pltpu.VMEM)
    hbm = pl.BlockSpec(memory_space=pl.ANY)
    f32, bf16, dma = jnp.float32, jnp.bfloat16, pltpu.SemaphoreType.DMA
    ring = pltpu.VMEM((SLOTS, heads, dim, block), bf16)
    k_upd, v_upd, om, _, _ = pl.pallas_call(
        attend_kernel,
        out_shape=(jax.ShapeDtypeStruct(k_t.shape, k_t.dtype), jax.ShapeDtypeStruct(v_t.shape, v_t.dtype), pltpu.VMEM((2, rows, width // 2 + 128), f32), ring, ring),
        in_specs=[hbm, vmem, vmem, vmem, vmem, hbm, hbm],
        out_specs=(hbm, hbm, vmem, vmem, vmem),
        scratch_shapes=[
            pltpu.SMEM((rows,), jnp.int32),
            dma((2, SLOTS)), dma((2, SLOTS)), dma,
        ],
        input_output_aliases={3: 3, 4: 4},
        compiler_params=pltpu.CompilerParams(vmem_limit_bytes=5 << 20),
        name="attend",
    )(pltpu.with_memory_space_constraint(positions, pltpu.HBM), *(pltpu.with_memory_space_constraint(x, pltpu.VMEM) for x in (q_rows, new_t, k_ring, v_ring)), k_t, v_t)
    return k_upd, v_upd, om


COLS = 512


def tail_kernel(dim, om_ref, hid_hbm, gain_hbm, wo_hbm, wgu_hbm, wd_hbm, out_ref,
                hid_ref, gain_ref, obuf, wo, wg, wu, wd, o_cat, o_snd, o_got, acc, ysnd, ygot, x1, r2, act, a_snd, a_got, x2,
                side_sem, wo_sem, wd_sem, gu_sem, o_send, o_recv, p_send, p_recv, a_send, a_recv, y_send, y_recv, g_send, g_recv):
    tp, sp = lax.axis_index('tp'), lax.axis_index('sp')
    core = lax.rem(sp, 2)
    partner = sp + 1 - 2 * core
    rows = hid_ref.shape[0]
    half_width = wo.shape[2]
    n_half = x1.shape[0] // 2
    n_gu = wg.shape[0]
    units = wd.shape[2]
    ffn = wgu_hbm.shape[1] // 2

    def column(j):
        return pl.ds(pl.multiple_of((core * n_half + j) * COLS, COLS), COLS)

    side = [pltpu.make_async_copy(hid_hbm, hid_ref, side_sem.at[0]), pltpu.make_async_copy(gain_hbm, gain_ref, side_sem.at[1])]
    out_copies, down_copies, gate_up_copies = [[], []], [[], []], []
    for k, owner in enumerate((core, 1 - core)):
        for j in range(n_half):
            out_copies[k].append(pltpu.make_async_copy(wo_hbm.at[pl.ds(owner * half_width, half_width), column(j)], wo.at[k, j], wo_sem.at[k, j]))
            down_copies[k].append(pltpu.make_async_copy(wd_hbm.at[pl.ds(owner * units, units), column(j)], wd.at[k, j], wd_sem.at[k, j]))
    for i in range(n_gu):
        first = core * units + i * COLS
        gate_up_copies.append(pltpu.make_async_copy(wgu_hbm.at[:, pl.ds(pl.multiple_of(first, COLS), COLS)], wg.at[i], gu_sem.at[0, i]))
        gate_up_copies.append(pltpu.make_async_copy(wgu_hbm.at[:, pl.ds(pl.multiple_of(ffn + first, COLS), COLS)], wu.at[i], gu_sem.at[1, i]))
    barrier = pltpu.get_barrier_semaphore()
    for step in range(1, 4):
        pl.semaphore_signal(barrier, inc=1, device_id={'sp': lax.rem(sp + step, 4)}, device_id_type=MESH)
    pl.semaphore_signal(barrier, inc=1, device_id={'tp': 1 - tp}, device_id_type=MESH)
    for copy in side + out_copies[0] + out_copies[1]:
        copy.start()
    pl.semaphore_wait(barrier, 4)

    sent = []

    def send(src, dst, send_sem, recv_sem, where):
        copy = pltpu.make_async_remote_copy(src_ref=src, dst_ref=dst, send_sem=send_sem, recv_sem=recv_sem, device_id=where, device_id_type=MESH)
        copy.start()
        sent.append(copy)
        return copy

    first_copies = []
    for step in (2, 1, 3):
        peer = lax.rem(sp + step, 4)
        first_copies.append(send(om_ref.at[lax.rem(peer, 2)], obuf.at[sp], o_send.at[step - 1], o_recv.at[step - 1], {'sp': peer}))
    obuf[sp] = om_ref[core]
    for copy in gate_up_copies:
        copy.start()
    for copy in first_copies:
        copy.wait_recv()

    heads = half_width // dim
    stats = [obuf[s, :, half_width:] for s in range(4)]
    top = functools.reduce(jnp.maximum, stats)
    alphas = [jnp.exp(st - top) for st in stats]
    total = functools.reduce(lambda a, b: a + b, [al * pltpu.roll(st, 128 - heads, 1) for al, st in zip(alphas, stats)])
    betas = [al / total for al in alphas]
    lane = lax.broadcasted_iota(jnp.int32, (rows, 128), 1)
    for k in range(half_width // 128):
        first, last = 128 * k // dim, (128 * k + 127) // dim
        value = None
        for s in range(4):
            scale = jnp.broadcast_to(betas[s][:, first:first + 1], (rows, 128))
            for h in range(first + 1, last + 1):
                scale = jnp.where(lane >= h * dim - 128 * k, betas[s][:, h:h + 1], scale)
            term = scale * obuf[s, :, 128 * k:128 * (k + 1)]
            value = term if value is None else value + term
        value = value.astype(jnp.bfloat16)
        o_cat[:, 128 * k:128 * (k + 1)] = value
        o_snd[:, 128 * k:128 * (k + 1)] = value.astype(jnp.float32)

    def product(lhs, w_ref, copies, j):
        copies[j].wait()
        return jnp.dot(lhs, w_ref[j], preferred_element_type=jnp.float32)

    def spread(stage, part_of, base_of, dst):
        second = []
        for j in range(n_half):
            ysnd[stage, j] = part_of(j).astype(jnp.bfloat16).astype(jnp.float32)
            second.append(send(ysnd.at[stage, j], ygot.at[stage, j], y_send.at[stage, j], y_recv.at[stage, j], {'tp': 1 - tp}))
        third = []
        for j in range(n_half):
            second[j].wait_recv()
            if stage == 0 and j == 0:
                for copy in down_copies[0] + down_copies[1]:
                    copy.start()
            dst[core * n_half + j] = base_of(j) + (ysnd[stage, j] + ygot[stage, j])
            third.append(send(dst.at[core * n_half + j], dst.at[core * n_half + j], g_send.at[stage, j], g_recv.at[stage, j], {'sp': partner}))
        for copy in third:
            copy.wait_recv()

    o_copy = send(o_snd, o_got, p_send, p_recv, {'sp': partner})
    for j in range(n_half):
        acc[j] = product(o_cat[...], wo.at[0], out_copies[0], j)
    for copy in side:
        copy.wait()
    o_copy.wait_recv()
    o_other = o_got[...].astype(jnp.bfloat16)
    spread(0, lambda j: acc[j] + product(o_other, wo.at[1], out_copies[1], j), lambda j: hid_ref[:, column(j)].astype(jnp.float32), x1)

    square = functools.reduce(lambda a, b: a + b, [x1[i] * x1[i] for i in range(2 * n_half)])
    inv = lax.rsqrt(jnp.sum(square, axis=1, keepdims=True) / (2 * n_half * COLS) + NORM_EPS)
    for i in range(2 * n_half):
        cut = slice(i * COLS, (i + 1) * COLS)
        r2[:, cut] = (x1[i] * inv * gain_ref[:, cut]).astype(jnp.bfloat16)

    a_copies = []
    for i in range(n_gu):
        gate_up_copies[2 * i].wait()
        gate_up_copies[2 * i + 1].wait()
        gate = jnp.dot(r2[...], wg[i], preferred_element_type=jnp.float32)
        up = jnp.dot(r2[...], wu[i], preferred_element_type=jnp.float32)
        value = (gate * jax.nn.sigmoid(gate) * up).astype(jnp.bfloat16)
        act[0, :, i * COLS:(i + 1) * COLS] = value
        a_snd[i] = value.astype(jnp.float32)
        a_copies.append(send(a_snd.at[i], a_got.at[i], a_send.at[i], a_recv.at[i], {'sp': partner}))
    for j in range(n_half):
        acc[j] = product(act[0], wd.at[0], down_copies[0], j)
    for i in range(n_gu):
        a_copies[i].wait_recv()
        act[1, :, i * COLS:(i + 1) * COLS] = a_got[i].astype(jnp.bfloat16)
    spread(1, lambda j: acc[j] + product(act[1], wd.at[1], down_copies[1], j), lambda j: x1[core * n_half + j], x2)
    for i in range(2 * n_half):
        out_ref[:, i * COLS:(i + 1) * COLS] = x2[i]
    for copy in sent:
        copy.wait_send()


def layer_tail(om, hidden, norm_mlp, w_out, w_gate_up, w_down, dim):
    rows, model = hidden.shape
    half_width, units = w_out.shape[0] // 2, w_down.shape[0] // 2
    n_wd, n_gu = model // COLS, units // COLS
    n_half = n_wd // 2
    f32, bf16 = jnp.float32, jnp.bfloat16
    vmem = pl.BlockSpec(memory_space=pltpu.VMEM)
    hbm = pl.BlockSpec(memory_space=pl.ANY)
    dma = pltpu.SemaphoreType.DMA
    out = pl.pallas_call(
        functools.partial(tail_kernel, dim),
        out_shape=pltpu.VMEM((rows, model), f32),
        in_specs=[vmem, hbm, hbm, hbm, hbm, hbm],
        out_specs=vmem,
        scratch_shapes=[
            pltpu.VMEM((rows, model), bf16),
            pltpu.VMEM((1, model), f32),
            pltpu.VMEM((4, rows, half_width + 128), f32),
            pltpu.VMEM((2, n_half, half_width, COLS), bf16),
            pltpu.VMEM((n_gu, model, COLS), bf16),
            pltpu.VMEM((n_gu, model, COLS), bf16),
            pltpu.VMEM((2, n_half, units, COLS), bf16),
            pltpu.VMEM((rows, half_width), bf16),
            pltpu.VMEM((rows, half_width), f32),
            pltpu.VMEM((rows, half_width), f32),
            pltpu.VMEM((n_half, rows, COLS), f32),
            pltpu.VMEM((2, n_half, rows, COLS), f32),
            pltpu.VMEM((2, n_half, rows, COLS), f32),
            pltpu.VMEM((n_wd, rows, COLS), f32),
            pltpu.VMEM((rows, model), bf16),
            pltpu.VMEM((2, rows, units), bf16),
            pltpu.VMEM((n_gu, rows, COLS), f32),
            pltpu.VMEM((n_gu, rows, COLS), f32),
            pltpu.VMEM((n_wd, rows, COLS), f32),
            dma((2,)), dma((2, n_half)), dma((2, n_half)), dma((2, n_gu)),
            dma((3,)), dma((3,)),
            dma, dma,
            dma((n_gu,)), dma((n_gu,)),
            dma((2, n_half)), dma((2, n_half)),
            dma((2, n_half)), dma((2, n_half)),
        ],
        compiler_params=pltpu.CompilerParams(collective_id=0, has_side_effects=True, vmem_limit_bytes=54 << 20),
        name="tail",
    )(pltpu.with_memory_space_constraint(om, pltpu.VMEM), *(pltpu.with_memory_space_constraint(x, pltpu.HBM) for x in (hidden, norm_mlp[None, :])), w_out, w_gate_up, w_down)
    return out.astype(bf16)


def solution(mesh):
    cache_spec = P('dp', 'sp', 'tp', None)

    def local_step(hidden, positions, norm_attn, norm_mlp, w_qkv, w_out, w_gate_up, w_down, k_cache, v_cache):
        num_rows, block_len, kv_local, head_dim = k_cache.shape
        k_t, v_t = k_cache.transpose(0, 2, 3, 1), v_cache.transpose(0, 2, 3, 1)
        q_rows, new_t, k_ring, v_ring = project(positions, hidden, norm_attn, w_qkv, k_t, v_t)
        k_upd, v_upd, om = attend(positions, q_rows, new_t, k_ring, v_ring, k_t, v_t)
        result = layer_tail(om, hidden, norm_mlp, w_out, w_gate_up, w_down, head_dim)
        return result, k_upd.transpose(0, 3, 1, 2), v_upd.transpose(0, 3, 1, 2)

    return jax.shard_map(local_step, mesh=mesh, in_specs=(P('dp', None), P('dp'), P(None), P(None), P(None, 'tp'), P('tp', None), P(None, 'tp'), P('tp', None), cache_spec, cache_spec), out_specs=(P('dp', None), cache_spec, cache_spec), check_vma=False)
```
